512 devices in a mesh: group: 2 (over y), plane: 16 (over z), planey: 8 (over x), ens: 2 (over core).
Axes of the slice: x: 8, y: 2, z: 16, core: 2. Of those that a mesh axis runs over, the one named last changes fastest.
The devices are a block of a 8x8x16 slice.
Arguments:
- u_prior: float32 [8, 2, 10, 256, 1024], P(('group', 'ens'), None, None, 'plane', 'planey'), parts along dimension 0, may hold values from -6 to 6
- friction_rows: int32 [8], P(('group', 'ens')), parts along dimension 0, may hold values from 0 to 15
- friction_table: float32 [32, 256, 1024], P('group', 'plane', 'planey'), parts along dimension 0, may hold values from 0.3 to 3
- bed_fixed: int32 [256, 1024], P('plane', 'planey'), may hold values from -536870912 to 536870911
- ice_mask: int32 [256, 1024], P('plane', 'planey'), may hold values 0 or 1
Outputs:
- mean_velocity: float32 [4, 10, 256, 1024], P('group', None, 'plane', 'planey'), parts along dimension 0
The draws below stay inside these ranges and needn't reach their ends.
There are 2 independent parts, one for each index of `group`. The reference program is written for one: setup_inputs(seed, part) draws one part's arguments, and reference() takes and returns one part's arrays. A program takes and returns all parts, laid end to end along the dimension named above; an argument that names none is the same for every part. Nothing has to cross between parts.
Inputs may be any that keep to these rules, and one draw needn't show every extreme that they name: `friction_rows`: each sample names one row of the friction table.
All inputs are finite; a program needn't handle non-finite values. No bound on the sum of `ice_mask` on one device may be relied on, other than what follows from the above.
Results may differ from the reference program's by a relative error of at most 0.0003.
Values sent between devices are 32-bit elements; how exact they have to be, the bound alone decides.
A program may use at most 64 MiB of HBM per device.

```python
import math
import jax
import jax.numpy as jnp
from jax import lax

NZ = 10
ITERS = 2
LEVELS = 16
SAMPLES = 4
NX = 256
NY = 1024


def with_ends(drawn, rng, least, largest):
    spot = [jax.random.randint(jax.random.fold_in(rng, axis), (), 0, length) for axis, length in enumerate(drawn.shape)]
    main_axis = drawn.shape.index(max(drawn.shape))
    next_to = spot[:main_axis] + [(spot[main_axis] + 1) % drawn.shape[main_axis]] + spot[main_axis + 1:]
    return drawn.at[tuple(spot)].set(least).at[tuple(next_to)].set(largest)


def shard_levels(stream_key, dims, shards, smallest, top_value):
    factor_of, own = 1.0, jax.random.fold_in(stream_key, 6)
    for axis_at, blocks in shards:
        draws = jnp.exp(jax.random.uniform(jax.random.fold_in(own, axis_at), (blocks,), jnp.float32, smallest / len(shards), top_value / len(shards)))
        factor_of = factor_of * jnp.repeat(draws, dims[axis_at] // blocks).reshape([-1 if axis == axis_at else 1 for axis in range(len(dims))])
    return factor_of


def scatter_about(stream_key, shape, width, bound, split=(), kind=jnp.bfloat16):
    values = jax.random.normal(stream_key, shape, jnp.float32) * width
    if len(split) > 0:
        values = shard_levels(stream_key, shape, split, -0.22, 0.18) * values
    return jnp.clip(values, min=-bound, max=bound).astype(kind)


def setup_inputs(seed: int = 0, part: int = 0) -> dict:
    keys = jax.random.split(jax.random.key(seed), 6)
    own_keys = jax.random.split(jax.random.fold_in(keys[5], part), 6)
    return {
        "u_prior": scatter_about(own_keys[0], (SAMPLES, 2, NZ, NX, NY), 1.0, 6.0, ((0, 2), (3, 16), (4, 8)), jnp.float32),
        "friction_rows": with_ends(jax.random.randint(own_keys[1], (SAMPLES,), 0, LEVELS), jax.random.fold_in(own_keys[1], 1), 0, LEVELS - 1).astype(jnp.int32),
        "friction_table": jnp.clip(jnp.exp(math.log(3.0) - 2.3025851 * jax.random.uniform(own_keys[2], (LEVELS, NX, NY), jnp.float32) ** shard_levels(own_keys[2], (LEVELS, NX, NY), ((1, 16), (2, 8)), -0.2, 0.2)), 0.3, 3.0),
        "bed_fixed": with_ends(jax.random.randint(keys[3], (NX, NY), -536870912, 536870912), jax.random.fold_in(keys[3], 1), -536870912, 536870911).astype(jnp.int32),
        "ice_mask": with_ends((jax.random.randint(keys[4], (NX, NY), 0, 8) < 7).astype(jnp.int32), jax.random.fold_in(keys[4], 1), 0, 1),
    }


bed_unit = 2.0 ** -29
factor_u = (2.0, 1.0, 0.5)
factor_v = (2.0, 0.5, 1.0)


def coefficient(offset):
    nonzero = len([entry for entry in offset if entry != 0])
    weight_u = 0.25 ** (nonzero - 1)
    weight_v = weight_u
    for dimension in range(3):
        if offset[dimension] != 0:
            weight_u = weight_u * factor_u[dimension]
            weight_v = weight_v * factor_v[dimension]
    return jnp.array([weight_u, weight_v], jnp.float32).reshape(2, 1, 1, 1)


def neighbour_sum(padded):
    layers = padded.shape[-3] - 2
    span_x = padded.shape[-2] - 2
    span_y = padded.shape[-1] - 2
    summed = None
    for step_z in (-1, 0, 1):
        for step_x in (-1, 0, 1):
            for step_y in (-1, 0, 1):
                if step_z == 0 and step_x == 0 and step_y == 0:
                    continue
                window = padded[..., 1 + step_z:1 + step_z + layers, 1 + step_x:1 + step_x + span_x, 1 + step_y:1 + step_y + span_y]
                addend = coefficient((step_z, step_x, step_y)) * window
                summed = addend if summed is None else summed + addend
    return summed


def strain_roots(extended):
    padded = jnp.pad(extended, [(0, 0)] * (extended.ndim - 3) + [(1, 1), (0, 0), (0, 0)])
    along_x = (padded[..., 1:-1, 2:, 1:-1] - padded[..., 1:-1, :-2, 1:-1]) * 0.5
    along_y = (padded[..., 1:-1, 1:-1, 2:] - padded[..., 1:-1, 1:-1, :-2]) * 0.5
    along_z = (padded[..., 2:, 1:-1, 1:-1] - padded[..., :-2, 1:-1, 1:-1]) * 0.5
    stretch_x = along_x[..., 0, :, :, :]
    stretch_y = along_y[..., 1, :, :, :]
    shear_one = along_y[..., 0, :, :, :]
    shear_two = along_x[..., 1, :, :, :]
    vertical_u = along_z[..., 0, :, :, :]
    vertical_v = along_z[..., 1, :, :, :]
    shear = shear_one + shear_two
    strain = stretch_x * stretch_x + stretch_y * stretch_y + stretch_x * stretch_y + 0.25 * shear * shear + 0.25 * (vertical_u * vertical_u + vertical_v * vertical_v)
    return jnp.power(strain + 0.1, -1.0 / 6.0)[..., None, :, :, :]


def reference(u_prior, friction_rows, friction_table, bed_fixed, ice_mask):
    cover = ice_mask.astype(jnp.float32)
    bed = bed_fixed.astype(jnp.float32) * bed_unit
    bed_pad = jnp.pad(bed, 1)
    slope_x = (bed_pad[2:, 1:-1] - bed_pad[:-2, 1:-1]) * 0.5
    slope_y = (bed_pad[1:-1, 2:] - bed_pad[1:-1, :-2]) * 0.5
    thickness = 1.0 + 2.0 * jnp.arange(NX, dtype=jnp.float32)[:, None] / (NX - 1)
    force = jnp.stack([-(cover * thickness * slope_x), -(cover * thickness * slope_y)])[:, None, :, :]
    bottom = (jnp.arange(NZ, dtype=jnp.int32) == 0).astype(jnp.float32)[:, None, None]
    levels = jnp.arange(LEVELS, dtype=jnp.int32)

    def solve(summed, inputs):
        prior, table_row = inputs
        extended = jnp.pad(prior, ((0, 0), (0, 0), (1, 1), (1, 1)))
        roots = cover * strain_roots(extended)
        across = neighbour_sum(jnp.pad(roots, ((0, 0), (1, 1), (1, 1), (1, 1))))
        chosen = (levels == table_row).astype(jnp.float32)
        friction = jnp.sum(chosen[:, None, None] * friction_table, axis=0)
        diag = cover * friction * bottom + (1.0 - cover)

        def operate(field):
            product = roots * field
            nearby = neighbour_sum(jnp.pad(product, ((0, 0), (1, 1), (1, 1), (1, 1))))
            return roots * (across * field - nearby) + diag * field

        solution = prior * cover
        residual = force - operate(solution)
        direction = residual
        norm_now = jnp.sum(residual * residual)
        for step in range(ITERS):
            image = operate(direction)
            alpha = norm_now / jnp.sum(direction * image)
            solution = solution + alpha * direction
            if step + 1 < ITERS:
                residual = residual - alpha * image
                norm_next = jnp.sum(residual * residual)
                direction = residual + (norm_next / norm_now) * direction
                norm_now = norm_next
        return summed + solution, None

    start = jnp.zeros((2, NZ, NX, NY), jnp.float32)
    summed = lax.scan(solve, start, (u_prior, friction_rows))[0]
    return summed / SAMPLES
```

```python
import functools

import jax
import jax.numpy as jnp
from jax import lax
from jax.experimental import pallas as pl
from jax.experimental.pallas import tpu as pltpu
from jax.sharding import PartitionSpec as P

bed_unit = 2.0 ** (-29)
HALO = 4
TOP = 8
OWN = TOP + HALO
PITCH = 8
MESH = pl.DeviceIdType.MESH
along_z = 0.5
along_x = (0.25, 0.125)
along_y = (0.125, 0.25)
BED, MASK, FRICTION = 4, 5, 6
EDGE_U, EDGE_R, EDGE_0, EDGE_1, EDGE_2 = 0, 2, 3, 5, 7


def kernel(
    sizes,
    u_hbm,
    picks,
    table_hbm,
    bed_hbm,
    mask_hbm,
    out,
    uw,
    mw,
    xo,
    xl,
    xr,
    table,
    bed_in,
    mask_in,
    strip,
    shifted,
    edge,
    fixed,
    roots,
    tr,
    tp,
    tq,
    field_a,
    all_residual,
    all_image,
    all_start,
    gram,
    ring_y,
    ring_x,
    local_sem,
    halo_send,
    halo_recv,
    hand_sem,
    pair_send,
    pair_recv,
    y_send,
    y_recv,
    x_send,
    x_recv,
):
    planes, planeys = sizes
    members, comps, layers, rows, cols = u_hbm.shape
    wide = rows + 2 * HALO
    end = TOP + wide
    plane = lax.axis_index("plane")
    planey = lax.axis_index("planey")
    ens = lax.axis_index("ens")

    def at(dx, dy):
        return {
            "plane": lax.rem(plane + dx + planes, planes),
            "planey": lax.rem(planey + dy + planeys, planeys),
        }

    partner = {"ens": 1 - ens}
    around = [(dx, dy) for dx in (-1, 0, 1) for dy in (-1, 0, 1) if (dx, dy) != (0, 0)]

    def exists(dx, dy):
        flag = None
        for step, index, count in ((dx, plane, planes), (dy, planey, planeys)):
            if step != 0:
                part = index > 0 if step < 0 else index < count - 1
                flag = part if flag is None else jnp.logical_and(flag, part)
        return flag

    barrier = pltpu.get_barrier_semaphore()
    for dx, dy in around:
        pl.semaphore_signal(barrier, inc=1, device_id=at(dx, dy), device_id_type=MESH)
    pl.semaphore_signal(barrier, inc=1, device_id=partner, device_id_type=MESH)

    load_u = pltpu.make_async_copy(
        u_hbm, uw.at[:, :, pl.ds(1, layers), pl.ds(OWN, rows), :], local_sem.at[0]
    )
    load_table = pltpu.make_async_copy(table_hbm, table, local_sem.at[1])
    load_bed = pltpu.make_async_copy(bed_hbm, bed_in, local_sem.at[2])
    load_mask = pltpu.make_async_copy(mask_hbm, mask_in, local_sem.at[3])
    for load in (load_u, load_bed, load_mask, load_table):
        load.start()

    for end_layer in (0, layers + 1):
        uw[:, :, end_layer, TOP:end, :] = jnp.zeros((members, comps, wide, cols), jnp.float32)
        for buffer in (tr, tp, tq):
            buffer[:, end_layer] = jnp.zeros(buffer.shape[:1] + buffer.shape[2:], jnp.float32)
    for step, first in ((-1, TOP), (1, OWN + rows)):

        @pl.when(jnp.logical_not(exists(step, 0)))
        def _():
            uw[:, :, 1 : 1 + layers, first : first + HALO, :] = jnp.zeros(
                (members, comps, layers, HALO, cols), jnp.float32
            )
            for buffer in (mw, xo, xl, xr):
                buffer[:, first : first + HALO, :] = jnp.zeros(
                    (buffer.shape[0], HALO, cols), jnp.float32
                )

    for step, buffer in ((-1, xl), (1, xr)):

        @pl.when(jnp.logical_not(exists(0, step)))
        def _():
            buffer[:, TOP:end, :] = jnp.zeros((buffer.shape[0], wide, cols), jnp.float32)

    sends = []

    def send(number, dx, dy, source, target):
        copy = pltpu.make_async_remote_copy(
            src_ref=source,
            dst_ref=target,
            send_sem=halo_send.at[number],
            recv_sem=halo_recv.at[number],
            device_id=at(dx, dy),
            device_id_type=MESH,
        )

        @pl.when(exists(dx, dy))
        def _():
            copy.start()

        sends.append((copy, exists(dx, dy), exists(-dx, -dy)))

    def row_range(dx):
        if dx < 0:
            return pl.ds(OWN, HALO), pl.ds(OWN + rows, HALO)
        if dx > 0:
            return pl.ds(OWN + rows - HALO, HALO), pl.ds(TOP, HALO)
        return pl.ds(OWN, rows), pl.ds(OWN, rows)

    load_u.wait()
    pl.semaphore_wait(barrier, len(around) + 1)
    body = pl.ds(1, layers)
    for dx in (-1, 1):
        here, there = row_range(dx)
        send(
            0 if dx < 0 else 1,
            dx,
            0,
            uw.at[:, :, body, here, :],
            uw.at[:, :, body, there, :],
        )

    hands = []
    for axis, count in (("plane", planes), ("planey", planeys)):
        reach = 1
        while reach * 2 <= count // 2:
            hands.append((reach, axis))
            reach *= 2
    hands.sort()

    def greet(number):
        reach, axis = hands[number]
        for step in (-reach, reach):
            target = at(step, 0) if axis == "plane" else at(0, step)
            pl.semaphore_signal(
                hand_sem.at[number], inc=1, device_id=target, device_id_type=MESH
            )

    def greeted(number):
        pl.semaphore_wait(hand_sem.at[number], 2)

    def greet_round(reach):
        for number, (distance, _) in enumerate(hands):
            if distance == reach:
                greet(number)

    def greeted_round(reach):
        for number, (distance, _) in enumerate(hands):
            if distance == reach:
                greeted(number)

    greet_round(1)

    lane = lax.broadcasted_iota(jnp.int32, (rows, cols), 1)
    group = lane // PITCH
    load_bed.wait()
    load_mask.wait()
    load_table.wait()
    bed_own = bed_in[...].astype(jnp.float32) * bed_unit
    mask_own = mask_in[...].astype(jnp.float32)
    mw[0, OWN : OWN + rows, :] = bed_own
    mw[1, OWN : OWN + rows, :] = mask_own
    for member in range(members):
        chosen = table[picks[member]]
        mw[2 + member, OWN : OWN + rows, :] = chosen
        xo[FRICTION + member, OWN : OWN + rows, :] = jnp.where(
            lane < PITCH, pltpu.roll(chosen, HALO, 1), 0.0
        )
    for dx in (-1, 1):
        here, there = row_range(dx)
        send(2 if dx < 0 else 3, dx, 0, mw.at[:, here, :], mw.at[:, there, :])

    def lane_packed(planes_of):
        packed = jnp.zeros((rows, cols), jnp.float32)
        for layer in range(layers):
            turned = pltpu.roll(planes_of(layer), (PITCH * layer + HALO) % cols, 1)
            packed = jnp.where(group == layer, turned, packed)
        return packed

    xo[BED, OWN : OWN + rows, :] = lane_packed(lambda layer: bed_own)
    xo[MASK, OWN : OWN + rows, :] = lane_packed(lambda layer: mask_own)
    for member in range(members):
        for comp in range(comps):
            xo[member * comps + comp, OWN : OWN + rows, :] = lane_packed(
                lambda layer: uw[member, comp, 1 + layer, OWN : OWN + rows, :]
            )
    for number, (dx, dy) in enumerate(around):
        here, there = row_range(dx)
        target = xo if dy == 0 else (xr if dy < 0 else xl)
        send(4 + number, dx, dy, xo.at[:, here, :], target.at[:, there, :])

    greeted_round(1)
    greet_round(2)

    for copy, sent, arrives in sends:

        @pl.when(arrives)
        def _():
            copy.wait_recv()

    lane = lax.broadcasted_iota(jnp.int32, (wide, cols), 1)
    first_lane = lane == 0
    last_lane = lane == cols - 1
    spot = lax.rem(lane, PITCH)
    outer_left = spot < HALO
    left_edge = spot == HALO - 1
    position = (
        plane * rows - HALO + lax.broadcasted_iota(jnp.int32, (wide, cols), 0)
    ).astype(jnp.float32)
    thickness = 1.0 + 2.0 * position / (rows * planes - 1)

    def sides(number, low=TOP, high=end):
        own = xo[number, low:high, :]
        return (
            jnp.where(outer_left, xl[number, low:high, :], own),
            jnp.where(outer_left, own, xr[number, low:high, :]),
        )

    def edges(pair):
        left, right = pair
        return jnp.where(
            left_edge, pltpu.roll(right, cols - 1, 1), pltpu.roll(left, 1, 1)
        )

    def y_pair(value, near):
        return (
            jnp.where(last_lane, near, pltpu.roll(value, cols - 1, 1)),
            jnp.where(first_lane, near, pltpu.roll(value, 1, 1)),
        )

    def turned_edge(value, layer):
        return pltpu.roll(value, cols - HALO - PITCH * layer, 1)

    mask_main = mw[1, TOP:end, :]
    bed_plus, bed_minus = y_pair(mw[0, TOP:end, :], turned_edge(edges(sides(BED)), 0))
    scale = -(mask_main * thickness)
    fixed[0] = mask_main
    fixed[1] = scale * ((mw[0, TOP + 1 : end + 1, :] - mw[0, TOP - 1 : end - 1, :]) * 0.5)
    fixed[2] = scale * ((bed_plus - bed_minus) * 0.5)
    strip_force = []
    for side, (bed_here, mask_here) in enumerate(zip(sides(BED), sides(MASK))):
        shifted[side, TOP:end, :] = bed_here
        down = shifted[side, TOP + 1 : end + 1, :] - shifted[side, TOP - 1 : end - 1, :]
        flat = pltpu.roll(bed_here, cols - 1, 1) - pltpu.roll(bed_here, 1, 1)
        scale = -(mask_here * thickness)
        fixed[3 + side] = mask_here
        fixed[5 + side] = scale * (down * 0.5)
        fixed[7 + side] = scale * (flat * 0.5)

    def power(strain4):
        return jnp.exp(jnp.log(strain4 * 0.25 + 0.1) * (-1.0 / 6.0))

    def strain4_of(ui, vi, uj, vj, uz, vz):
        shear = uj + vi
        return ui * ui + vj * vj + ui * vj + 0.25 * (shear * shear + (uz * uz + vz * vz))

    def strip_k(pair, comp, slot):
        result = []
        for side, value in enumerate(pair):
            value = value + along_y[comp] * (
                pltpu.roll(value, cols - 1, 1) + pltpu.roll(value, 1, 1)
            )
            value = value + along_z * (
                pltpu.roll(value, cols - PITCH, 1) + pltpu.roll(value, PITCH, 1)
            )
            shifted[slot + side, TOP:end, :] = value
            result.append(
                value
                + along_x[comp]
                * (
                    shifted[slot + side, TOP + 1 : end + 1, :]
                    + shifted[slot + side, TOP - 1 : end - 1, :]
                )
            )
        return result

    own_top = lax.broadcasted_iota(jnp.int32, (8, cols), 0) >= HALO

    def own_sum(value):
        total = jnp.where(own_top, value[:8], value[wide - 8 :])
        for low in range(8, wide - 8, 8):
            total = total + value[low : low + 8]
        return total

    def sample(member, carry):
        base = member * comps
        for comp in range(comps):
            pair = sides(base + comp)
            edge[EDGE_U + comp] = edges(pair)
            for side in range(2):
                strip[comp * 2 + side, TOP:end, :] = pair[side]
        strip_roots = []
        strip_diag = []
        friction_pair = sides(FRICTION + member)
        for side in range(2):
            value = [strip[comp * 2 + side, TOP:end, :] for comp in range(comps)]
            step_i = [
                strip[comp * 2 + side, TOP + 1 : end + 1, :]
                - strip[comp * 2 + side, TOP - 1 : end - 1, :]
                for comp in range(comps)
            ]
            step_j = [pltpu.roll(v, cols - 1, 1) - pltpu.roll(v, 1, 1) for v in value]
            step_z = [pltpu.roll(v, cols - PITCH, 1) - pltpu.roll(v, PITCH, 1) for v in value]
            here = fixed[3 + side]
            strip_roots.append(
                here
                * power(
                    strain4_of(
                        step_i[0], step_i[1], step_j[0], step_j[1], step_z[0], step_z[1]
                    )
                )
            )
            strip_diag.append(here * friction_pair[side] + (1.0 - here))
        edge[EDGE_R] = edges(strip_roots)
        for comp in range(comps):
            around_roots = strip_k(strip_roots, comp, comp * 2)
            start = [
                fixed[3 + side] * strip[comp * 2 + side, TOP:end, :] for side in range(2)
            ]
            field = [strip_roots[side] * start[side] for side in range(2)]
            edge[EDGE_0 + comp] = edges(field)
            near = strip_k(field, comp, comp * 2)
            four = [4.0 * strip_roots[side] for side in range(2)]
            main = [
                four[side] * around_roots[side] + strip_diag[side] for side in range(2)
            ]
            residual = [
                fixed[5 + 2 * comp + side]
                - (main[side] * start[side] - four[side] * near[side])
                for side in range(2)
            ]
            field = [strip_roots[side] * residual[side] for side in range(2)]
            edge[EDGE_1 + comp] = edges(field)
            near = strip_k(field, comp, comp * 2)
            image = [
                main[side] * residual[side] - four[side] * near[side] for side in range(2)
            ]
            edge[EDGE_2 + comp] = edges([strip_roots[side] * image[side] for side in range(2)])

        def roots_and_start(layer, carry):
            here = fixed[0]
            value = [uw[member, comp, layer + 1, TOP:end, :] for comp in range(comps)]
            step_i = [
                uw[member, comp, layer + 1, TOP + 1 : end + 1, :]
                - uw[member, comp, layer + 1, TOP - 1 : end - 1, :]
                for comp in range(comps)
            ]
            step_j = []
            for comp in range(comps):
                plus, minus = y_pair(value[comp], turned_edge(edge[EDGE_U + comp], layer))
                step_j.append(plus - minus)
            step_z = [
                uw[member, comp, layer + 2, TOP:end, :] - uw[member, comp, layer, TOP:end, :]
                for comp in range(comps)
            ]
            root = here * power(
                strain4_of(step_i[0], step_i[1], step_j[0], step_j[1], step_z[0], step_z[1])
            )
            roots[layer] = root
            plus, minus = y_pair(root, turned_edge(edge[EDGE_R], layer))
            both = plus + minus
            for comp in range(comps):
                tr[comp, layer + 1, TOP:end, :] = root + along_y[comp] * both
                field = root * (here * value[comp])
                plus, minus = y_pair(field, turned_edge(edge[EDGE_0 + comp], layer))
                tp[comp, layer + 1, TOP:end, :] = field + along_y[comp] * (plus + minus)
            return carry

        def x_sum(buffer, comp, layer):
            return buffer[comp, layer, TOP:end, :] + along_x[comp] * (
                buffer[comp, layer, TOP + 1 : end + 1, :]
                + buffer[comp, layer, TOP - 1 : end - 1, :]
            )

        lax.fori_loop(0, layers, roots_and_start, 0, unroll=UNROLL)
        slot = members * ens + member
        empty = jnp.zeros((wide, cols), jnp.float32)

        def residual_layer(layer, carry):
            before, now, total = carry
            root = roots[layer]
            four = 4.0 * root
            here = fixed[0]
            bottom = jnp.where(layer == 0, 1.0, 0.0)
            diag = here * mw[2 + member, TOP:end, :] * bottom + (1.0 - here)
            after = []
            for comp in range(comps):
                after_r = x_sum(tr, comp, layer + 2)
                after_p = x_sum(tp, comp, layer + 2)
                after += [after_r, after_p]
                around_roots = now[2 * comp] + along_z * (before[2 * comp] + after_r)
                near = now[2 * comp + 1] + along_z * (before[2 * comp + 1] + after_p)
                main = four * around_roots + diag
                start = here * uw[member, comp, layer + 1, TOP:end, :]
                residual = fixed[1 + comp] - (main * start - four * near)
                field_a[comp, layer] = main
                all_residual[slot, comp, layer] = residual
                total = total + own_sum(residual * residual)
                field = root * residual
                plus, minus = y_pair(field, turned_edge(edge[EDGE_1 + comp], layer))
                tq[comp, layer + 1, TOP:end, :] = field + along_y[comp] * (plus + minus)
            return tuple(now), tuple(after), total

        nothing = jnp.zeros((8, cols), jnp.float32)
        first = tuple(
            x_sum(buffer, comp, 1) for comp in range(comps) for buffer in (tr, tp)
        )
        _, _, gram_rr = lax.fori_loop(
            0, layers, residual_layer, ((empty,) * 4, first, nothing), unroll=UNROLL
        )

        def image_layer(layer, carry):
            before, now, total_ra, total_aa = carry
            root = roots[layer]
            four = 4.0 * root
            after = []
            for comp in range(comps):
                after_p = x_sum(tq, comp, layer + 2)
                after.append(after_p)
                near = now[comp] + along_z * (before[comp] + after_p)
                residual = all_residual[slot, comp, layer]
                image = field_a[comp, layer] * residual - four * near
                all_image[slot, comp, layer] = image
                total_ra = total_ra + own_sum(residual * image)
                total_aa = total_aa + own_sum(image * image)
                field = root * image
                plus, minus = y_pair(field, turned_edge(edge[EDGE_2 + comp], layer))
                tp[comp, layer + 1, TOP:end, :] = field + along_y[comp] * (plus + minus)
            return tuple(now), tuple(after), total_ra, total_aa

        first = tuple(x_sum(tq, comp, 1) for comp in range(comps))
        _, _, gram_ra, gram_aa = lax.fori_loop(
            0,
            layers,
            image_layer,
            ((empty,) * 2, first, nothing, nothing),
            unroll=UNROLL,
        )

        def own_x_sum(comp, layer):
            return tp[comp, layer, OWN : OWN + rows, :] + along_x[comp] * (
                tp[comp, layer, OWN + 1 : OWN + rows + 1, :]
                + tp[comp, layer, OWN - 1 : OWN + rows - 1, :]
            )

        def second_layer(layer, carry):
            before, now, total = carry
            four = 4.0 * roots[layer, HALO : HALO + rows, :]
            after = []
            for comp in range(comps):
                after_p = own_x_sum(comp, layer + 2)
                after.append(after_p)
                near = now[comp] + along_z * (before[comp] + after_p)
                image = all_image[slot, comp, layer, HALO : HALO + rows, :]
                second = (
                    field_a[comp, layer, HALO : HALO + rows, :] * image - four * near
                )
                product = image * second
                for low in range(0, rows, 8):
                    total = total + product[low : low + 8]
            return tuple(now), tuple(after), total

        empty_own = jnp.zeros((rows, cols), jnp.float32)
        first = tuple(own_x_sum(comp, 1) for comp in range(comps))
        _, _, gram_ab = lax.fori_loop(
            0, layers, second_layer, ((empty_own,) * 2, first, nothing), unroll=UNROLL
        )
        for number, value in enumerate((gram_rr, gram_ra, gram_aa, gram_ab)):
            gram[4 * member + number] = value
        return carry

    greeted_round(2)
    greet_round(4)
    lax.fori_loop(0, members, sample, 0)
    for reach in (4, 8, 16):
        greeted_round(reach)
        if reach > 2:
            greet_round(2 * reach)
    pl.semaphore_signal(
        hand_sem.at[len(hands)], inc=1, device_id=partner, device_id_type=MESH
    )

    lines = 4 * members
    total = jnp.sum(gram[...], axis=1)
    total = jnp.sum(total, axis=1, keepdims=True)
    lane = lax.broadcasted_iota(jnp.int32, (lines, cols), 1)
    line = lax.broadcasted_iota(jnp.int32, (lines, cols), 0)
    message = jnp.sum(
        jnp.where(lane == line + lines * ens, total, 0.0), axis=0, keepdims=True
    )
    pl.semaphore_wait(hand_sem.at[len(hands)], 1)

    def exchange(ring, me, count, target, send_sem, recv_sem, value):
        ring[me] = value
        copies = []
        for offset in range(1, count):
            copy = pltpu.make_async_remote_copy(
                src_ref=ring.at[me],
                dst_ref=ring.at[me],
                send_sem=send_sem.at[offset],
                recv_sem=recv_sem.at[offset],
                device_id=target(lax.rem(me + offset, count)),
                device_id_type=MESH,
            )
            copy.start()
            copies.append(copy)
        return copies

    cores = 2
    copies_y = exchange(
        ring_y,
        planey * cores + ens,
        planeys * cores,
        lambda peer: {"planey": peer // cores, "ens": lax.rem(peer, cores)},
        y_send,
        y_recv,
        message,
    )

    mine = pl.ds(members * ens, members)
    inner = pl.ds(HALO, rows)
    fields = []
    for comp in range(comps):
        for layer in range(layers):
            total = None
            for member in range(members):
                start = mw[1, OWN : OWN + rows, :] * uw[member, comp, layer + 1, OWN : OWN + rows, :]
                total = start if total is None else total + start
            all_start[ens, comp, layer] = total
    for number, (source, target) in enumerate(
        (
            (all_residual.at[mine, :, :, inner, :],) * 2,
            (all_image.at[mine, :, :, inner, :],) * 2,
            (all_start.at[ens],) * 2,
        )
    ):
        copy = pltpu.make_async_remote_copy(
            src_ref=source,
            dst_ref=target,
            send_sem=pair_send.at[number],
            recv_sem=pair_recv.at[number],
            device_id=partner,
            device_id_type=MESH,
        )
        copy.start()
        fields.append(copy)

    for copy in copies_y:
        copy.wait_recv()
    copies_x = exchange(
        ring_x,
        plane,
        planes,
        lambda peer: {"plane": peer},
        x_send,
        x_recv,
        jnp.sum(ring_y[...], axis=0),
    )
    for copy in fields:
        copy.wait_recv()
    for copy in copies_x:
        copy.wait_recv()
    sums = jnp.sum(ring_x[...], axis=0)
    gram_rr = sums
    gram_ra = pltpu.roll(sums, cols - 1, 1)
    gram_aa = pltpu.roll(sums, cols - 2, 1)
    gram_ab = pltpu.roll(sums, cols - 3, 1)
    first_step = gram_rr / gram_ra
    norm_next = gram_rr - 2.0 * first_step * gram_ra + first_step * first_step * gram_aa
    growth = 1.0 + norm_next / gram_rr
    curve = (
        growth * growth * gram_ra
        - 2.0 * growth * first_step * gram_aa
        + first_step * first_step * gram_ab
    )
    second_step = norm_next / curve
    samples = members * cores
    share = 1.0 / samples
    for_residual = share * (first_step + second_step * growth)
    for_image = share * (second_step * first_step)
    lane = lax.broadcasted_iota(jnp.int32, (1, cols), 1)

    def pick(value, number):
        return jnp.sum(jnp.where(lane == 4 * number, value, 0.0), axis=1, keepdims=True)

    weights = [(pick(for_residual, k), pick(for_image, k)) for k in range(samples)]

    def combine(layer, carry):
        for comp in range(comps):
            total = share * (all_start[0, comp, layer] + all_start[1, comp, layer])
            for number in range(samples):
                total = total + (
                    weights[number][0] * all_residual[number, comp, layer, HALO : HALO + rows, :]
                    - weights[number][1] * all_image[number, comp, layer, HALO : HALO + rows, :]
                )
            out[comp, layer] = total
        return carry

    lax.fori_loop(0, layers, combine, 0, unroll=UNROLL)

    for copy, sent, arrives in sends:

        @pl.when(sent)
        def _():
            copy.wait_send()

    for copy in copies_y + fields + copies_x:
        copy.wait_send()


UNROLL = 2


def body(sizes, u_prior, friction_rows, friction_table, bed_fixed, ice_mask):
    planes, planeys = sizes
    members, comps, layers, rows, cols = u_prior.shape
    wide = rows + 2 * HALO
    deep = rows + 24
    samples = 2 * members
    f32 = jnp.float32
    anywhere = pl.BlockSpec(memory_space=pl.ANY)
    fields = FRICTION + members
    vmem = pltpu.VMEM
    dma = pltpu.SemaphoreType.DMA
    return pl.pallas_call(
        functools.partial(kernel, sizes),
        out_shape=jax.ShapeDtypeStruct((comps, layers, rows, cols), f32),
        in_specs=[
            anywhere,
            pl.BlockSpec(memory_space=pltpu.SMEM),
            anywhere,
            anywhere,
            anywhere,
        ],
        out_specs=pl.BlockSpec(memory_space=pltpu.VMEM),
        scratch_shapes=[
            vmem((members, comps, layers + 2, deep, cols), f32),
            vmem((2 + members, deep, cols), f32),
            vmem((fields, deep, cols), f32),
            vmem((fields, deep, cols), f32),
            vmem((fields, deep, cols), f32),
            vmem(friction_table.shape, f32),
            vmem((rows, cols), jnp.int32),
            vmem((rows, cols), jnp.int32),
            vmem((2 * comps, deep, cols), f32),
            vmem((2 * comps, deep, cols), f32),
            vmem((9, wide, cols), f32),
            vmem((9, wide, cols), f32),
            vmem((layers, wide, cols), f32),
            vmem((comps, layers + 2, deep, cols), f32),
            vmem((comps, layers + 2, deep, cols), f32),
            vmem((comps, layers + 2, deep, cols), f32),
            vmem((comps, layers, wide, cols), f32),
            vmem((samples, comps, layers, wide, cols), f32),
            vmem((samples, comps, layers, wide, cols), f32),
            vmem((2, comps, layers, rows, cols), f32),
            vmem((4 * members, 8, cols), f32),
            vmem((2 * planeys, 1, cols), f32),
            vmem((planes, 1, cols), f32),
            dma((4,)),
            dma((12,)),
            dma((12,)),
            pltpu.SemaphoreType.REGULAR((8,)),
            dma((3,)),
            dma((3,)),
            dma((2 * planeys,)),
            dma((2 * planeys,)),
            dma((planes,)),
            dma((planes,)),
        ],
        compiler_params=pltpu.CompilerParams(
            collective_id=0, has_side_effects=True, vmem_limit_bytes=48 * 1024 * 1024
        ),
    )(u_prior, friction_rows, friction_table, bed_fixed, ice_mask)


def solution(mesh):
    in_specs = (
        P(("group", "ens"), None, None, "plane", "planey"),
        P(("group", "ens")),
        P("group", "plane", "planey"),
        P("plane", "planey"),
        P("plane", "planey"),
    )
    out_specs = P("group", None, "plane", "planey")
    sizes = (mesh.shape["plane"], mesh.shape["planey"])
    return jax.shard_map(
        functools.partial(body, sizes),
        mesh=mesh,
        in_specs=in_specs,
        out_specs=out_specs,
        check_vma=False,
    )
```

```python
import contextlib
import functools

import jax
import jax.numpy as jnp
from jax import lax
from jax.experimental import pallas as pl
from jax.experimental.pallas import tpu as pltpu
from jax.sharding import PartitionSpec as P

bed_unit = 2.0 ** (-29)
HALO = 4
TOP = 8
OWN = TOP + HALO
PITCH = 8
MESH = pl.DeviceIdType.MESH
along_z = 0.5
along_x = (0.25, 0.125)
along_y = (0.125, 0.25)
BED, MASK, FRICTION = 4, 5, 6
UNROLL = 10


def scope(name):
    return contextlib.nullcontext()


EDGE_U, EDGE_R, EDGE_0, EDGE_1, EDGE_2 = 0, 2, 3, 5, 7


def kernel(
    sizes,
    u_hbm,
    picks_hbm,
    table_hbm,
    bed_hbm,
    mask_hbm,
    out,
    uw,
    mw,
    xo,
    xl,
    xr,
    table,
    bed_in,
    mask_in,
    picks,
    strip,
    shifted,
    edge,
    fixed,
    roots,
    tr,
    tp,
    tq,
    field_a,
    all_residual,
    all_image,
    all_start,
    gram,
    ring_y,
    ring_x,
    local_sem,
    halo_send,
    halo_recv,
    hand_sem,
    pair_send,
    pair_recv,
    y_send,
    y_recv,
    x_send,
    x_recv,
):
    planes, planeys = sizes
    members, comps, layers, rows, cols = u_hbm.shape
    wide = rows + 2 * HALO
    end = TOP + wide
    plane = lax.axis_index("plane")
    planey = lax.axis_index("planey")
    ens = lax.axis_index("ens")

    def at(dx, dy):
        return {
            "plane": lax.rem(plane + dx + planes, planes),
            "planey": lax.rem(planey + dy + planeys, planeys),
        }

    partner = {"ens": 1 - ens}
    around = [(dx, dy) for dx in (-1, 0, 1) for dy in (-1, 0, 1) if (dx, dy) != (0, 0)]

    def exists(dx, dy):
        flag = None
        for step, index, count in ((dx, plane, planes), (dy, planey, planeys)):
            if step != 0:
                part = index > 0 if step < 0 else index < count - 1
                flag = part if flag is None else jnp.logical_and(flag, part)
        return flag

    barrier = pltpu.get_barrier_semaphore()
    for dx, dy in around:
        pl.semaphore_signal(barrier, inc=1, device_id=at(dx, dy), device_id_type=MESH)
    pl.semaphore_signal(barrier, inc=1, device_id=partner, device_id_type=MESH)

    load_u = pltpu.make_async_copy(
        u_hbm, uw.at[:, :, pl.ds(1, layers), pl.ds(OWN, rows), :], local_sem.at[0]
    )
    load_table = pltpu.make_async_copy(table_hbm, table, local_sem.at[1])
    load_bed = pltpu.make_async_copy(bed_hbm, bed_in, local_sem.at[2])
    load_mask = pltpu.make_async_copy(mask_hbm, mask_in, local_sem.at[3])
    load_picks = pltpu.make_async_copy(picks_hbm, picks, local_sem.at[4])
    for load in (load_u, load_bed, load_mask, load_picks, load_table):
        load.start()

    for end_layer in (0, layers + 1):
        uw[:, :, end_layer, TOP:end, :] = jnp.zeros((members, comps, wide, cols), jnp.float32)
        for buffer in (tr, tp, tq):
            buffer[:, end_layer] = jnp.zeros(buffer.shape[:1] + buffer.shape[2:], jnp.float32)
    for step, first in ((-1, TOP), (1, OWN + rows)):

        @pl.when(jnp.logical_not(exists(step, 0)))
        def _():
            uw[:, :, 1 : 1 + layers, first : first + HALO, :] = jnp.zeros(
                (members, comps, layers, HALO, cols), jnp.float32
            )
            for buffer in (mw, xo, xl, xr):
                buffer[:, first : first + HALO, :] = jnp.zeros(
                    (buffer.shape[0], HALO, cols), jnp.float32
                )

    for step, buffer in ((-1, xl), (1, xr)):

        @pl.when(jnp.logical_not(exists(0, step)))
        def _():
            buffer[:, TOP:end, :] = jnp.zeros((buffer.shape[0], wide, cols), jnp.float32)

    sends = []

    def send(number, dx, dy, source, target):
        copy = pltpu.make_async_remote_copy(
            src_ref=source,
            dst_ref=target,
            send_sem=halo_send.at[number],
            recv_sem=halo_recv.at[number],
            device_id=at(dx, dy),
            device_id_type=MESH,
        )

        @pl.when(exists(dx, dy))
        def _():
            copy.start()

        sends.append((copy, exists(dx, dy), exists(-dx, -dy)))

    def row_range(dx):
        if dx < 0:
            return pl.ds(OWN, HALO), pl.ds(OWN + rows, HALO)
        if dx > 0:
            return pl.ds(OWN + rows - HALO, HALO), pl.ds(TOP, HALO)
        return pl.ds(OWN, rows), pl.ds(OWN, rows)

    hands = []
    for axis, count in (("plane", planes), ("planey", planeys)):
        reach = 1
        while reach * 2 <= count // 2:
            hands.append((reach, axis))
            reach *= 2
    hands.sort()

    def greet(number):
        reach, axis = hands[number]
        for step in (-reach, reach):
            target = at(step, 0) if axis == "plane" else at(0, step)
            pl.semaphore_signal(
                hand_sem.at[number], inc=1, device_id=target, device_id_type=MESH
            )

    def greeted(number):
        pl.semaphore_wait(hand_sem.at[number], 2)

    def greet_round(reach):
        for number, (distance, _) in enumerate(hands):
            if distance == reach:
                greet(number)

    def greeted_round(reach):
        for number, (distance, _) in enumerate(hands):
            if distance == reach:
                greeted(number)

    with scope("p0_load"):
        load_u.wait()
        load_bed.wait()
        load_mask.wait()
        load_picks.wait()
        load_table.wait()
    lane = lax.broadcasted_iota(jnp.int32, (rows, cols), 1)
    group = lane // PITCH
    bed_own = bed_in[...].astype(jnp.float32) * bed_unit
    mask_own = mask_in[...].astype(jnp.float32)
    mw[0, OWN : OWN + rows, :] = bed_own
    mw[1, OWN : OWN + rows, :] = mask_own
    for member in range(members):
        chosen = table[picks[member]]
        mw[2 + member, OWN : OWN + rows, :] = chosen
        xo[FRICTION + member, OWN : OWN + rows, :] = jnp.where(
            lane < PITCH, pltpu.roll(chosen, HALO, 1), 0.0
        )

    def lane_packed(planes_of):
        packed = jnp.zeros((rows, cols), jnp.float32)
        for layer in range(layers):
            turned = pltpu.roll(planes_of(layer), (PITCH * layer + HALO) % cols, 1)
            packed = jnp.where(group == layer, turned, packed)
        return packed

    xo[BED, OWN : OWN + rows, :] = lane_packed(lambda layer: bed_own)
    xo[MASK, OWN : OWN + rows, :] = lane_packed(lambda layer: mask_own)
    for member in range(members):
        for comp in range(comps):
            xo[member * comps + comp, OWN : OWN + rows, :] = lane_packed(
                lambda layer: uw[member, comp, 1 + layer, OWN : OWN + rows, :]
            )

    with scope("p1_barrier"):
        pl.semaphore_wait(barrier, len(around) + 1)
    body = pl.ds(1, layers)
    for dx in (-1, 1):
        here, there = row_range(dx)
        send(
            0 if dx < 0 else 1,
            dx,
            0,
            uw.at[:, :, body, here, :],
            uw.at[:, :, body, there, :],
        )
    greet_round(1)
    for number, (dx, dy) in enumerate(around):
        here, there = row_range(dx)
        target = xo if dy == 0 else (xr if dy < 0 else xl)
        send(4 + number, dx, dy, xo.at[:, here, :], target.at[:, there, :])
    for dx in (-1, 1):
        here, there = row_range(dx)
        send(2 if dx < 0 else 3, dx, 0, mw.at[:, here, :], mw.at[:, there, :])

    with scope("p3_greeted1"):
        greeted_round(1)
    greet_round(2)

    with scope("p4_halo"):
        for copy, sent, arrives in sends:

            @pl.when(arrives)
            def _():
                copy.wait_recv()

    lane = lax.broadcasted_iota(jnp.int32, (wide, cols), 1)
    first_lane = lane == 0
    last_lane = lane == cols - 1
    spot = lax.rem(lane, PITCH)
    outer_left = spot < HALO
    left_edge = spot == HALO - 1
    position = (
        plane * rows - HALO + lax.broadcasted_iota(jnp.int32, (wide, cols), 0)
    ).astype(jnp.float32)
    thickness = 1.0 + 2.0 * position / (rows * planes - 1)

    def sides(number, low=TOP, high=end):
        own = xo[number, low:high, :]
        return (
            jnp.where(outer_left, xl[number, low:high, :], own),
            jnp.where(outer_left, own, xr[number, low:high, :]),
        )

    def edges(pair):
        left, right = pair
        return jnp.where(
            left_edge, pltpu.roll(right, cols - 1, 1), pltpu.roll(left, 1, 1)
        )

    def y_pair(value, near):
        return (
            jnp.where(last_lane, near, pltpu.roll(value, cols - 1, 1)),
            jnp.where(first_lane, near, pltpu.roll(value, 1, 1)),
        )

    def turned_edge(value, layer):
        return pltpu.roll(value, cols - HALO - PITCH * layer, 1)

    mask_main = mw[1, TOP:end, :]
    bed_plus, bed_minus = y_pair(mw[0, TOP:end, :], turned_edge(edges(sides(BED)), 0))
    scale = -(mask_main * thickness)
    fixed[0] = mask_main
    fixed[1] = scale * ((mw[0, TOP + 1 : end + 1, :] - mw[0, TOP - 1 : end - 1, :]) * 0.5)
    fixed[2] = scale * ((bed_plus - bed_minus) * 0.5)
    strip_force = []
    for side, (bed_here, mask_here) in enumerate(zip(sides(BED), sides(MASK))):
        shifted[side, TOP:end, :] = bed_here
        down = shifted[side, TOP + 1 : end + 1, :] - shifted[side, TOP - 1 : end - 1, :]
        flat = pltpu.roll(bed_here, cols - 1, 1) - pltpu.roll(bed_here, 1, 1)
        scale = -(mask_here * thickness)
        fixed[3 + side] = mask_here
        fixed[5 + side] = scale * (down * 0.5)
        fixed[7 + side] = scale * (flat * 0.5)

    def power(strain4):
        return jnp.exp(jnp.log(strain4 * 0.25 + 0.1) * (-1.0 / 6.0))

    def strain4_of(ui, vi, uj, vj, uz, vz):
        shear = uj + vi
        return ui * ui + vj * vj + ui * vj + 0.25 * (shear * shear + (uz * uz + vz * vz))

    def strip_k(pair, comp, slot):
        result = []
        for side, value in enumerate(pair):
            value = value + along_y[comp] * (
                pltpu.roll(value, cols - 1, 1) + pltpu.roll(value, 1, 1)
            )
            value = value + along_z * (
                pltpu.roll(value, cols - PITCH, 1) + pltpu.roll(value, PITCH, 1)
            )
            shifted[slot + side, TOP:end, :] = value
            result.append(
                value
                + along_x[comp]
                * (
                    shifted[slot + side, TOP + 1 : end + 1, :]
                    + shifted[slot + side, TOP - 1 : end - 1, :]
                )
            )
        return result

    own_top = lax.broadcasted_iota(jnp.int32, (8, cols), 0) >= HALO

    def own_sum(value):
        total = jnp.where(own_top, value[:8], value[wide - 8 :])
        for low in range(8, wide - 8, 8):
            total = total + value[low : low + 8]
        return total

    def sample(member, carry):
        base = member * comps
        for comp in range(comps):
            pair = sides(base + comp)
            edge[EDGE_U + comp] = edges(pair)
            for side in range(2):
                strip[comp * 2 + side, TOP:end, :] = pair[side]
        strip_roots = []
        strip_diag = []
        friction_pair = sides(FRICTION + member)
        for side in range(2):
            value = [strip[comp * 2 + side, TOP:end, :] for comp in range(comps)]
            step_i = [
                strip[comp * 2 + side, TOP + 1 : end + 1, :]
                - strip[comp * 2 + side, TOP - 1 : end - 1, :]
                for comp in range(comps)
            ]
            step_j = [pltpu.roll(v, cols - 1, 1) - pltpu.roll(v, 1, 1) for v in value]
            step_z = [pltpu.roll(v, cols - PITCH, 1) - pltpu.roll(v, PITCH, 1) for v in value]
            here = fixed[3 + side]
            strip_roots.append(
                here
                * power(
                    strain4_of(
                        step_i[0], step_i[1], step_j[0], step_j[1], step_z[0], step_z[1]
                    )
                )
            )
            strip_diag.append(here * friction_pair[side] + (1.0 - here))
        edge[EDGE_R] = edges(strip_roots)
        for comp in range(comps):
            around_roots = strip_k(strip_roots, comp, comp * 2)
            start = [
                fixed[3 + side] * strip[comp * 2 + side, TOP:end, :] for side in range(2)
            ]
            field = [strip_roots[side] * start[side] for side in range(2)]
            edge[EDGE_0 + comp] = edges(field)
            near = strip_k(field, comp, comp * 2)
            four = [4.0 * strip_roots[side] for side in range(2)]
            main = [
                four[side] * around_roots[side] + strip_diag[side] for side in range(2)
            ]
            residual = [
                fixed[5 + 2 * comp + side]
                - (main[side] * start[side] - four[side] * near[side])
                for side in range(2)
            ]
            field = [strip_roots[side] * residual[side] for side in range(2)]
            edge[EDGE_1 + comp] = edges(field)
            near = strip_k(field, comp, comp * 2)
            image = [
                main[side] * residual[side] - four[side] * near[side] for side in range(2)
            ]
            edge[EDGE_2 + comp] = edges([strip_roots[side] * image[side] for side in range(2)])

        def roots_and_start(layer, carry):
            here = fixed[0]
            value = [uw[member, comp, layer + 1, TOP:end, :] for comp in range(comps)]
            step_i = [
                uw[member, comp, layer + 1, TOP + 1 : end + 1, :]
                - uw[member, comp, layer + 1, TOP - 1 : end - 1, :]
                for comp in range(comps)
            ]
            step_j = []
            for comp in range(comps):
                plus, minus = y_pair(value[comp], turned_edge(edge[EDGE_U + comp], layer))
                step_j.append(plus - minus)
            step_z = [
                uw[member, comp, layer + 2, TOP:end, :] - uw[member, comp, layer, TOP:end, :]
                for comp in range(comps)
            ]
            root = here * power(
                strain4_of(step_i[0], step_i[1], step_j[0], step_j[1], step_z[0], step_z[1])
            )
            roots[layer] = root
            plus, minus = y_pair(root, turned_edge(edge[EDGE_R], layer))
            both = plus + minus
            for comp in range(comps):
                tr[comp, layer + 1, TOP:end, :] = root + along_y[comp] * both
                field = root * (here * value[comp])
                plus, minus = y_pair(field, turned_edge(edge[EDGE_0 + comp], layer))
                tp[comp, layer + 1, TOP:end, :] = field + along_y[comp] * (plus + minus)
            return carry

        def x_sum(buffer, comp, layer):
            return buffer[comp, layer, TOP:end, :] + along_x[comp] * (
                buffer[comp, layer, TOP + 1 : end + 1, :]
                + buffer[comp, layer, TOP - 1 : end - 1, :]
            )

        with scope("q1_roots"):
            lax.fori_loop(0, layers, roots_and_start, 0, unroll=UNROLL)
        slot = members * ens + member
        empty = jnp.zeros((wide, cols), jnp.float32)

        def residual_layer(layer, carry):
            before, now, total = carry
            root = roots[layer]
            four = 4.0 * root
            here = fixed[0]
            bottom = jnp.where(layer == 0, 1.0, 0.0)
            diag = here * mw[2 + member, TOP:end, :] * bottom + (1.0 - here)
            after = []
            for comp in range(comps):
                after_r = x_sum(tr, comp, layer + 2)
                after_p = x_sum(tp, comp, layer + 2)
                after += [after_r, after_p]
                around_roots = now[2 * comp] + along_z * (before[2 * comp] + after_r)
                near = now[2 * comp + 1] + along_z * (before[2 * comp + 1] + after_p)
                main = four * around_roots + diag
                start = here * uw[member, comp, layer + 1, TOP:end, :]
                residual = fixed[1 + comp] - (main * start - four * near)
                field_a[comp, layer] = main
                all_residual[slot, comp, layer] = residual
                total = total + own_sum(residual * residual)
                field = root * residual
                plus, minus = y_pair(field, turned_edge(edge[EDGE_1 + comp], layer))
                tq[comp, layer + 1, TOP:end, :] = field + along_y[comp] * (plus + minus)
            return tuple(now), tuple(after), total

        nothing = jnp.zeros((8, cols), jnp.float32)
        first = tuple(
            x_sum(buffer, comp, 1) for comp in range(comps) for buffer in (tr, tp)
        )
        with scope("q2_residual"):
            _, _, gram_rr = lax.fori_loop(
                0, layers, residual_layer, ((empty,) * 4, first, nothing), unroll=UNROLL
            )

        def image_layer(layer, carry):
            before, now, total_ra, total_aa = carry
            root = roots[layer]
            four = 4.0 * root
            after = []
            for comp in range(comps):
                after_p = x_sum(tq, comp, layer + 2)
                after.append(after_p)
                near = now[comp] + along_z * (before[comp] + after_p)
                residual = all_residual[slot, comp, layer]
                image = field_a[comp, layer] * residual - four * near
                all_image[slot, comp, layer] = image
                total_ra = total_ra + own_sum(residual * image)
                total_aa = total_aa + own_sum(image * image)
                field = root * image
                plus, minus = y_pair(field, turned_edge(edge[EDGE_2 + comp], layer))
                tp[comp, layer + 1, TOP:end, :] = field + along_y[comp] * (plus + minus)
            return tuple(now), tuple(after), total_ra, total_aa

        first = tuple(x_sum(tq, comp, 1) for comp in range(comps))
        with scope("q3_image"):
            _, _, gram_ra, gram_aa = lax.fori_loop(
                0,
                layers,
                image_layer,
                ((empty,) * 2, first, nothing, nothing),
                unroll=UNROLL,
            )

        def own_x_sum(comp, layer):
            return tp[comp, layer, OWN : OWN + rows, :] + along_x[comp] * (
                tp[comp, layer, OWN + 1 : OWN + rows + 1, :]
                + tp[comp, layer, OWN - 1 : OWN + rows - 1, :]
            )

        def second_layer(layer, carry):
            before, now, total = carry
            four = 4.0 * roots[layer, HALO : HALO + rows, :]
            after = []
            for comp in range(comps):
                after_p = own_x_sum(comp, layer + 2)
                after.append(after_p)
                near = now[comp] + along_z * (before[comp] + after_p)
                image = all_image[slot, comp, layer, HALO : HALO + rows, :]
                second = (
                    field_a[comp, layer, HALO : HALO + rows, :] * image - four * near
                )
                product = image * second
                for low in range(0, rows, 8):
                    total = total + product[low : low + 8]
            return tuple(now), tuple(after), total

        empty_own = jnp.zeros((rows, cols), jnp.float32)
        first = tuple(own_x_sum(comp, 1) for comp in range(comps))
        with scope("q4_second"):
            _, _, gram_ab = lax.fori_loop(
                0, layers, second_layer, ((empty_own,) * 2, first, nothing), unroll=UNROLL
            )
        for number, value in enumerate((gram_rr, gram_ra, gram_aa, gram_ab)):
            gram[4 * member + number] = value
        return carry

    with scope("p5_greeted2"):
        greeted_round(2)
    greet_round(4)

    def one_sample(member, carry):
        sample(member, carry)

        @pl.when(member == 0)
        def _():
            with scope("p6_greeted4"):
                for reach in (4, 8, 16):
                    greeted_round(reach)
                    if reach > 2:
                        greet_round(2 * reach)
            pl.semaphore_signal(
                hand_sem.at[len(hands)], inc=1, device_id=partner, device_id_type=MESH
            )

        return carry

    with scope("p6_samples"):
        lax.fori_loop(0, members, one_sample, 0)

    lines = 4 * members
    total = jnp.sum(gram[...], axis=1)
    total = jnp.sum(total, axis=1, keepdims=True)
    lane = lax.broadcasted_iota(jnp.int32, (lines, cols), 1)
    line = lax.broadcasted_iota(jnp.int32, (lines, cols), 0)
    message = jnp.sum(
        jnp.where(lane == line + lines * ens, total, 0.0), axis=0, keepdims=True
    )
    with scope("p7_hand"):
        pl.semaphore_wait(hand_sem.at[len(hands)], 1)

    def exchange(ring, me, count, target, send_sem, recv_sem, value):
        ring[me] = value
        for offset in sorted(range(1, count), key=lambda k: -min(k, count - k)):
            pltpu.make_async_remote_copy(
                src_ref=ring.at[me],
                dst_ref=ring.at[me],
                send_sem=send_sem.at[0],
                recv_sem=recv_sem.at[0],
                device_id=target(lax.rem(me + offset, count)),
                device_id_type=MESH,
            ).start()
        return pltpu.make_async_remote_copy(
            src_ref=ring.at[pl.ds(0, count - 1)],
            dst_ref=ring.at[pl.ds(0, count - 1)],
            send_sem=send_sem.at[0],
            recv_sem=recv_sem.at[0],
            device_id=target(lax.rem(me + 1, count)),
            device_id_type=MESH,
        )

    cores = 2
    copies_y = exchange(
        ring_y,
        planey * cores + ens,
        planeys * cores,
        lambda peer: {"planey": peer // cores, "ens": lax.rem(peer, cores)},
        y_send,
        y_recv,
        message,
    )

    mine = pl.ds(members * ens, members)
    inner = pl.ds(HALO, rows)
    fields = []
    for comp in range(comps):
        for layer in range(layers):
            total = None
            for member in range(members):
                start = mw[1, OWN : OWN + rows, :] * uw[member, comp, layer + 1, OWN : OWN + rows, :]
                total = start if total is None else total + start
            all_start[ens, comp, layer] = total
    for number, (source, target) in enumerate(
        (
            (all_residual.at[mine, :, :, inner, :],) * 2,
            (all_image.at[mine, :, :, inner, :],) * 2,
            (all_start.at[ens],) * 2,
        )
    ):
        copy = pltpu.make_async_remote_copy(
            src_ref=source,
            dst_ref=target,
            send_sem=pair_send.at[number],
            recv_sem=pair_recv.at[number],
            device_id=partner,
            device_id_type=MESH,
        )
        copy.start()
        fields.append(copy)

    for copy, sent, arrives in sends:

        @pl.when(sent)
        def _():
            copy.wait_send()

    with scope("p8_ary"):
        copies_y.wait_recv()
    copies_x = exchange(
        ring_x,
        plane,
        planes,
        lambda peer: {"plane": peer},
        x_send,
        x_recv,
        jnp.sum(ring_y[...], axis=0),
    )
    for copy in fields:
        copy.wait_recv()
    for copy in fields + [copies_y]:
        copy.wait_send()
    with scope("p9_arx"):
        copies_x.wait_recv()
    sums = jnp.sum(ring_x[...], axis=0)
    gram_rr = sums
    gram_ra = pltpu.roll(sums, cols - 1, 1)
    gram_aa = pltpu.roll(sums, cols - 2, 1)
    gram_ab = pltpu.roll(sums, cols - 3, 1)
    first_step = gram_rr / gram_ra
    norm_next = gram_rr - 2.0 * first_step * gram_ra + first_step * first_step * gram_aa
    growth = 1.0 + norm_next / gram_rr
    curve = (
        growth * growth * gram_ra
        - 2.0 * growth * first_step * gram_aa
        + first_step * first_step * gram_ab
    )
    second_step = norm_next / curve
    samples = members * cores
    share = 1.0 / samples
    for_residual = share * (first_step + second_step * growth)
    for_image = share * (second_step * first_step)
    lane = lax.broadcasted_iota(jnp.int32, (1, cols), 1)

    def pick(value, number):
        return jnp.sum(jnp.where(lane == 4 * number, value, 0.0), axis=1, keepdims=True)

    weights = [(pick(for_residual, k), pick(for_image, k)) for k in range(samples)]

    def combine(layer, carry):
        for comp in range(comps):
            total = share * (all_start[0, comp, layer] + all_start[1, comp, layer])
            for number in range(samples):
                total = total + (
                    weights[number][0] * all_residual[number, comp, layer, HALO : HALO + rows, :]
                    - weights[number][1] * all_image[number, comp, layer, HALO : HALO + rows, :]
                )
            out[comp, layer] = total
        return carry

    with scope("pa_combine"):
        lax.fori_loop(0, layers, combine, 0, unroll=UNROLL)
    with scope("pb_sent"):
        copies_x.wait_send()


def body(sizes, u_prior, friction_rows, friction_table, bed_fixed, ice_mask):
    planes, planeys = sizes
    members, comps, layers, rows, cols = u_prior.shape
    wide = rows + 2 * HALO
    deep = rows + 24
    samples = 2 * members
    f32 = jnp.float32
    anywhere = pl.BlockSpec(memory_space=pltpu.HBM)
    fields = FRICTION + members
    vmem = pltpu.VMEM
    dma = pltpu.SemaphoreType.DMA
    return pl.pallas_call(
        functools.partial(kernel, sizes),
        out_shape=jax.ShapeDtypeStruct((comps, layers, rows, cols), f32),
        in_specs=[anywhere] * 5,
        out_specs=pl.BlockSpec(memory_space=pltpu.VMEM),
        scratch_shapes=[
            vmem((members, comps, layers + 2, deep, cols), f32),
            vmem((2 + members, deep, cols), f32),
            vmem((fields, deep, cols), f32),
            vmem((fields, deep, cols), f32),
            vmem((fields, deep, cols), f32),
            vmem(friction_table.shape, f32),
            vmem((rows, cols), jnp.int32),
            vmem((rows, cols), jnp.int32),
            pltpu.SMEM((members,), jnp.int32),
            vmem((2 * comps, deep, cols), f32),
            vmem((2 * comps, deep, cols), f32),
            vmem((9, wide, cols), f32),
            vmem((9, wide, cols), f32),
            vmem((layers, wide, cols), f32),
            vmem((comps, layers + 2, deep, cols), f32),
            vmem((comps, layers + 2, deep, cols), f32),
            vmem((comps, layers + 2, deep, cols), f32),
            vmem((comps, layers, wide, cols), f32),
            vmem((samples, comps, layers, wide, cols), f32),
            vmem((samples, comps, layers, wide, cols), f32),
            vmem((2, comps, layers, rows, cols), f32),
            vmem((4 * members, 8, cols), f32),
            vmem((2 * planeys, 1, cols), f32),
            vmem((planes, 1, cols), f32),
            dma((5,)),
            dma((12,)),
            dma((12,)),
            pltpu.SemaphoreType.REGULAR((8,)),
            dma((3,)),
            dma((3,)),
            dma((1,)),
            dma((1,)),
            dma((1,)),
            dma((1,)),
        ],
        compiler_params=pltpu.CompilerParams(
            collective_id=0, has_side_effects=True, vmem_limit_bytes=48 * 1024 * 1024
        ),
    )(*[
        pltpu.with_memory_space_constraint(x, pltpu.HBM)
        for x in (u_prior, friction_rows, friction_table, bed_fixed, ice_mask)
    ])


def solution(mesh):
    in_specs = (
        P(("group", "ens"), None, None, "plane", "planey"),
        P(("group", "ens")),
        P("group", "plane", "planey"),
        P("plane", "planey"),
        P("plane", "planey"),
    )
    out_specs = P("group", None, "plane", "planey")
    sizes = (mesh.shape["plane"], mesh.shape["planey"])
    return jax.shard_map(
        functools.partial(body, sizes),
        mesh=mesh,
        in_specs=in_specs,
        out_specs=out_specs,
        check_vma=False,
    )
```

```python
import contextlib
import functools

import jax
import jax.numpy as jnp
from jax import lax
from jax.experimental import pallas as pl
from jax.experimental.pallas import tpu as pltpu
from jax.sharding import PartitionSpec as P

bed_unit = 2.0 ** (-29)
HALO = 4
TOP = 8
OWN = TOP + HALO
PITCH = 8
MESH = pl.DeviceIdType.MESH
along_z = 0.5
along_x = (0.25, 0.125)
along_y = (0.125, 0.25)
BED, MASK = 0, 1
UNROLL = 10


def scope(name):
    return contextlib.nullcontext()


EDGE_U, EDGE_R, EDGE_0, EDGE_1, EDGE_2 = 0, 2, 3, 5, 7


def kernel(
    sizes,
    u_hbm,
    picks_hbm,
    table_hbm,
    bed_hbm,
    mask_hbm,
    out,
    uw,
    mw,
    xo,
    xl,
    xr,
    table,
    bed_in,
    mask_in,
    picks,
    strip,
    shifted,
    edge,
    fixed,
    roots,
    step_y,
    tr,
    tp,
    tq,
    field_a,
    all_residual,
    all_image,
    all_start,
    gram,
    ring_y,
    ring_x,
    local_sem,
    halo_send,
    halo_recv,
    hand_sem,
    pair_send,
    pair_recv,
    y_send,
    y_recv,
    x_send,
    x_recv,
):
    planes, planeys = sizes
    members, comps, layers, rows, cols = u_hbm.shape
    wide = rows + 2 * HALO
    end = TOP + wide
    plane = lax.axis_index("plane")
    planey = lax.axis_index("planey")
    ens = lax.axis_index("ens")

    def at(dx, dy):
        return {
            "plane": lax.rem(plane + dx + planes, planes),
            "planey": lax.rem(planey + dy + planeys, planeys),
        }

    partner = {"ens": 1 - ens}
    around = [(dx, dy) for dx in (-1, 0, 1) for dy in (-1, 0, 1) if (dx, dy) != (0, 0)]

    def exists(dx, dy):
        flag = None
        for step, index, count in ((dx, plane, planes), (dy, planey, planeys)):
            if step != 0:
                part = index > 0 if step < 0 else index < count - 1
                flag = part if flag is None else jnp.logical_and(flag, part)
        return flag

    def load_member(member):
        return pltpu.make_async_copy(
            u_hbm.at[member],
            uw.at[member, :, pl.ds(1, layers), pl.ds(OWN, rows), :],
            local_sem.at[member],
        )

    load_u = [load_member(member) for member in range(members)]
    load_table = pltpu.make_async_copy(table_hbm, table, local_sem.at[members])
    load_bed = pltpu.make_async_copy(bed_hbm, bed_in, local_sem.at[members + 1])
    load_mask = pltpu.make_async_copy(mask_hbm, mask_in, local_sem.at[members + 2])
    load_picks = pltpu.make_async_copy(picks_hbm, picks, local_sem.at[members + 3])
    for load in (load_u[0], load_picks, load_table, load_bed, load_mask, *load_u[1:]):
        load.start()

    barrier = pltpu.get_barrier_semaphore()
    for dx, dy in around:
        pl.semaphore_signal(barrier, inc=1, device_id=at(dx, dy), device_id_type=MESH)
    pl.semaphore_signal(barrier, inc=1, device_id=partner, device_id_type=MESH)

    for end_layer in (0, layers + 1):
        uw[:, :, end_layer, TOP:end, :] = jnp.zeros((members, comps, wide, cols), jnp.float32)
        for buffer in (tr, tp, tq):
            buffer[:, end_layer] = jnp.zeros(buffer.shape[:1] + buffer.shape[2:], jnp.float32)
    for step, first in ((-1, TOP), (1, OWN + rows)):

        @pl.when(jnp.logical_not(exists(step, 0)))
        def _():
            uw[:, :, 1 : 1 + layers, first : first + HALO, :] = jnp.zeros(
                (members, comps, layers, HALO, cols), jnp.float32
            )
            for buffer in (mw, xo, xl, xr):
                buffer[:, first : first + HALO, :] = jnp.zeros(
                    (buffer.shape[0], HALO, cols), jnp.float32
                )

    for step, buffer in ((-1, xl), (1, xr)):

        @pl.when(jnp.logical_not(exists(0, step)))
        def _():
            buffer[:, TOP:end, :] = jnp.zeros((buffer.shape[0], wide, cols), jnp.float32)

    sends = [[] for _ in range(members)]

    def send(part, dx, dy, source, target):
        number = sum(len(group) for group in sends)
        copy = pltpu.make_async_remote_copy(
            src_ref=source,
            dst_ref=target,
            send_sem=halo_send.at[number],
            recv_sem=halo_recv.at[number],
            device_id=at(dx, dy),
            device_id_type=MESH,
        )

        @pl.when(exists(dx, dy))
        def _():
            copy.start()

        sends[part].append((copy, exists(dx, dy), exists(-dx, -dy)))

    def first_field(member):
        return 2 + member * (1 + comps)

    def row_range(dx):
        if dx < 0:
            return pl.ds(OWN, HALO), pl.ds(OWN + rows, HALO)
        if dx > 0:
            return pl.ds(OWN + rows - HALO, HALO), pl.ds(TOP, HALO)
        return pl.ds(OWN, rows), pl.ds(OWN, rows)

    hands = []
    for axis, count in (("plane", planes), ("planey", planeys)):
        reach = 1
        while reach * 2 <= count // 2:
            hands.append((reach, axis))
            reach *= 2
    hands.sort()

    def greet(number):
        reach, axis = hands[number]
        for step in (-reach, reach):
            target = at(step, 0) if axis == "plane" else at(0, step)
            pl.semaphore_signal(
                hand_sem.at[number], inc=1, device_id=target, device_id_type=MESH
            )

    def greeted(number):
        pl.semaphore_wait(hand_sem.at[number], 2)

    def greet_round(reach):
        for number, (distance, _) in enumerate(hands):
            if distance == reach:
                greet(number)

    def greeted_round(reach):
        for number, (distance, _) in enumerate(hands):
            if distance == reach:
                greeted(number)

    lane = lax.broadcasted_iota(jnp.int32, (rows, cols), 1)
    group = lane // PITCH

    def lane_packed(planes_of):
        packed = jnp.zeros((rows, cols), jnp.float32)
        for layer in range(layers):
            turned = pltpu.roll(planes_of(layer), (PITCH * layer + HALO) % cols, 1)
            packed = jnp.where(group == layer, turned, packed)
        return packed

    body = pl.ds(1, layers)
    for member in range(members):
        with scope("p0_load"):
            load_u[member].wait()
        if member == 0:
            with scope("p1_barrier"):
                pl.semaphore_wait(barrier, len(around) + 1)
        for dx in (-1, 1):
            here, there = row_range(dx)
            send(
                member,
                dx,
                0,
                uw.at[member, :, body, here, :],
                uw.at[member, :, body, there, :],
            )
        base = first_field(member)
        if member == 0:
            greet_round(1)
            load_bed.wait()
            load_mask.wait()
            load_picks.wait()
            load_table.wait()
            bed_own = bed_in[...].astype(jnp.float32) * bed_unit
            mask_own = mask_in[...].astype(jnp.float32)
            mw[0, OWN : OWN + rows, :] = bed_own
            mw[1, OWN : OWN + rows, :] = mask_own
            xo[BED, OWN : OWN + rows, :] = lane_packed(lambda layer: bed_own)
            xo[MASK, OWN : OWN + rows, :] = lane_packed(lambda layer: mask_own)
            for other in range(members):
                chosen = table[picks[other]]
                mw[2 + other, OWN : OWN + rows, :] = chosen
                xo[first_field(other), OWN : OWN + rows, :] = jnp.where(
                    lane < PITCH, pltpu.roll(chosen, HALO, 1), 0.0
                )
        for comp in range(comps):
            xo[base + 1 + comp, OWN : OWN + rows, :] = lane_packed(
                lambda layer: uw[member, comp, 1 + layer, OWN : OWN + rows, :]
            )
        low = 0 if member == 0 else base
        part = pl.ds(low, base + 1 + comps - low)
        for dx, dy in around:
            here, there = row_range(dx)
            target = xo if dy == 0 else (xr if dy < 0 else xl)
            send(member, dx, dy, xo.at[part, here, :], target.at[part, there, :])
        if member == 0:
            for dx in (-1, 1):
                here, there = row_range(dx)
                send(0, dx, 0, mw.at[:, here, :], mw.at[:, there, :])

    with scope("p3_greeted1"):
        greeted_round(1)
    greet_round(2)
    with scope("p5_greeted2"):
        greeted_round(2)
    greet_round(4)

    def arrived(member):
        with scope("p4_halo"):
            for copy, sent, arrives in sends[member]:

                @pl.when(arrives)
                def _():
                    copy.wait_recv()

    arrived(0)

    lane = lax.broadcasted_iota(jnp.int32, (wide, cols), 1)
    first_lane = lane == 0
    last_lane = lane == cols - 1
    spot = lax.rem(lane, PITCH)
    outer_left = spot < HALO
    left_edge = spot == HALO - 1
    position = (
        plane * rows - HALO + lax.broadcasted_iota(jnp.int32, (wide, cols), 0)
    ).astype(jnp.float32)
    thickness = 1.0 + 2.0 * position / (rows * planes - 1)

    def sides(number, low=TOP, high=end):
        own = xo[number, low:high, :]
        return (
            jnp.where(outer_left, xl[number, low:high, :], own),
            jnp.where(outer_left, own, xr[number, low:high, :]),
        )

    def edges(pair):
        left, right = pair
        return jnp.where(
            left_edge, pltpu.roll(right, cols - 1, 1), pltpu.roll(left, 1, 1)
        )

    def y_pair(value, near):
        return (
            jnp.where(last_lane, near, pltpu.roll(value, cols - 1, 1)),
            jnp.where(first_lane, near, pltpu.roll(value, 1, 1)),
        )

    def turned_edge(value, layer):
        return pltpu.roll(value, cols - HALO - PITCH * layer, 1)

    mask_main = mw[1, TOP:end, :]
    bed_plus, bed_minus = y_pair(mw[0, TOP:end, :], turned_edge(edges(sides(BED)), 0))
    scale = -(mask_main * thickness)
    fixed[0] = mask_main
    fixed[1] = scale * ((mw[0, TOP + 1 : end + 1, :] - mw[0, TOP - 1 : end - 1, :]) * 0.5)
    fixed[2] = scale * ((bed_plus - bed_minus) * 0.5)
    strip_force = []
    for side, (bed_here, mask_here) in enumerate(zip(sides(BED), sides(MASK))):
        shifted[side, TOP:end, :] = bed_here
        down = shifted[side, TOP + 1 : end + 1, :] - shifted[side, TOP - 1 : end - 1, :]
        flat = pltpu.roll(bed_here, cols - 1, 1) - pltpu.roll(bed_here, 1, 1)
        scale = -(mask_here * thickness)
        fixed[3 + side] = mask_here
        fixed[5 + side] = scale * (down * 0.5)
        fixed[7 + side] = scale * (flat * 0.5)

    def power(strain4):
        return jnp.exp(jnp.log(strain4 * 0.25 + 0.1) * (-1.0 / 6.0))

    def strain4_of(ui, vi, uj, vj, uz, vz):
        shear = uj + vi
        return ui * ui + vj * vj + ui * vj + 0.25 * (shear * shear + (uz * uz + vz * vz))

    def strip_k(pair, comp, slot):
        result = []
        for side, value in enumerate(pair):
            value = value + along_y[comp] * (
                pltpu.roll(value, cols - 1, 1) + pltpu.roll(value, 1, 1)
            )
            value = value + along_z * (
                pltpu.roll(value, cols - PITCH, 1) + pltpu.roll(value, PITCH, 1)
            )
            shifted[slot + side, TOP:end, :] = value
            result.append(
                value
                + along_x[comp]
                * (
                    shifted[slot + side, TOP + 1 : end + 1, :]
                    + shifted[slot + side, TOP - 1 : end - 1, :]
                )
            )
        return result

    own_top = lax.broadcasted_iota(jnp.int32, (8, cols), 0) >= HALO

    def own_sum(value):
        total = jnp.where(own_top, value[:8], value[wide - 8 :])
        for low in range(8, wide - 8, 8):
            total = total + value[low : low + 8]
        return total

    def sample(member):
        base = first_field(member)
        for comp in range(comps):
            pair = sides(base + 1 + comp)
            edge[EDGE_U + comp] = edges(pair)
            for side in range(2):
                strip[comp * 2 + side, TOP:end, :] = pair[side]
        strip_roots = []
        strip_diag = []
        friction_pair = sides(base)
        for side in range(2):
            value = [strip[comp * 2 + side, TOP:end, :] for comp in range(comps)]
            step_i = [
                strip[comp * 2 + side, TOP + 1 : end + 1, :]
                - strip[comp * 2 + side, TOP - 1 : end - 1, :]
                for comp in range(comps)
            ]
            step_j = [pltpu.roll(v, cols - 1, 1) - pltpu.roll(v, 1, 1) for v in value]
            step_z = [pltpu.roll(v, cols - PITCH, 1) - pltpu.roll(v, PITCH, 1) for v in value]
            here = fixed[3 + side]
            strip_roots.append(
                here
                * power(
                    strain4_of(
                        step_i[0], step_i[1], step_j[0], step_j[1], step_z[0], step_z[1]
                    )
                )
            )
            strip_diag.append(here * friction_pair[side] + (1.0 - here))
        edge[EDGE_R] = edges(strip_roots)
        for comp in range(comps):
            around_roots = strip_k(strip_roots, comp, comp * 2)
            start = [
                fixed[3 + side] * strip[comp * 2 + side, TOP:end, :] for side in range(2)
            ]
            field = [strip_roots[side] * start[side] for side in range(2)]
            edge[EDGE_0 + comp] = edges(field)
            near = strip_k(field, comp, comp * 2)
            four = [4.0 * strip_roots[side] for side in range(2)]
            main = [
                four[side] * around_roots[side] + strip_diag[side] for side in range(2)
            ]
            residual = [
                fixed[5 + 2 * comp + side]
                - (main[side] * start[side] - four[side] * near[side])
                for side in range(2)
            ]
            field = [strip_roots[side] * residual[side] for side in range(2)]
            edge[EDGE_1 + comp] = edges(field)
            near = strip_k(field, comp, comp * 2)
            image = [
                main[side] * residual[side] - four[side] * near[side] for side in range(2)
            ]
            edge[EDGE_2 + comp] = edges([strip_roots[side] * image[side] for side in range(2)])

        for comp in range(comps):
            for layer in range(layers):
                plus, minus = y_pair(
                    uw[member, comp, layer + 1, TOP:end, :],
                    turned_edge(edge[EDGE_U + comp], layer),
                )
                step_y[comp, layer] = plus - minus
        for layer in range(layers):
            step_i = [
                uw[member, comp, layer + 1, TOP + 1 : end + 1, :]
                - uw[member, comp, layer + 1, TOP - 1 : end - 1, :]
                for comp in range(comps)
            ]
            step_z = [
                uw[member, comp, layer + 2, TOP:end, :] - uw[member, comp, layer, TOP:end, :]
                for comp in range(comps)
            ]
            roots[layer] = fixed[0] * power(
                strain4_of(
                    step_i[0],
                    step_i[1],
                    step_y[0, layer],
                    step_y[1, layer],
                    step_z[0],
                    step_z[1],
                )
            )
        for layer in range(layers):
            root = roots[layer]
            plus, minus = y_pair(root, turned_edge(edge[EDGE_R], layer))
            both = plus + minus
            for comp in range(comps):
                tr[comp, layer + 1, TOP:end, :] = root + along_y[comp] * both
                field = root * (fixed[0] * uw[member, comp, layer + 1, TOP:end, :])
                plus, minus = y_pair(field, turned_edge(edge[EDGE_0 + comp], layer))
                tp[comp, layer + 1, TOP:end, :] = field + along_y[comp] * (plus + minus)

        def x_sum(buffer, comp, layer):
            return buffer[comp, layer, TOP:end, :] + along_x[comp] * (
                buffer[comp, layer, TOP + 1 : end + 1, :]
                + buffer[comp, layer, TOP - 1 : end - 1, :]
            )

        slot = members * ens + member
        empty = jnp.zeros((wide, cols), jnp.float32)

        def residual_layer(layer, carry):
            before, now, total = carry
            root = roots[layer]
            four = 4.0 * root
            here = fixed[0]
            bottom = jnp.where(layer == 0, 1.0, 0.0)
            diag = here * mw[2 + member, TOP:end, :] * bottom + (1.0 - here)
            after = []
            for comp in range(comps):
                after_r = x_sum(tr, comp, layer + 2)
                after_p = x_sum(tp, comp, layer + 2)
                after += [after_r, after_p]
                around_roots = now[2 * comp] + along_z * (before[2 * comp] + after_r)
                near = now[2 * comp + 1] + along_z * (before[2 * comp + 1] + after_p)
                main = four * around_roots + diag
                start = here * uw[member, comp, layer + 1, TOP:end, :]
                residual = fixed[1 + comp] - (main * start - four * near)
                field_a[comp, layer] = main
                all_residual[slot, comp, layer] = residual
                total = total + own_sum(residual * residual)
                field = root * residual
                plus, minus = y_pair(field, turned_edge(edge[EDGE_1 + comp], layer))
                tq[comp, layer + 1, TOP:end, :] = field + along_y[comp] * (plus + minus)
            return tuple(now), tuple(after), total

        nothing = jnp.zeros((8, cols), jnp.float32)
        first = tuple(
            x_sum(buffer, comp, 1) for comp in range(comps) for buffer in (tr, tp)
        )
        with scope("q2_residual"):
            _, _, gram_rr = lax.fori_loop(
                0, layers, residual_layer, ((empty,) * 4, first, nothing), unroll=UNROLL
            )

        def image_layer(layer, carry):
            before, now, total_ra, total_aa = carry
            root = roots[layer]
            four = 4.0 * root
            after = []
            for comp in range(comps):
                after_p = x_sum(tq, comp, layer + 2)
                after.append(after_p)
                near = now[comp] + along_z * (before[comp] + after_p)
                residual = all_residual[slot, comp, layer]
                image = field_a[comp, layer] * residual - four * near
                all_image[slot, comp, layer] = image
                total_ra = total_ra + own_sum(residual * image)
                total_aa = total_aa + own_sum(image * image)
                field = root * image
                plus, minus = y_pair(field, turned_edge(edge[EDGE_2 + comp], layer))
                tp[comp, layer + 1, TOP:end, :] = field + along_y[comp] * (plus + minus)
            return tuple(now), tuple(after), total_ra, total_aa

        first = tuple(x_sum(tq, comp, 1) for comp in range(comps))
        with scope("q3_image"):
            _, _, gram_ra, gram_aa = lax.fori_loop(
                0,
                layers,
                image_layer,
                ((empty,) * 2, first, nothing, nothing),
                unroll=UNROLL,
            )

        def own_x_sum(comp, layer):
            return tp[comp, layer, OWN : OWN + rows, :] + along_x[comp] * (
                tp[comp, layer, OWN + 1 : OWN + rows + 1, :]
                + tp[comp, layer, OWN - 1 : OWN + rows - 1, :]
            )

        def second_layer(layer, carry):
            before, now, total = carry
            four = 4.0 * roots[layer, HALO : HALO + rows, :]
            after = []
            for comp in range(comps):
                after_p = own_x_sum(comp, layer + 2)
                after.append(after_p)
                near = now[comp] + along_z * (before[comp] + after_p)
                image = all_image[slot, comp, layer, HALO : HALO + rows, :]
                second = (
                    field_a[comp, layer, HALO : HALO + rows, :] * image - four * near
                )
                product = image * second
                for low in range(0, rows, 8):
                    total = total + product[low : low + 8]
            return tuple(now), tuple(after), total

        empty_own = jnp.zeros((rows, cols), jnp.float32)
        first = tuple(own_x_sum(comp, 1) for comp in range(comps))
        with scope("q4_second"):
            _, _, gram_ab = lax.fori_loop(
                0, layers, second_layer, ((empty_own,) * 2, first, nothing), unroll=UNROLL
            )
        for number, value in enumerate((gram_rr, gram_ra, gram_aa, gram_ab)):
            gram[4 * member + number] = value

    def to_partner(number, source, target):
        copy = pltpu.make_async_remote_copy(
            src_ref=source,
            dst_ref=target,
            send_sem=pair_send.at[number],
            recv_sem=pair_recv.at[number],
            device_id=partner,
            device_id_type=MESH,
        )
        copy.start()
        fields.append(copy)

    fields = []
    inner = pl.ds(HALO, rows)

    def share_member(member):
        slot = members * ens + member
        for number, buffer in enumerate((all_residual, all_image)):
            block = buffer.at[slot, :, :, inner, :]
            to_partner(2 * member + number, block, block)

    for member in range(members):
        if member > 0:
            arrived(member)
        with scope("p6_sample"):
            sample(member)
        if member == 0:
            with scope("p6_greeted4"):
                for reach in (4, 8, 16):
                    greeted_round(reach)
                    if reach > 2:
                        greet_round(2 * reach)
            pl.semaphore_signal(
                hand_sem.at[len(hands)], inc=1, device_id=partner, device_id_type=MESH
            )
        if member < members - 1:
            share_member(member)

    lines = 4 * members
    total = jnp.sum(gram[...], axis=1)
    total = jnp.sum(total, axis=1, keepdims=True)
    lane = lax.broadcasted_iota(jnp.int32, (lines, cols), 1)
    line = lax.broadcasted_iota(jnp.int32, (lines, cols), 0)
    message = jnp.sum(
        jnp.where(lane == line + lines * ens, total, 0.0), axis=0, keepdims=True
    )
    with scope("p7_hand"):
        pl.semaphore_wait(hand_sem.at[len(hands)], 1)

    def exchange(ring, me, count, target, send_sem, recv_sem, value):
        ring[me] = value
        for offset in sorted(range(1, count), key=lambda k: -min(k, count - k)):
            pltpu.make_async_remote_copy(
                src_ref=ring.at[me],
                dst_ref=ring.at[me],
                send_sem=send_sem.at[0],
                recv_sem=recv_sem.at[0],
                device_id=target(lax.rem(me + offset, count)),
                device_id_type=MESH,
            ).start()
        return pltpu.make_async_remote_copy(
            src_ref=ring.at[pl.ds(0, count - 1)],
            dst_ref=ring.at[pl.ds(0, count - 1)],
            send_sem=send_sem.at[0],
            recv_sem=recv_sem.at[0],
            device_id=target(lax.rem(me + 1, count)),
            device_id_type=MESH,
        )

    cores = 2
    copies_y = exchange(
        ring_y,
        planey * cores + ens,
        planeys * cores,
        lambda peer: {"planey": peer // cores, "ens": lax.rem(peer, cores)},
        y_send,
        y_recv,
        message,
    )

    for comp in range(comps):
        for layer in range(layers):
            total = None
            for member in range(members):
                start = mw[1, OWN : OWN + rows, :] * uw[member, comp, layer + 1, OWN : OWN + rows, :]
                total = start if total is None else total + start
            all_start[ens, comp, layer] = total
    for part in sends:
        for copy, sent, arrives in part:

            @pl.when(sent)
            def _():
                copy.wait_send()

    with scope("p8_ary"):
        copies_y.wait_recv()
    copies_x = exchange(
        ring_x,
        plane,
        planes,
        lambda peer: {"plane": peer},
        x_send,
        x_recv,
        jnp.sum(ring_y[...], axis=0),
    )
    share_member(members - 1)
    to_partner(2 * members, all_start.at[ens], all_start.at[ens])
    copies_y.wait_send()
    for copy in fields:
        copy.wait_recv()
        copy.wait_send()
    with scope("p9_arx"):
        copies_x.wait_recv()
    sums = jnp.sum(ring_x[...], axis=0)
    gram_rr = sums
    gram_ra = pltpu.roll(sums, cols - 1, 1)
    gram_aa = pltpu.roll(sums, cols - 2, 1)
    gram_ab = pltpu.roll(sums, cols - 3, 1)
    first_step = gram_rr / gram_ra
    norm_next = gram_rr - 2.0 * first_step * gram_ra + first_step * first_step * gram_aa
    growth = 1.0 + norm_next / gram_rr
    curve = (
        growth * growth * gram_ra
        - 2.0 * growth * first_step * gram_aa
        + first_step * first_step * gram_ab
    )
    second_step = norm_next / curve
    samples = members * cores
    share = 1.0 / samples
    for_residual = share * (first_step + second_step * growth)
    for_image = share * (second_step * first_step)
    lane = lax.broadcasted_iota(jnp.int32, (1, cols), 1)

    def pick(value, number):
        return jnp.sum(jnp.where(lane == 4 * number, value, 0.0), axis=1, keepdims=True)

    weights = [(pick(for_residual, k), pick(for_image, k)) for k in range(samples)]

    def combine(layer, carry):
        for comp in range(comps):
            total = share * (all_start[0, comp, layer] + all_start[1, comp, layer])
            for number in range(samples):
                total = total + (
                    weights[number][0] * all_residual[number, comp, layer, HALO : HALO + rows, :]
                    - weights[number][1] * all_image[number, comp, layer, HALO : HALO + rows, :]
                )
            out[comp, layer] = total
        return carry

    with scope("pa_combine"):
        lax.fori_loop(0, layers, combine, 0, unroll=UNROLL)
    with scope("pb_sent"):
        copies_x.wait_send()


def body(sizes, u_prior, friction_rows, friction_table, bed_fixed, ice_mask):
    planes, planeys = sizes
    members, comps, layers, rows, cols = u_prior.shape
    wide = rows + 2 * HALO
    deep = rows + 24
    samples = 2 * members
    f32 = jnp.float32
    anywhere = pl.BlockSpec(memory_space=pltpu.HBM)
    fields = 2 + members * (1 + comps)
    vmem = pltpu.VMEM
    dma = pltpu.SemaphoreType.DMA
    return pl.pallas_call(
        functools.partial(kernel, sizes),
        out_shape=jax.ShapeDtypeStruct((comps, layers, rows, cols), f32),
        in_specs=[anywhere] * 5,
        out_specs=pl.BlockSpec(memory_space=pltpu.VMEM),
        scratch_shapes=[
            vmem((members, comps, layers + 2, deep, cols), f32),
            vmem((2 + members, deep, cols), f32),
            vmem((fields, deep, cols), f32),
            vmem((fields, deep, cols), f32),
            vmem((fields, deep, cols), f32),
            vmem(friction_table.shape, f32),
            vmem((rows, cols), jnp.int32),
            vmem((rows, cols), jnp.int32),
            pltpu.SMEM((members,), jnp.int32),
            vmem((2 * comps, deep, cols), f32),
            vmem((2 * comps, deep, cols), f32),
            vmem((9, wide, cols), f32),
            vmem((9, wide, cols), f32),
            vmem((layers, wide, cols), f32),
            vmem((comps, layers, wide, cols), f32),
            vmem((comps, layers + 2, deep, cols), f32),
            vmem((comps, layers + 2, deep, cols), f32),
            vmem((comps, layers + 2, deep, cols), f32),
            vmem((comps, layers, wide, cols), f32),
            vmem((samples, comps, layers, wide, cols), f32),
            vmem((samples, comps, layers, wide, cols), f32),
            vmem((2, comps, layers, rows, cols), f32),
            vmem((4 * members, 8, cols), f32),
            vmem((2 * planeys, 1, cols), f32),
            vmem((planes, 1, cols), f32),
            dma((members + 4,)),
            dma((2 + 10 * members,)),
            dma((2 + 10 * members,)),
            pltpu.SemaphoreType.REGULAR((8,)),
            dma((2 * members + 1,)),
            dma((2 * members + 1,)),
            dma((1,)),
            dma((1,)),
            dma((1,)),
            dma((1,)),
        ],
        compiler_params=pltpu.CompilerParams(
            collective_id=0, has_side_effects=True, vmem_limit_bytes=48 * 1024 * 1024
        ),
    )(*[
        pltpu.with_memory_space_constraint(x, pltpu.HBM)
        for x in (u_prior, friction_rows, friction_table, bed_fixed, ice_mask)
    ])


def solution(mesh):
    in_specs = (
        P(("group", "ens"), None, None, "plane", "planey"),
        P(("group", "ens")),
        P("group", "plane", "planey"),
        P("plane", "planey"),
        P("plane", "planey"),
    )
    out_specs = P("group", None, "plane", "planey")
    sizes = (mesh.shape["plane"], mesh.shape["planey"])
    return jax.shard_map(
        functools.partial(body, sizes),
        mesh=mesh,
        in_specs=in_specs,
        out_specs=out_specs,
        check_vma=False,
    )
```

```python
import contextlib
import functools

import jax
import jax.numpy as jnp
from jax import lax
from jax.experimental import pallas as pl
from jax.experimental.pallas import tpu as pltpu
from jax.sharding import PartitionSpec as P

bed_unit = 2.0 ** (-29)
HALO = 4
TOP = 8
OWN = TOP + HALO
PITCH = 8
MESH = pl.DeviceIdType.MESH
along_z = 0.5
along_x = (0.25, 0.125)
along_y = (0.125, 0.25)
MASK = 0
UNROLL = 10


def scope(name):
    return contextlib.nullcontext()


EDGE_U, EDGE_R, EDGE_0, EDGE_1, EDGE_2 = 0, 2, 3, 5, 7


def kernel(
    sizes,
    u_hbm,
    picks_hbm,
    table_hbm,
    bed_hbm,
    mask_hbm,
    out,
    uw,
    mw,
    xo,
    xl,
    xr,
    table,
    bed_in,
    mask_in,
    picks,
    strip,
    shifted,
    strip_kept,
    tally,
    edge,
    fixed,
    roots,
    step_y,
    tr,
    tp,
    tq,
    field_a,
    all_residual,
    all_image,
    all_start,
    gram,
    ring_y,
    ring_x,
    local_sem,
    halo_send,
    halo_recv,
    hand_sem,
    pair_send,
    pair_recv,
    y_send,
    y_recv,
    x_send,
    x_recv,
):
    planes, planeys = sizes
    members, comps, layers, rows, cols = u_hbm.shape
    wide = rows + 2 * HALO
    end = TOP + wide
    plane = lax.axis_index("plane")
    planey = lax.axis_index("planey")
    ens = lax.axis_index("ens")

    def at(dx, dy):
        return {
            "plane": lax.rem(plane + dx + planes, planes),
            "planey": lax.rem(planey + dy + planeys, planeys),
        }

    partner = {"ens": 1 - ens}
    around = [(dx, dy) for dx in (-1, 0, 1) for dy in (-1, 0, 1) if (dx, dy) != (0, 0)]

    def exists(dx, dy):
        flag = None
        for step, index, count in ((dx, plane, planes), (dy, planey, planeys)):
            if step != 0:
                part = index > 0 if step < 0 else index < count - 1
                flag = part if flag is None else jnp.logical_and(flag, part)
        return flag

    bed_field = 1 + comps

    def friction_field(member):
        return bed_field + 1 + member * (1 + comps) - (comps if member > 0 else 0)

    def u_field(member):
        return 1 if member == 0 else friction_field(member) + 1

    def load_member(member):
        return pltpu.make_async_copy(
            u_hbm.at[member],
            uw.at[member, :, pl.ds(1, layers), pl.ds(OWN, rows), :],
            local_sem.at[member],
        )

    load_u = [load_member(member) for member in range(members)]
    load_picks = pltpu.make_async_copy(picks_hbm, picks, local_sem.at[members])
    load_maps = [
        pltpu.make_async_copy(source, target, local_sem.at[members + 1])
        for source, target in ((table_hbm, table), (bed_hbm, bed_in), (mask_hbm, mask_in))
    ]
    maps_rows = (table.shape[0] + 2) * rows
    for load in (load_u[0], load_picks, *load_maps, *load_u[1:]):
        load.start()

    barrier = pltpu.get_barrier_semaphore()
    for dx, dy in around:
        pl.semaphore_signal(barrier, inc=1, device_id=at(dx, dy), device_id_type=MESH)
    pl.semaphore_signal(barrier, inc=1, device_id=partner, device_id_type=MESH)

    for end_layer in (0, layers + 1):
        uw[:, :, end_layer, TOP:end, :] = jnp.zeros((members, comps, wide, cols), jnp.float32)
        for buffer in (tr, tp, tq):
            buffer[:, end_layer] = jnp.zeros(buffer.shape[:1] + buffer.shape[2:], jnp.float32)
    for step, first in ((-1, TOP), (1, OWN + rows)):

        @pl.when(jnp.logical_not(exists(step, 0)))
        def _():
            uw[:, :, 1 : 1 + layers, first : first + HALO, :] = jnp.zeros(
                (members, comps, layers, HALO, cols), jnp.float32
            )
            for buffer in (mw, xo, xl, xr):
                buffer[:, first : first + HALO, :] = jnp.zeros(
                    (buffer.shape[0], HALO, cols), jnp.float32
                )

    for step, buffer in ((-1, xl), (1, xr)):

        @pl.when(jnp.logical_not(exists(0, step)))
        def _():
            buffer[:, TOP:end, :] = jnp.zeros((buffer.shape[0], wide, cols), jnp.float32)

    def kind(dx, dy):
        return "both" if dx != 0 and dy != 0 else ("x" if dx != 0 else "y")

    def send(part, dx, dy, *pairs):
        copies = [
            pltpu.make_async_remote_copy(
                src_ref=source,
                dst_ref=target,
                send_sem=halo_send.at[0],
                recv_sem=halo_recv.at[part],
                device_id=at(dx, dy),
                device_id_type=MESH,
            )
            for source, target in pairs
        ]

        @pl.when(exists(dx, dy))
        def _():
            for copy in copies:
                copy.start()

        if dx >= 0 and dy >= 0:
            for source, _ in pairs:
                count = 1
                for size in source.shape[:-1]:
                    count *= size
                rows_of[part][kind(dx, dy)] += count

    rows_of = [{"x": 0, "y": 0, "both": 0} for _ in range(1 + members)]

    def each_total(counts, action):
        ends_x = jnp.logical_or(plane == 0, plane == planes - 1)
        ends_y = jnp.logical_or(planey == 0, planey == planeys - 1)
        for many_x in (1, 2):
            for many_y in (1, 2):
                total = many_x * counts["x"] + many_y * counts["y"]
                total += many_x * many_y * counts["both"]
                here_x = ends_x if many_x == 1 else jnp.logical_not(ends_x)
                here_y = ends_y if many_y == 1 else jnp.logical_not(ends_y)

                @pl.when(jnp.logical_and(here_x, here_y))
                def _():
                    action(total)

    def counted(total, part):
        block = tally.at[pl.ds(0, total)]
        return pltpu.make_async_remote_copy(
            src_ref=block,
            dst_ref=block,
            send_sem=halo_send.at[0],
            recv_sem=halo_recv.at[part],
            device_id=partner,
            device_id_type=MESH,
        )

    def row_range(dx):
        if dx < 0:
            return pl.ds(OWN, HALO), pl.ds(OWN + rows, HALO)
        if dx > 0:
            return pl.ds(OWN + rows - HALO, HALO), pl.ds(TOP, HALO)
        return pl.ds(OWN, rows), pl.ds(OWN, rows)

    hands = []
    for axis, count in (("plane", planes), ("planey", planeys)):
        reach = 1
        while reach * 2 <= count // 2:
            hands.append((reach, axis))
            reach *= 2
    hands.sort()

    def greet(number):
        reach, axis = hands[number]
        for step in (-reach, reach):
            target = at(step, 0) if axis == "plane" else at(0, step)
            pl.semaphore_signal(
                hand_sem.at[number], inc=1, device_id=target, device_id_type=MESH
            )

    def greeted(number):
        pl.semaphore_wait(hand_sem.at[number], 2)

    def greet_round(reach):
        for number, (distance, _) in enumerate(hands):
            if distance == reach:
                greet(number)

    def greeted_round(reach):
        for number, (distance, _) in enumerate(hands):
            if distance == reach:
                greeted(number)

    lane = lax.broadcasted_iota(jnp.int32, (rows, cols), 1)
    group = lane // PITCH

    def lane_packed(planes_of):
        packed = jnp.zeros((rows, cols), jnp.float32)
        for layer in range(layers):
            turned = pltpu.roll(planes_of(layer), (PITCH * layer + HALO) % cols, 1)
            packed = jnp.where(group == layer, turned, packed)
        return packed

    body = pl.ds(1, layers)

    def send_u(part, member):
        for dx in (-1, 1):
            here, there = row_range(dx)
            send(
                part,
                dx,
                0,
                (uw.at[member, :, body, here, :], uw.at[member, :, body, there, :]),
            )

    def pack_u(member):
        for comp in range(comps):
            xo[u_field(member) + comp, OWN : OWN + rows, :] = lane_packed(
                lambda layer: uw[member, comp, 1 + layer, OWN : OWN + rows, :]
            )

    def send_packed(part, low, count, map_low, map_count):
        fields_here = pl.ds(low, count)
        maps_here = pl.ds(map_low, map_count)
        for dx, dy in sorted(around, key=lambda d: -abs(d[0])):
            here, there = row_range(dx)
            target = xo if dy == 0 else (xr if dy < 0 else xl)
            pairs = [(xo.at[fields_here, here, :], target.at[fields_here, there, :])]
            if dy == 0:
                pairs.append((mw.at[maps_here, here, :], mw.at[maps_here, there, :]))
            send(part, dx, dy, *pairs)

    with scope("p0_load"):
        load_u[0].wait()
    with scope("p1_barrier"):
        pl.semaphore_wait(barrier, len(around) + 1)
    send_u(0, 0)
    block = tally.at[pl.ds(0, maps_rows)]
    pltpu.make_async_copy(block, block, local_sem.at[members + 1]).wait()
    load_picks.wait()
    mask_own = mask_in[...].astype(jnp.float32)
    bed_own = bed_in[...].astype(jnp.float32) * bed_unit
    mw[0, OWN : OWN + rows, :] = mask_own
    xo[MASK, OWN : OWN + rows, :] = lane_packed(lambda layer: mask_own)
    pack_u(0)
    send_packed(0, 0, 1 + comps, 0, 1)
    greet_round(1)
    mw[1, OWN : OWN + rows, :] = bed_own
    xo[bed_field, OWN : OWN + rows, :] = lane_packed(lambda layer: bed_own)
    for member in range(members):
        chosen = table[picks[member]]
        mw[2 + member, OWN : OWN + rows, :] = chosen
        xo[friction_field(member), OWN : OWN + rows, :] = jnp.where(
            lane < PITCH, pltpu.roll(chosen, HALO, 1), 0.0
        )
    send_packed(1, bed_field, 2, 1, 2)
    for member in range(1, members):
        load_u[member].wait()
        send_u(1 + member, member)
        pack_u(member)
        send_packed(1 + member, friction_field(member), 1 + comps, 2 + member, 1)

    with scope("p3_greeted1"):
        greeted_round(1)
    greet_round(2)
    with scope("p5_greeted2"):
        greeted_round(2)
    greet_round(4)
    pl.semaphore_signal(
        hand_sem.at[len(hands)], inc=1, device_id=partner, device_id_type=MESH
    )

    def arrived(part):
        with scope("p4_halo%d" % part):
            each_total(rows_of[part], lambda total: counted(total, part).wait_recv())

    arrived(0)

    lane = lax.broadcasted_iota(jnp.int32, (wide, cols), 1)
    first_lane = lane == 0
    last_lane = lane == cols - 1
    spot = lax.rem(lane, PITCH)
    outer_left = spot < HALO
    left_edge = spot == HALO - 1
    position = (
        plane * rows - HALO + lax.broadcasted_iota(jnp.int32, (wide, cols), 0)
    ).astype(jnp.float32)
    thickness = 1.0 + 2.0 * position / (rows * planes - 1)

    def sides(number, low=TOP, high=end):
        own = xo[number, low:high, :]
        return (
            jnp.where(outer_left, xl[number, low:high, :], own),
            jnp.where(outer_left, own, xr[number, low:high, :]),
        )

    def edges(pair):
        left, right = pair
        return jnp.where(
            left_edge, pltpu.roll(right, cols - 1, 1), pltpu.roll(left, 1, 1)
        )

    def y_pair(value, near):
        return (
            jnp.where(last_lane, near, pltpu.roll(value, cols - 1, 1)),
            jnp.where(first_lane, near, pltpu.roll(value, 1, 1)),
        )

    def turned_edge(value, layer):
        return pltpu.roll(value, cols - HALO - PITCH * layer, 1)

    mask_main = mw[0, TOP:end, :]
    fixed[0] = mask_main
    for side, mask_here in enumerate(sides(MASK)):
        fixed[3 + side] = mask_here

    def forces():
        bed_pair = sides(bed_field)
        bed_plus, bed_minus = y_pair(mw[1, TOP:end, :], turned_edge(edges(bed_pair), 0))
        scale = -(fixed[0] * thickness)
        fixed[1] = scale * (
            (mw[1, TOP + 1 : end + 1, :] - mw[1, TOP - 1 : end - 1, :]) * 0.5
        )
        fixed[2] = scale * ((bed_plus - bed_minus) * 0.5)
        for side, bed_here in enumerate(bed_pair):
            shifted[side, TOP:end, :] = bed_here
            down = shifted[side, TOP + 1 : end + 1, :] - shifted[side, TOP - 1 : end - 1, :]
            flat = pltpu.roll(bed_here, cols - 1, 1) - pltpu.roll(bed_here, 1, 1)
            scale = -(fixed[3 + side] * thickness)
            fixed[5 + side] = scale * (down * 0.5)
            fixed[7 + side] = scale * (flat * 0.5)

    def power(strain4):
        return jnp.exp(jnp.log(strain4 * 0.25 + 0.1) * (-1.0 / 6.0))

    def strain4_of(ui, vi, uj, vj, uz, vz):
        shear = uj + vi
        return ui * ui + vj * vj + ui * vj + 0.25 * (shear * shear + (uz * uz + vz * vz))

    def strip_k(pair, comp, slot):
        result = []
        for side, value in enumerate(pair):
            value = value + along_y[comp] * (
                pltpu.roll(value, cols - 1, 1) + pltpu.roll(value, 1, 1)
            )
            value = value + along_z * (
                pltpu.roll(value, cols - PITCH, 1) + pltpu.roll(value, PITCH, 1)
            )
            shifted[slot + side, TOP:end, :] = value
            result.append(
                value
                + along_x[comp]
                * (
                    shifted[slot + side, TOP + 1 : end + 1, :]
                    + shifted[slot + side, TOP - 1 : end - 1, :]
                )
            )
        return result

    own_top = lax.broadcasted_iota(jnp.int32, (8, cols), 0) >= HALO

    def own_sum(value):
        total = jnp.where(own_top, value[:8], value[wide - 8 :])
        for low in range(8, wide - 8, 8):
            total = total + value[low : low + 8]
        return total

    def strip_start(member):
        for comp in range(comps):
            pair = sides(u_field(member) + comp)
            edge[EDGE_U + comp] = edges(pair)
            for side in range(2):
                strip[comp * 2 + side, TOP:end, :] = pair[side]
        strip_roots = []
        for side in range(2):
            value = [strip[comp * 2 + side, TOP:end, :] for comp in range(comps)]
            step_i = [
                strip[comp * 2 + side, TOP + 1 : end + 1, :]
                - strip[comp * 2 + side, TOP - 1 : end - 1, :]
                for comp in range(comps)
            ]
            step_j = [pltpu.roll(v, cols - 1, 1) - pltpu.roll(v, 1, 1) for v in value]
            step_z = [pltpu.roll(v, cols - PITCH, 1) - pltpu.roll(v, PITCH, 1) for v in value]
            strip_roots.append(
                fixed[3 + side]
                * power(
                    strain4_of(
                        step_i[0], step_i[1], step_j[0], step_j[1], step_z[0], step_z[1]
                    )
                )
            )
            strip_kept[side] = strip_roots[side]
        edge[EDGE_R] = edges(strip_roots)
        for comp in range(comps):
            around_roots = strip_k(strip_roots, comp, comp * 2)
            field = [
                strip_roots[side] * (fixed[3 + side] * strip[comp * 2 + side, TOP:end, :])
                for side in range(2)
            ]
            edge[EDGE_0 + comp] = edges(field)
            near = strip_k(field, comp, 4 + comp * 2)
            for side in range(2):
                strip_kept[2 + 4 * comp + side] = around_roots[side]
                strip_kept[4 + 4 * comp + side] = near[side]

    def strip_end(member):
        strip_roots = [strip_kept[side] for side in range(2)]
        four = [4.0 * root for root in strip_roots]
        friction_pair = sides(friction_field(member))
        diag = [
            fixed[3 + side] * friction_pair[side] + (1.0 - fixed[3 + side])
            for side in range(2)
        ]
        for comp in range(comps):
            main = [
                four[side] * strip_kept[2 + 4 * comp + side] + diag[side]
                for side in range(2)
            ]
            residual = [
                fixed[5 + 2 * comp + side]
                - (
                    main[side] * (fixed[3 + side] * strip[comp * 2 + side, TOP:end, :])
                    - four[side] * strip_kept[4 + 4 * comp + side]
                )
                for side in range(2)
            ]
            field = [strip_roots[side] * residual[side] for side in range(2)]
            edge[EDGE_1 + comp] = edges(field)
            near = strip_k(field, comp, comp * 2)
            image = [
                main[side] * residual[side] - four[side] * near[side] for side in range(2)
            ]
            edge[EDGE_2 + comp] = edges([strip_roots[side] * image[side] for side in range(2)])

    def share_start(member):
        for comp in range(comps):
            for layer in range(layers):
                plus, minus = y_pair(
                    uw[member, comp, layer + 1, TOP:end, :],
                    turned_edge(edge[EDGE_U + comp], layer),
                )
                step_y[comp, layer] = plus - minus
        for layer in range(layers):
            step_i = [
                uw[member, comp, layer + 1, TOP + 1 : end + 1, :]
                - uw[member, comp, layer + 1, TOP - 1 : end - 1, :]
                for comp in range(comps)
            ]
            step_z = [
                uw[member, comp, layer + 2, TOP:end, :] - uw[member, comp, layer, TOP:end, :]
                for comp in range(comps)
            ]
            roots[layer] = fixed[0] * power(
                strain4_of(
                    step_i[0],
                    step_i[1],
                    step_y[0, layer],
                    step_y[1, layer],
                    step_z[0],
                    step_z[1],
                )
            )
        for layer in range(layers):
            root = roots[layer]
            plus, minus = y_pair(root, turned_edge(edge[EDGE_R], layer))
            both = plus + minus
            for comp in range(comps):
                tr[comp, layer + 1, TOP:end, :] = root + along_y[comp] * both
                field = root * (fixed[0] * uw[member, comp, layer + 1, TOP:end, :])
                plus, minus = y_pair(field, turned_edge(edge[EDGE_0 + comp], layer))
                tp[comp, layer + 1, TOP:end, :] = field + along_y[comp] * (plus + minus)

    def x_sum(buffer, comp, layer):
        return buffer[comp, layer, TOP:end, :] + along_x[comp] * (
            buffer[comp, layer, TOP + 1 : end + 1, :]
            + buffer[comp, layer, TOP - 1 : end - 1, :]
        )

    def share_end(member):
        slot = members * ens + member
        empty = jnp.zeros((wide, cols), jnp.float32)

        def residual_layer(layer, carry):
            before, now, total = carry
            root = roots[layer]
            four = 4.0 * root
            here = fixed[0]
            bottom = jnp.where(layer == 0, 1.0, 0.0)
            diag = here * mw[2 + member, TOP:end, :] * bottom + (1.0 - here)
            after = []
            for comp in range(comps):
                after_r = x_sum(tr, comp, layer + 2)
                after_p = x_sum(tp, comp, layer + 2)
                after += [after_r, after_p]
                around_roots = now[2 * comp] + along_z * (before[2 * comp] + after_r)
                near = now[2 * comp + 1] + along_z * (before[2 * comp + 1] + after_p)
                main = four * around_roots + diag
                start = here * uw[member, comp, layer + 1, TOP:end, :]
                residual = fixed[1 + comp] - (main * start - four * near)
                field_a[comp, layer] = main
                all_residual[slot, comp, layer] = residual
                total = total + own_sum(residual * residual)
                field = root * residual
                plus, minus = y_pair(field, turned_edge(edge[EDGE_1 + comp], layer))
                tq[comp, layer + 1, TOP:end, :] = field + along_y[comp] * (plus + minus)
            return tuple(now), tuple(after), total

        nothing = jnp.zeros((8, cols), jnp.float32)
        first = tuple(
            x_sum(buffer, comp, 1) for comp in range(comps) for buffer in (tr, tp)
        )
        with scope("q2_residual"):
            _, _, gram_rr = lax.fori_loop(
                0, layers, residual_layer, ((empty,) * 4, first, nothing), unroll=UNROLL
            )

        def image_layer(layer, carry):
            before, now, total_ra, total_aa = carry
            root = roots[layer]
            four = 4.0 * root
            after = []
            for comp in range(comps):
                after_p = x_sum(tq, comp, layer + 2)
                after.append(after_p)
                near = now[comp] + along_z * (before[comp] + after_p)
                residual = all_residual[slot, comp, layer]
                image = field_a[comp, layer] * residual - four * near
                all_image[slot, comp, layer] = image
                total_ra = total_ra + own_sum(residual * image)
                total_aa = total_aa + own_sum(image * image)
                field = root * image
                plus, minus = y_pair(field, turned_edge(edge[EDGE_2 + comp], layer))
                tp[comp, layer + 1, TOP:end, :] = field + along_y[comp] * (plus + minus)
            return tuple(now), tuple(after), total_ra, total_aa

        first = tuple(x_sum(tq, comp, 1) for comp in range(comps))
        with scope("q3_image"):
            _, _, gram_ra, gram_aa = lax.fori_loop(
                0,
                layers,
                image_layer,
                ((empty,) * 2, first, nothing, nothing),
                unroll=UNROLL,
            )

        def own_x_sum(comp, layer):
            return tp[comp, layer, OWN : OWN + rows, :] + along_x[comp] * (
                tp[comp, layer, OWN + 1 : OWN + rows + 1, :]
                + tp[comp, layer, OWN - 1 : OWN + rows - 1, :]
            )

        def second_layer(layer, carry):
            before, now, total = carry
            four = 4.0 * roots[layer, HALO : HALO + rows, :]
            after = []
            for comp in range(comps):
                after_p = own_x_sum(comp, layer + 2)
                after.append(after_p)
                near = now[comp] + along_z * (before[comp] + after_p)
                image = all_image[slot, comp, layer, HALO : HALO + rows, :]
                second = (
                    field_a[comp, layer, HALO : HALO + rows, :] * image - four * near
                )
                product = image * second
                for low in range(0, rows, 8):
                    total = total + product[low : low + 8]
            return tuple(now), tuple(after), total

        empty_own = jnp.zeros((rows, cols), jnp.float32)
        first = tuple(own_x_sum(comp, 1) for comp in range(comps))
        with scope("q4_second"):
            _, _, gram_ab = lax.fori_loop(
                0, layers, second_layer, ((empty_own,) * 2, first, nothing), unroll=UNROLL
            )
        for number, value in enumerate((gram_rr, gram_ra, gram_aa, gram_ab)):
            gram[4 * member + number] = value

    def to_partner(block):
        pltpu.make_async_remote_copy(
            src_ref=block,
            dst_ref=block,
            send_sem=pair_send.at[0],
            recv_sem=pair_recv.at[0],
            device_id=partner,
            device_id_type=MESH,
        ).start()

    inner = pl.ds(HALO, rows)

    def share_member(member):
        slot = members * ens + member
        for buffer in (all_residual, all_image):
            to_partner(buffer.at[slot, :, :, inner, :])

    for member in range(members):
        if member > 0:
            arrived(1 + member)
        with scope("q0_start"):
            strip_start(member)
            share_start(member)
        if member == 0:
            arrived(1)
            forces()
        with scope("q1_end"):
            strip_end(member)
            share_end(member)
        if member < members - 1:
            share_member(member)

    lines = 4 * members
    total = jnp.sum(gram[...], axis=1)
    total = jnp.sum(total, axis=1, keepdims=True)
    lane = lax.broadcasted_iota(jnp.int32, (lines, cols), 1)
    line = lax.broadcasted_iota(jnp.int32, (lines, cols), 0)
    message = jnp.sum(
        jnp.where(lane == line + lines * ens, total, 0.0), axis=0, keepdims=True
    )
    with scope("p7_hand"):
        pl.semaphore_wait(hand_sem.at[len(hands)], 1)

    def exchange(ring, me, count, target, send_sem, recv_sem, value):
        ring[me] = value
        for offset in sorted(range(1, count), key=lambda k: -min(k, count - k)):
            pltpu.make_async_remote_copy(
                src_ref=ring.at[me],
                dst_ref=ring.at[me],
                send_sem=send_sem.at[0],
                recv_sem=recv_sem.at[0],
                device_id=target(lax.rem(me + offset, count)),
                device_id_type=MESH,
            ).start()
        return pltpu.make_async_remote_copy(
            src_ref=ring.at[pl.ds(0, count - 1)],
            dst_ref=ring.at[pl.ds(0, count - 1)],
            send_sem=send_sem.at[0],
            recv_sem=recv_sem.at[0],
            device_id=target(lax.rem(me + 1, count)),
            device_id_type=MESH,
        )

    cores = 2
    copies_y = exchange(
        ring_y,
        planey * cores + ens,
        planeys * cores,
        lambda peer: {"planey": peer // cores, "ens": lax.rem(peer, cores)},
        y_send,
        y_recv,
        message,
    )

    for comp in range(comps):
        for layer in range(layers):
            total = None
            for member in range(members):
                start = mw[0, OWN : OWN + rows, :] * uw[member, comp, layer + 1, OWN : OWN + rows, :]
                total = start if total is None else total + start
            all_start[ens, comp, layer] = total
    everything = {
        name: sum(counts[name] for counts in rows_of) for name in ("x", "y", "both")
    }
    each_total(everything, lambda total: counted(total, 0).wait_send())
    with scope("p8_ary"):
        copies_y.wait_recv()
    with scope("p6_greeted4"):
        for reach in (4, 8, 16):
            greeted_round(reach)
            if reach > 2:
                greet_round(2 * reach)
    copies_x = exchange(
        ring_x,
        plane,
        planes,
        lambda peer: {"plane": peer},
        x_send,
        x_recv,
        jnp.sum(ring_y[...], axis=0),
    )
    share_member(members - 1)
    to_partner(all_start.at[ens])
    copies_y.wait_send()
    block = all_residual.at[:, :, :, pl.ds(0, (2 * members + 1) * rows // (2 * members)), :]
    fields = pltpu.make_async_remote_copy(
        src_ref=block,
        dst_ref=block,
        send_sem=pair_send.at[0],
        recv_sem=pair_recv.at[0],
        device_id=partner,
        device_id_type=MESH,
    )
    fields.wait_send()
    fields.wait_recv()
    with scope("p9_arx"):
        copies_x.wait_recv()
    sums = jnp.sum(ring_x[...], axis=0)
    gram_rr = sums
    gram_ra = pltpu.roll(sums, cols - 1, 1)
    gram_aa = pltpu.roll(sums, cols - 2, 1)
    gram_ab = pltpu.roll(sums, cols - 3, 1)
    first_step = gram_rr / gram_ra
    norm_next = gram_rr - 2.0 * first_step * gram_ra + first_step * first_step * gram_aa
    growth = 1.0 + norm_next / gram_rr
    curve = (
        growth * growth * gram_ra
        - 2.0 * growth * first_step * gram_aa
        + first_step * first_step * gram_ab
    )
    second_step = norm_next / curve
    samples = members * cores
    share = 1.0 / samples
    for_residual = share * (first_step + second_step * growth)
    for_image = share * (second_step * first_step)
    lane = lax.broadcasted_iota(jnp.int32, (1, cols), 1)

    def pick(value, number):
        return jnp.sum(jnp.where(lane == 4 * number, value, 0.0), axis=1, keepdims=True)

    weights = [(pick(for_residual, k), pick(for_image, k)) for k in range(samples)]

    def combine(layer, carry):
        for comp in range(comps):
            total = share * (all_start[0, comp, layer] + all_start[1, comp, layer])
            for number in range(samples):
                total = total + (
                    weights[number][0] * all_residual[number, comp, layer, HALO : HALO + rows, :]
                    - weights[number][1] * all_image[number, comp, layer, HALO : HALO + rows, :]
                )
            out[comp, layer] = total
        return carry

    with scope("pa_combine"):
        lax.fori_loop(0, layers, combine, 0, unroll=UNROLL)
    with scope("pb_sent"):
        copies_x.wait_send()


def body(sizes, u_prior, friction_rows, friction_table, bed_fixed, ice_mask):
    planes, planeys = sizes
    members, comps, layers, rows, cols = u_prior.shape
    wide = rows + 2 * HALO
    deep = rows + 24
    samples = 2 * members
    f32 = jnp.float32
    anywhere = pl.BlockSpec(memory_space=pltpu.HBM)
    fields = 2 + members * (1 + comps)
    vmem = pltpu.VMEM
    dma = pltpu.SemaphoreType.DMA
    return pl.pallas_call(
        functools.partial(kernel, sizes),
        out_shape=jax.ShapeDtypeStruct((comps, layers, rows, cols), f32),
        in_specs=[anywhere] * 5,
        out_specs=pl.BlockSpec(memory_space=pltpu.VMEM),
        scratch_shapes=[
            vmem((members, comps, layers + 2, deep, cols), f32),
            vmem((2 + members, deep, cols), f32),
            vmem((fields, deep, cols), f32),
            vmem((fields, deep, cols), f32),
            vmem((fields, deep, cols), f32),
            vmem(friction_table.shape, f32),
            vmem((rows, cols), jnp.int32),
            vmem((rows, cols), jnp.int32),
            pltpu.SMEM((members,), jnp.int32),
            vmem((2 * comps, deep, cols), f32),
            vmem((4 * comps, deep, cols), f32),
            vmem((2 + 4 * comps, wide, cols), f32),
            vmem((1536, cols), f32),
            vmem((9, wide, cols), f32),
            vmem((9, wide, cols), f32),
            vmem((layers, wide, cols), f32),
            vmem((comps, layers, wide, cols), f32),
            vmem((comps, layers + 2, deep, cols), f32),
            vmem((comps, layers + 2, deep, cols), f32),
            vmem((comps, layers + 2, deep, cols), f32),
            vmem((comps, layers, wide, cols), f32),
            vmem((samples, comps, layers, wide, cols), f32),
            vmem((samples, comps, layers, wide, cols), f32),
            vmem((2, comps, layers, rows, cols), f32),
            vmem((4 * members, 8, cols), f32),
            vmem((2 * planeys, 1, cols), f32),
            vmem((planes, 1, cols), f32),
            dma((members + 2,)),
            dma((1,)),
            dma((1 + members,)),
            pltpu.SemaphoreType.REGULAR((6,)),
            dma((1,)),
            dma((1,)),
            dma((1,)),
            dma((1,)),
            dma((1,)),
            dma((1,)),
        ],
        compiler_params=pltpu.CompilerParams(
            collective_id=0, has_side_effects=True, vmem_limit_bytes=48 * 1024 * 1024
        ),
    )(*[
        pltpu.with_memory_space_constraint(x, pltpu.HBM)
        for x in (u_prior, friction_rows, friction_table, bed_fixed, ice_mask)
    ])


def solution(mesh):
    in_specs = (
        P(("group", "ens"), None, None, "plane", "planey"),
        P(("group", "ens")),
        P("group", "plane", "planey"),
        P("plane", "planey"),
        P("plane", "planey"),
    )
    out_specs = P("group", None, "plane", "planey")
    sizes = (mesh.shape["plane"], mesh.shape["planey"])
    return jax.shard_map(
        functools.partial(body, sizes),
        mesh=mesh,
        in_specs=in_specs,
        out_specs=out_specs,
        check_vma=False,
    )
```

```python
import contextlib
import functools

import jax
import jax.numpy as jnp
from jax import lax
from jax.experimental import pallas as pl
from jax.experimental.pallas import tpu as pltpu
from jax.sharding import PartitionSpec as P

bed_unit = 2.0 ** (-29)
HALO = 4
TOP = 8
OWN = TOP + HALO
PITCH = 8
MESH = pl.DeviceIdType.MESH
along_z = 0.5
along_x = (0.25, 0.125)
along_y = (0.125, 0.25)
MASK = 0
UNROLL = 10


def scope(name):
    return contextlib.nullcontext()


EDGE_U, EDGE_R, EDGE_0, EDGE_1, EDGE_2 = 0, 2, 3, 5, 7


def kernel(
    sizes,
    u_hbm,
    picks_hbm,
    table_hbm,
    bed_hbm,
    mask_hbm,
    out,
    uw,
    mw,
    xo,
    xl,
    xr,
    table,
    bed_in,
    mask_in,
    picks,
    strip,
    shifted,
    strip_kept,
    lane_matrix,
    tally,
    edge,
    fixed,
    roots,
    step_y,
    tr,
    tp,
    tq,
    field_a,
    all_residual,
    all_image,
    all_start,
    gram,
    ring_y,
    ring_x,
    local_sem,
    halo_send,
    halo_recv,
    hand_sem,
    pair_send,
    pair_recv,
    y_send,
    y_recv,
    x_send,
    x_recv,
):
    planes, planeys = sizes
    members, comps, layers, rows, cols = u_hbm.shape
    wide = rows + 2 * HALO
    end = TOP + wide
    plane = lax.axis_index("plane")
    planey = lax.axis_index("planey")
    ens = lax.axis_index("ens")

    def at(dx, dy):
        return {
            "plane": lax.rem(plane + dx + planes, planes),
            "planey": lax.rem(planey + dy + planeys, planeys),
        }

    partner = {"ens": 1 - ens}
    around = [(dx, dy) for dx in (-1, 0, 1) for dy in (-1, 0, 1) if (dx, dy) != (0, 0)]

    def exists(dx, dy):
        flag = None
        for step, index, count in ((dx, plane, planes), (dy, planey, planeys)):
            if step != 0:
                part = index > 0 if step < 0 else index < count - 1
                flag = part if flag is None else jnp.logical_and(flag, part)
        return flag

    bed_field = 1 + comps

    def friction_field(member):
        return bed_field + 1 + member * (1 + comps) - (comps if member > 0 else 0)

    def u_field(member):
        return 1 if member == 0 else friction_field(member) + 1

    def load_member(member):
        return pltpu.make_async_copy(
            u_hbm.at[member],
            uw.at[member, :, pl.ds(1, layers), pl.ds(OWN, rows), :],
            local_sem.at[member],
        )

    load_u = [load_member(member) for member in range(members)]
    load_picks = pltpu.make_async_copy(picks_hbm, picks, local_sem.at[members])
    load_maps = [
        pltpu.make_async_copy(source, target, local_sem.at[members + 1])
        for source, target in ((table_hbm, table), (bed_hbm, bed_in), (mask_hbm, mask_in))
    ]
    maps_rows = (table.shape[0] + 2) * rows
    for load in (load_u[0], load_picks, *load_maps, *load_u[1:]):
        load.start()

    barrier = pltpu.get_barrier_semaphore()
    for dx, dy in around:
        pl.semaphore_signal(barrier, inc=1, device_id=at(dx, dy), device_id_type=MESH)
    pl.semaphore_signal(barrier, inc=1, device_id=partner, device_id_type=MESH)

    for end_layer in (0, layers + 1):
        uw[:, :, end_layer, TOP:end, :] = jnp.zeros((members, comps, wide, cols), jnp.float32)
        for buffer in (tr, tp, tq):
            buffer[:, end_layer] = jnp.zeros(buffer.shape[:1] + buffer.shape[2:], jnp.float32)
    for step, first in ((-1, TOP), (1, OWN + rows)):

        @pl.when(jnp.logical_not(exists(step, 0)))
        def _():
            uw[:, :, 1 : 1 + layers, first : first + HALO, :] = jnp.zeros(
                (members, comps, layers, HALO, cols), jnp.float32
            )
            for buffer in (mw, xo, xl, xr):
                buffer[:, first : first + HALO, :] = jnp.zeros(
                    (buffer.shape[0], HALO, cols), jnp.float32
                )

    for step, buffer in ((-1, xl), (1, xr)):

        @pl.when(jnp.logical_not(exists(0, step)))
        def _():
            buffer[:, TOP:end, :] = jnp.zeros((buffer.shape[0], wide, cols), jnp.float32)

    def kind(dx, dy):
        return "both" if dx != 0 and dy != 0 else ("x" if dx != 0 else "y")

    def send(part, dx, dy, *pairs):
        copies = [
            pltpu.make_async_remote_copy(
                src_ref=source,
                dst_ref=target,
                send_sem=halo_send.at[0],
                recv_sem=halo_recv.at[part],
                device_id=at(dx, dy),
                device_id_type=MESH,
            )
            for source, target in pairs
        ]

        @pl.when(exists(dx, dy))
        def _():
            for copy in copies:
                copy.start()

        if dx >= 0 and dy >= 0:
            for source, _ in pairs:
                count = 1
                for size in source.shape[:-1]:
                    count *= size
                rows_of[part][kind(dx, dy)] += count

    rows_of = [{"x": 0, "y": 0, "both": 0} for _ in range(1 + members)]

    def each_total(counts, action):
        ends_x = jnp.logical_or(plane == 0, plane == planes - 1)
        ends_y = jnp.logical_or(planey == 0, planey == planeys - 1)
        for many_x in (1, 2):
            for many_y in (1, 2):
                total = many_x * counts["x"] + many_y * counts["y"]
                total += many_x * many_y * counts["both"]
                here_x = ends_x if many_x == 1 else jnp.logical_not(ends_x)
                here_y = ends_y if many_y == 1 else jnp.logical_not(ends_y)

                @pl.when(jnp.logical_and(here_x, here_y))
                def _():
                    action(total)

    def counted(total, part):
        block = tally.at[pl.ds(0, total)]
        return pltpu.make_async_remote_copy(
            src_ref=block,
            dst_ref=block,
            send_sem=halo_send.at[0],
            recv_sem=halo_recv.at[part],
            device_id=partner,
            device_id_type=MESH,
        )

    def row_range(dx):
        if dx < 0:
            return pl.ds(OWN, HALO), pl.ds(OWN + rows, HALO)
        if dx > 0:
            return pl.ds(OWN + rows - HALO, HALO), pl.ds(TOP, HALO)
        return pl.ds(OWN, rows), pl.ds(OWN, rows)

    hands = []
    for axis, count in (("plane", planes), ("planey", planeys)):
        reach = 1
        while reach * 2 <= count // 2:
            hands.append((reach, axis))
            reach *= 2
    hands.sort()

    def greet(number):
        reach, axis = hands[number]
        for step in (-reach, reach):
            target = at(step, 0) if axis == "plane" else at(0, step)
            pl.semaphore_signal(
                hand_sem.at[number], inc=1, device_id=target, device_id_type=MESH
            )

    def greeted(number):
        pl.semaphore_wait(hand_sem.at[number], 2)

    def greet_round(reach):
        for number, (distance, _) in enumerate(hands):
            if distance == reach:
                greet(number)

    def greeted_round(reach):
        for number, (distance, _) in enumerate(hands):
            if distance == reach:
                greeted(number)

    lane = lax.broadcasted_iota(jnp.int32, (rows, cols), 1)
    group = lane // PITCH

    def lane_packed(planes_of):
        packed = jnp.zeros((rows, cols), jnp.float32)
        for layer in range(layers):
            turned = pltpu.roll(planes_of(layer), (PITCH * layer + HALO) % cols, 1)
            packed = jnp.where(group == layer, turned, packed)
        return packed

    body = pl.ds(1, layers)

    def send_u(part, member):
        for dx in (-1, 1):
            here, there = row_range(dx)
            send(
                part,
                dx,
                0,
                (uw.at[member, :, body, here, :], uw.at[member, :, body, there, :]),
            )

    def pack_u(member):
        for comp in range(comps):
            xo[u_field(member) + comp, OWN : OWN + rows, :] = lane_packed(
                lambda layer: uw[member, comp, 1 + layer, OWN : OWN + rows, :]
            )

    def send_packed(part, low, count, map_low, map_count):
        fields_here = pl.ds(low, count)
        maps_here = pl.ds(map_low, map_count)
        for dx, dy in sorted(around, key=lambda d: -abs(d[0])):
            here, there = row_range(dx)
            target = xo if dy == 0 else (xr if dy < 0 else xl)
            pairs = [(xo.at[fields_here, here, :], target.at[fields_here, there, :])]
            if dy == 0:
                pairs.append((mw.at[maps_here, here, :], mw.at[maps_here, there, :]))
            send(part, dx, dy, *pairs)

    with scope("p0_load"):
        load_u[0].wait()
    with scope("p1_barrier"):
        pl.semaphore_wait(barrier, len(around) + 1)
    send_u(0, 0)
    block = tally.at[pl.ds(0, maps_rows)]
    pltpu.make_async_copy(block, block, local_sem.at[members + 1]).wait()
    load_picks.wait()
    mask_own = mask_in[...].astype(jnp.float32)
    bed_own = bed_in[...].astype(jnp.float32) * bed_unit
    mw[0, OWN : OWN + rows, :] = mask_own
    xo[MASK, OWN : OWN + rows, :] = lane_packed(lambda layer: mask_own)
    pack_u(0)
    send_packed(0, 0, 1 + comps, 0, 1)
    greet_round(1)
    mw[1, OWN : OWN + rows, :] = bed_own
    xo[bed_field, OWN : OWN + rows, :] = lane_packed(lambda layer: bed_own)
    for member in range(members):
        chosen = table[picks[member]]
        mw[2 + member, OWN : OWN + rows, :] = chosen
        xo[friction_field(member), OWN : OWN + rows, :] = jnp.where(
            lane < PITCH, pltpu.roll(chosen, HALO, 1), 0.0
        )
    send_packed(1, bed_field, 2, 1, 2)
    for member in range(1, members):
        load_u[member].wait()
        send_u(1 + member, member)
        pack_u(member)
        send_packed(1 + member, friction_field(member), 1 + comps, 2 + member, 1)

    with scope("p3_greeted1"):
        greeted_round(1)
    greet_round(2)
    with scope("p5_greeted2"):
        greeted_round(2)
    greet_round(4)
    pl.semaphore_signal(
        hand_sem.at[len(hands)], inc=1, device_id=partner, device_id_type=MESH
    )

    def arrived(part):
        with scope("p4_halo%d" % part):
            each_total(rows_of[part], lambda total: counted(total, part).wait_recv())

    bf16 = jnp.bfloat16
    apart = lax.broadcasted_iota(jnp.int32, (cols, cols), 0) - lax.broadcasted_iota(
        jnp.int32, (cols, cols), 1
    )

    def at_steps(step):
        return jnp.where(apart == step, 1.0, 0.0)

    near_z = at_steps(PITCH) + at_steps(-PITCH)
    corners = (
        at_steps(PITCH + 1) + at_steps(PITCH - 1) + at_steps(1 - PITCH) + at_steps(-PITCH - 1)
    )
    near_y = at_steps(1) + at_steps(-1)
    lane_sums = [
        at_steps(0)
        + along_y[comp] * near_y
        + along_z * near_z
        + along_y[comp] * along_z * corners
        for comp in range(comps)
    ]
    lane_steps = [at_steps(1) - at_steps(-1), at_steps(PITCH) - at_steps(-PITCH)]
    for number, matrix in enumerate(lane_sums + lane_steps):
        matrix = matrix.astype(bf16)
        lane_matrix[number, :cols, :] = matrix
        lane_matrix[number, cols:, :] = matrix

    arrived(0)

    lane = lax.broadcasted_iota(jnp.int32, (wide, cols), 1)
    first_lane = lane == 0
    last_lane = lane == cols - 1
    spot = lax.rem(lane, PITCH)
    outer_left = spot < HALO
    left_edge = spot == HALO - 1
    position = (
        plane * rows - HALO + lax.broadcasted_iota(jnp.int32, (wide, cols), 0)
    ).astype(jnp.float32)
    thickness = 1.0 + 2.0 * position / (rows * planes - 1)

    def sides(number, low=TOP, high=end):
        own = xo[number, low:high, :]
        return (
            jnp.where(outer_left, xl[number, low:high, :], own),
            jnp.where(outer_left, own, xr[number, low:high, :]),
        )

    def edges(pair):
        left, right = pair
        return jnp.where(
            left_edge, pltpu.roll(right, cols - 1, 1), pltpu.roll(left, 1, 1)
        )

    def y_pair(value, near):
        return (
            jnp.where(last_lane, near, pltpu.roll(value, cols - 1, 1)),
            jnp.where(first_lane, near, pltpu.roll(value, 1, 1)),
        )

    def turned_edge(value, layer):
        return pltpu.roll(value, cols - HALO - PITCH * layer, 1)

    mask_main = mw[0, TOP:end, :]
    fixed[0] = mask_main
    for side, mask_here in enumerate(sides(MASK)):
        fixed[3 + side] = mask_here

    def forces():
        bed_pair = sides(bed_field)
        bed_plus, bed_minus = y_pair(mw[1, TOP:end, :], turned_edge(edges(bed_pair), 0))
        scale = -(fixed[0] * thickness)
        fixed[1] = scale * (
            (mw[1, TOP + 1 : end + 1, :] - mw[1, TOP - 1 : end - 1, :]) * 0.5
        )
        fixed[2] = scale * ((bed_plus - bed_minus) * 0.5)
        for side, bed_here in enumerate(bed_pair):
            shifted[side, TOP:end, :] = bed_here
            down = shifted[side, TOP + 1 : end + 1, :] - shifted[side, TOP - 1 : end - 1, :]
            flat = pltpu.roll(bed_here, cols - 1, 1) - pltpu.roll(bed_here, 1, 1)
            scale = -(fixed[3 + side] * thickness)
            fixed[5 + side] = scale * (down * 0.5)
            fixed[7 + side] = scale * (flat * 0.5)

    def power(strain4):
        return jnp.exp(jnp.log(strain4 * 0.25 + 0.1) * (-1.0 / 6.0))

    def strain4_of(ui, vi, uj, vj, uz, vz):
        shear = uj + vi
        return ui * ui + vj * vj + ui * vj + 0.25 * (shear * shear + (uz * uz + vz * vz))

    def lane_halves(values):
        stacked = jnp.concatenate(values, axis=0)
        high = stacked.astype(bf16)
        low = (stacked - high.astype(jnp.float32)).astype(bf16)
        return jnp.concatenate([high, low], axis=1)

    def lane_product(halves, number):
        product = jnp.dot(
            halves, lane_matrix[number], preferred_element_type=jnp.float32
        )
        return [product[low : low + wide] for low in range(0, product.shape[0], wide)]

    def strip_k(pair, comp, slot):
        result = []
        for side, value in enumerate(lane_product(lane_halves(pair), comp)):
            shifted[slot + side, TOP:end, :] = value
            result.append(
                value
                + along_x[comp]
                * (
                    shifted[slot + side, TOP + 1 : end + 1, :]
                    + shifted[slot + side, TOP - 1 : end - 1, :]
                )
            )
        return result

    own_top = lax.broadcasted_iota(jnp.int32, (8, cols), 0) >= HALO

    def own_sum(value):
        total = jnp.where(own_top, value[:8], value[wide - 8 :])
        for low in range(8, wide - 8, 8):
            total = total + value[low : low + 8]
        return total

    def strip_start(member):
        for comp in range(comps):
            pair = sides(u_field(member) + comp)
            edge[EDGE_U + comp] = edges(pair)
            for side in range(2):
                strip[comp * 2 + side, TOP:end, :] = pair[side]
        strip_roots = []
        halves = lane_halves([strip[k, TOP:end, :] for k in range(2 * comps)])
        steps_j = lane_product(halves, comps)
        steps_z = lane_product(halves, comps + 1)
        for side in range(2):
            step_i = [
                strip[comp * 2 + side, TOP + 1 : end + 1, :]
                - strip[comp * 2 + side, TOP - 1 : end - 1, :]
                for comp in range(comps)
            ]
            step_j = [steps_j[comp * 2 + side] for comp in range(comps)]
            step_z = [steps_z[comp * 2 + side] for comp in range(comps)]
            strip_roots.append(
                fixed[3 + side]
                * power(
                    strain4_of(
                        step_i[0], step_i[1], step_j[0], step_j[1], step_z[0], step_z[1]
                    )
                )
            )
            strip_kept[side] = strip_roots[side]
        edge[EDGE_R] = edges(strip_roots)
        for comp in range(comps):
            around_roots = strip_k(strip_roots, comp, comp * 2)
            field = [
                strip_roots[side] * (fixed[3 + side] * strip[comp * 2 + side, TOP:end, :])
                for side in range(2)
            ]
            edge[EDGE_0 + comp] = edges(field)
            near = strip_k(field, comp, 4 + comp * 2)
            for side in range(2):
                strip_kept[2 + 4 * comp + side] = around_roots[side]
                strip_kept[4 + 4 * comp + side] = near[side]

    def strip_end(member):
        strip_roots = [strip_kept[side] for side in range(2)]
        four = [4.0 * root for root in strip_roots]
        friction_pair = sides(friction_field(member))
        diag = [
            fixed[3 + side] * friction_pair[side] + (1.0 - fixed[3 + side])
            for side in range(2)
        ]
        for comp in range(comps):
            main = [
                four[side] * strip_kept[2 + 4 * comp + side] + diag[side]
                for side in range(2)
            ]
            residual = [
                fixed[5 + 2 * comp + side]
                - (
                    main[side] * (fixed[3 + side] * strip[comp * 2 + side, TOP:end, :])
                    - four[side] * strip_kept[4 + 4 * comp + side]
                )
                for side in range(2)
            ]
            field = [strip_roots[side] * residual[side] for side in range(2)]
            edge[EDGE_1 + comp] = edges(field)
            near = strip_k(field, comp, comp * 2)
            image = [
                main[side] * residual[side] - four[side] * near[side] for side in range(2)
            ]
            edge[EDGE_2 + comp] = edges([strip_roots[side] * image[side] for side in range(2)])

    def share_start(member):
        for comp in range(comps):
            for layer in range(layers):
                plus, minus = y_pair(
                    uw[member, comp, layer + 1, TOP:end, :],
                    turned_edge(edge[EDGE_U + comp], layer),
                )
                step_y[comp, layer] = plus - minus
        for layer in range(layers):
            step_i = [
                uw[member, comp, layer + 1, TOP + 1 : end + 1, :]
                - uw[member, comp, layer + 1, TOP - 1 : end - 1, :]
                for comp in range(comps)
            ]
            step_z = [
                uw[member, comp, layer + 2, TOP:end, :] - uw[member, comp, layer, TOP:end, :]
                for comp in range(comps)
            ]
            roots[layer] = fixed[0] * power(
                strain4_of(
                    step_i[0],
                    step_i[1],
                    step_y[0, layer],
                    step_y[1, layer],
                    step_z[0],
                    step_z[1],
                )
            )
        for layer in range(layers):
            root = roots[layer]
            plus, minus = y_pair(root, turned_edge(edge[EDGE_R], layer))
            both = plus + minus
            for comp in range(comps):
                tr[comp, layer + 1, TOP:end, :] = root + along_y[comp] * both
                field = root * (fixed[0] * uw[member, comp, layer + 1, TOP:end, :])
                plus, minus = y_pair(field, turned_edge(edge[EDGE_0 + comp], layer))
                tp[comp, layer + 1, TOP:end, :] = field + along_y[comp] * (plus + minus)

    def x_sum(buffer, comp, layer):
        return buffer[comp, layer, TOP:end, :] + along_x[comp] * (
            buffer[comp, layer, TOP + 1 : end + 1, :]
            + buffer[comp, layer, TOP - 1 : end - 1, :]
        )

    def share_end(member):
        slot = members * ens + member
        empty = jnp.zeros((wide, cols), jnp.float32)

        def residual_layer(layer, carry):
            before, now, total = carry
            root = roots[layer]
            four = 4.0 * root
            here = fixed[0]
            bottom = jnp.where(layer == 0, 1.0, 0.0)
            diag = here * mw[2 + member, TOP:end, :] * bottom + (1.0 - here)
            after = []
            for comp in range(comps):
                after_r = x_sum(tr, comp, layer + 2)
                after_p = x_sum(tp, comp, layer + 2)
                after += [after_r, after_p]
                around_roots = now[2 * comp] + along_z * (before[2 * comp] + after_r)
                near = now[2 * comp + 1] + along_z * (before[2 * comp + 1] + after_p)
                main = four * around_roots + diag
                start = here * uw[member, comp, layer + 1, TOP:end, :]
                residual = fixed[1 + comp] - (main * start - four * near)
                field_a[comp, layer] = main
                all_residual[slot, comp, layer] = residual
                total = total + own_sum(residual * residual)
                field = root * residual
                plus, minus = y_pair(field, turned_edge(edge[EDGE_1 + comp], layer))
                tq[comp, layer + 1, TOP:end, :] = field + along_y[comp] * (plus + minus)
            return tuple(now), tuple(after), total

        nothing = jnp.zeros((8, cols), jnp.float32)
        first = tuple(
            x_sum(buffer, comp, 1) for comp in range(comps) for buffer in (tr, tp)
        )
        with scope("q2_residual"):
            _, _, gram_rr = lax.fori_loop(
                0, layers, residual_layer, ((empty,) * 4, first, nothing), unroll=UNROLL
            )

        def image_layer(layer, carry):
            before, now, total_ra, total_aa = carry
            root = roots[layer]
            four = 4.0 * root
            after = []
            for comp in range(comps):
                after_p = x_sum(tq, comp, layer + 2)
                after.append(after_p)
                near = now[comp] + along_z * (before[comp] + after_p)
                residual = all_residual[slot, comp, layer]
                image = field_a[comp, layer] * residual - four * near
                all_image[slot, comp, layer] = image
                total_ra = total_ra + own_sum(residual * image)
                total_aa = total_aa + own_sum(image * image)
                field = root * image
                plus, minus = y_pair(field, turned_edge(edge[EDGE_2 + comp], layer))
                tp[comp, layer + 1, TOP:end, :] = field + along_y[comp] * (plus + minus)
            return tuple(now), tuple(after), total_ra, total_aa

        first = tuple(x_sum(tq, comp, 1) for comp in range(comps))
        with scope("q3_image"):
            _, _, gram_ra, gram_aa = lax.fori_loop(
                0,
                layers,
                image_layer,
                ((empty,) * 2, first, nothing, nothing),
                unroll=UNROLL,
            )

        def own_x_sum(comp, layer):
            return tp[comp, layer, OWN : OWN + rows, :] + along_x[comp] * (
                tp[comp, layer, OWN + 1 : OWN + rows + 1, :]
                + tp[comp, layer, OWN - 1 : OWN + rows - 1, :]
            )

        def second_layer(layer, carry):
            before, now, total = carry
            four = 4.0 * roots[layer, HALO : HALO + rows, :]
            after = []
            for comp in range(comps):
                after_p = own_x_sum(comp, layer + 2)
                after.append(after_p)
                near = now[comp] + along_z * (before[comp] + after_p)
                image = all_image[slot, comp, layer, HALO : HALO + rows, :]
                second = (
                    field_a[comp, layer, HALO : HALO + rows, :] * image - four * near
                )
                product = image * second
                for low in range(0, rows, 8):
                    total = total + product[low : low + 8]
            return tuple(now), tuple(after), total

        empty_own = jnp.zeros((rows, cols), jnp.float32)
        first = tuple(own_x_sum(comp, 1) for comp in range(comps))
        with scope("q4_second"):
            _, _, gram_ab = lax.fori_loop(
                0, layers, second_layer, ((empty_own,) * 2, first, nothing), unroll=UNROLL
            )
        for number, value in enumerate((gram_rr, gram_ra, gram_aa, gram_ab)):
            gram[4 * member + number] = value

    def to_partner(block):
        pltpu.make_async_remote_copy(
            src_ref=block,
            dst_ref=block,
            send_sem=pair_send.at[0],
            recv_sem=pair_recv.at[0],
            device_id=partner,
            device_id_type=MESH,
        ).start()

    inner = pl.ds(HALO, rows)

    def share_member(member):
        slot = members * ens + member
        for buffer in (all_residual, all_image):
            to_partner(buffer.at[slot, :, :, inner, :])

    for member in range(members):
        if member > 0:
            arrived(1 + member)
        with scope("q0_start"):
            strip_start(member)
            share_start(member)
        if member == 0:
            arrived(1)
            forces()
        with scope("q1_end"):
            strip_end(member)
            share_end(member)
        if member < members - 1:
            share_member(member)

    lines = 4 * members
    total = jnp.sum(gram[...], axis=1)
    total = jnp.sum(total, axis=1, keepdims=True)
    lane = lax.broadcasted_iota(jnp.int32, (lines, cols), 1)
    line = lax.broadcasted_iota(jnp.int32, (lines, cols), 0)
    message = jnp.sum(
        jnp.where(lane == line + lines * ens, total, 0.0), axis=0, keepdims=True
    )
    with scope("p7_hand"):
        pl.semaphore_wait(hand_sem.at[len(hands)], 1)

    def exchange(ring, me, count, target, send_sem, recv_sem, value, sign=-1):
        ring[me] = value
        for offset in sorted(range(1, count), key=lambda k: sign * min(k, count - k)):
            pltpu.make_async_remote_copy(
                src_ref=ring.at[me],
                dst_ref=ring.at[me],
                send_sem=send_sem.at[0],
                recv_sem=recv_sem.at[0],
                device_id=target(lax.rem(me + offset, count)),
                device_id_type=MESH,
            ).start()
        return pltpu.make_async_remote_copy(
            src_ref=ring.at[pl.ds(0, count - 1)],
            dst_ref=ring.at[pl.ds(0, count - 1)],
            send_sem=send_sem.at[0],
            recv_sem=recv_sem.at[0],
            device_id=target(lax.rem(me + 1, count)),
            device_id_type=MESH,
        )

    cores = 2
    copies_y = exchange(
        ring_y,
        planey * cores + ens,
        planeys * cores,
        lambda peer: {"planey": peer // cores, "ens": lax.rem(peer, cores)},
        y_send,
        y_recv,
        message,
    )

    share_member(members - 1)
    for comp in range(comps):
        for layer in range(layers):
            total = None
            for member in range(members):
                start = mw[0, OWN : OWN + rows, :] * uw[member, comp, layer + 1, OWN : OWN + rows, :]
                total = start if total is None else total + start
            all_start[ens, comp, layer] = total
    to_partner(all_start.at[ens])
    everything = {
        name: sum(counts[name] for counts in rows_of) for name in ("x", "y", "both")
    }
    each_total(everything, lambda total: counted(total, 0).wait_send())
    with scope("p8_ary"):
        copies_y.wait_recv()
    with scope("p6_greeted4"):
        for reach in (4, 8, 16):
            greeted_round(reach)
            if reach > 2:
                greet_round(2 * reach)
    copies_x = exchange(
        ring_x,
        plane,
        planes,
        lambda peer: {"plane": peer},
        x_send,
        x_recv,
        jnp.sum(ring_y[...], axis=0),
        sign=1,
    )
    copies_y.wait_send()
    block = all_residual.at[:, :, :, pl.ds(0, (2 * members + 1) * rows // (2 * members)), :]
    fields = pltpu.make_async_remote_copy(
        src_ref=block,
        dst_ref=block,
        send_sem=pair_send.at[0],
        recv_sem=pair_recv.at[0],
        device_id=partner,
        device_id_type=MESH,
    )
    fields.wait_send()
    fields.wait_recv()
    with scope("p9_arx"):
        copies_x.wait_recv()
    sums = jnp.sum(ring_x[...], axis=0)
    gram_rr = sums
    gram_ra = pltpu.roll(sums, cols - 1, 1)
    gram_aa = pltpu.roll(sums, cols - 2, 1)
    gram_ab = pltpu.roll(sums, cols - 3, 1)
    first_step = gram_rr / gram_ra
    norm_next = gram_rr - 2.0 * first_step * gram_ra + first_step * first_step * gram_aa
    growth = 1.0 + norm_next / gram_rr
    curve = (
        growth * growth * gram_ra
        - 2.0 * growth * first_step * gram_aa
        + first_step * first_step * gram_ab
    )
    second_step = norm_next / curve
    samples = members * cores
    share = 1.0 / samples
    for_residual = share * (first_step + second_step * growth)
    for_image = share * (second_step * first_step)
    lane = lax.broadcasted_iota(jnp.int32, (1, cols), 1)

    def pick(value, number):
        return jnp.sum(jnp.where(lane == 4 * number, value, 0.0), axis=1, keepdims=True)

    weights = [(pick(for_residual, k), pick(for_image, k)) for k in range(samples)]

    def combine(layer, carry):
        for comp in range(comps):
            total = share * (all_start[0, comp, layer] + all_start[1, comp, layer])
            for number in range(samples):
                total = total + (
                    weights[number][0] * all_residual[number, comp, layer, HALO : HALO + rows, :]
                    - weights[number][1] * all_image[number, comp, layer, HALO : HALO + rows, :]
                )
            out[comp, layer] = total
        return carry

    with scope("pa_combine"):
        lax.fori_loop(0, layers, combine, 0, unroll=UNROLL)
    with scope("pb_sent"):
        copies_x.wait_send()


def body(sizes, u_prior, friction_rows, friction_table, bed_fixed, ice_mask):
    planes, planeys = sizes
    members, comps, layers, rows, cols = u_prior.shape
    wide = rows + 2 * HALO
    deep = rows + 24
    samples = 2 * members
    f32 = jnp.float32
    anywhere = pl.BlockSpec(memory_space=pltpu.HBM)
    fields = 2 + members * (1 + comps)
    vmem = pltpu.VMEM
    dma = pltpu.SemaphoreType.DMA
    return pl.pallas_call(
        functools.partial(kernel, sizes),
        out_shape=jax.ShapeDtypeStruct((comps, layers, rows, cols), f32),
        in_specs=[anywhere] * 5,
        out_specs=pl.BlockSpec(memory_space=pltpu.VMEM),
        scratch_shapes=[
            vmem((members, comps, layers + 2, deep, cols), f32),
            vmem((2 + members, deep, cols), f32),
            vmem((fields, deep, cols), f32),
            vmem((fields, deep, cols), f32),
            vmem((fields, deep, cols), f32),
            vmem(friction_table.shape, f32),
            vmem((rows, cols), jnp.int32),
            vmem((rows, cols), jnp.int32),
            pltpu.SMEM((members,), jnp.int32),
            vmem((2 * comps, deep, cols), f32),
            vmem((4 * comps, deep, cols), f32),
            vmem((2 + 4 * comps, wide, cols), f32),
            vmem((4, 2 * cols, cols), jnp.bfloat16),
            vmem((1536, cols), f32),
            vmem((9, wide, cols), f32),
            vmem((9, wide, cols), f32),
            vmem((layers, wide, cols), f32),
            vmem((comps, layers, wide, cols), f32),
            vmem((comps, layers + 2, deep, cols), f32),
            vmem((comps, layers + 2, deep, cols), f32),
            vmem((comps, layers + 2, deep, cols), f32),
            vmem((comps, layers, wide, cols), f32),
            vmem((samples, comps, layers, wide, cols), f32),
            vmem((samples, comps, layers, wide, cols), f32),
            vmem((2, comps, layers, rows, cols), f32),
            vmem((4 * members, 8, cols), f32),
            vmem((2 * planeys, 1, cols), f32),
            vmem((planes, 1, cols), f32),
            dma((members + 2,)),
            dma((1,)),
            dma((1 + members,)),
            pltpu.SemaphoreType.REGULAR((6,)),
            dma((1,)),
            dma((1,)),
            dma((1,)),
            dma((1,)),
            dma((1,)),
            dma((1,)),
        ],
        compiler_params=pltpu.CompilerParams(
            collective_id=0, has_side_effects=True, vmem_limit_bytes=48 * 1024 * 1024
        ),
    )(*[
        pltpu.with_memory_space_constraint(x, pltpu.HBM)
        for x in (u_prior, friction_rows, friction_table, bed_fixed, ice_mask)
    ])


def solution(mesh):
    in_specs = (
        P(("group", "ens"), None, None, "plane", "planey"),
        P(("group", "ens")),
        P("group", "plane", "planey"),
        P("plane", "planey"),
        P("plane", "planey"),
    )
    out_specs = P("group", None, "plane", "planey")
    sizes = (mesh.shape["plane"], mesh.shape["planey"])
    return jax.shard_map(
        functools.partial(body, sizes),
        mesh=mesh,
        in_specs=in_specs,
        out_specs=out_specs,
        check_vma=False,
    )
```

```python
import contextlib
import functools

import jax
import jax.numpy as jnp
from jax import lax
from jax.experimental import pallas as pl
from jax.experimental.pallas import tpu as pltpu
from jax.sharding import PartitionSpec as P

bed_unit = 2.0 ** (-29)
HALO = 4
TOP = 8
OWN = TOP + HALO
PITCH = 8
MESH = pl.DeviceIdType.MESH
along_z = 0.5
along_x = (0.25, 0.125)
along_y = (0.125, 0.25)
MASK = 0
UNROLL = 10


def scope(name):
    return contextlib.nullcontext()


EDGE_U, EDGE_R, EDGE_0, EDGE_1, EDGE_2 = 0, 2, 3, 5, 7


def kernel(
    sizes,
    u_hbm,
    picks_hbm,
    table_hbm,
    bed_hbm,
    mask_hbm,
    out,
    uw,
    mw,
    xo,
    xl,
    xr,
    table,
    bed_in,
    mask_in,
    picks,
    strip,
    shifted,
    strip_kept,
    lane_matrix,
    tally,
    edge,
    fixed,
    roots,
    step_y,
    tr,
    tp,
    tq,
    field_a,
    all_residual,
    all_image,
    all_start,
    gram,
    ring_y,
    ring_x,
    local_sem,
    halo_send,
    halo_recv,
    hand_sem,
    pair_send,
    pair_recv,
    y_send,
    y_recv,
    x_send,
    x_recv,
):
    planes, planeys = sizes
    members, comps, layers, rows, cols = u_hbm.shape
    wide = rows + 2 * HALO
    end = TOP + wide
    plane = lax.axis_index("plane")
    planey = lax.axis_index("planey")
    ens = lax.axis_index("ens")

    def at(dx, dy):
        return {
            "plane": lax.rem(plane + dx + planes, planes),
            "planey": lax.rem(planey + dy + planeys, planeys),
        }

    partner = {"ens": 1 - ens}
    around = [(dx, dy) for dx in (-1, 0, 1) for dy in (-1, 0, 1) if (dx, dy) != (0, 0)]

    def exists(dx, dy):
        flag = None
        for step, index, count in ((dx, plane, planes), (dy, planey, planeys)):
            if step != 0:
                part = index > 0 if step < 0 else index < count - 1
                flag = part if flag is None else jnp.logical_and(flag, part)
        return flag

    bed_field = 1 + comps

    def friction_field(member):
        return bed_field + 1 + member * (1 + comps) - (comps if member > 0 else 0)

    def u_field(member):
        return 1 if member == 0 else friction_field(member) + 1

    def load_member(member):
        return pltpu.make_async_copy(
            u_hbm.at[member],
            uw.at[member, :, pl.ds(1, layers), pl.ds(OWN, rows), :],
            local_sem.at[member],
        )

    load_u = [load_member(member) for member in range(members)]
    load_picks = pltpu.make_async_copy(picks_hbm, picks, local_sem.at[members])
    load_maps = [
        pltpu.make_async_copy(source, target, local_sem.at[members + 1])
        for source, target in ((table_hbm, table), (bed_hbm, bed_in), (mask_hbm, mask_in))
    ]
    maps_rows = (table.shape[0] + 2) * rows
    for load in (load_u[0], load_picks, *load_maps, *load_u[1:]):
        load.start()

    barrier = pltpu.get_barrier_semaphore()
    for dx, dy in around:
        pl.semaphore_signal(barrier, inc=1, device_id=at(dx, dy), device_id_type=MESH)
    pl.semaphore_signal(barrier, inc=1, device_id=partner, device_id_type=MESH)

    for end_layer in (0, layers + 1):
        uw[:, :, end_layer, TOP:end, :] = jnp.zeros((members, comps, wide, cols), jnp.float32)
        for buffer in (tr, tp, tq):
            buffer[:, end_layer] = jnp.zeros(buffer.shape[:1] + buffer.shape[2:], jnp.float32)
    for step, first in ((-1, TOP), (1, OWN + rows)):

        @pl.when(jnp.logical_not(exists(step, 0)))
        def _():
            uw[:, :, 1 : 1 + layers, first : first + HALO, :] = jnp.zeros(
                (members, comps, layers, HALO, cols), jnp.float32
            )
            for buffer in (mw, xo, xl, xr):
                buffer[:, first : first + HALO, :] = jnp.zeros(
                    (buffer.shape[0], HALO, cols), jnp.float32
                )

    for step, buffer in ((-1, xl), (1, xr)):

        @pl.when(jnp.logical_not(exists(0, step)))
        def _():
            buffer[:, TOP:end, :] = jnp.zeros((buffer.shape[0], wide, cols), jnp.float32)

    def kind(dx, dy):
        return "both" if dx != 0 and dy != 0 else ("x" if dx != 0 else "y")

    def send(part, dx, dy, *pairs):
        copies = [
            pltpu.make_async_remote_copy(
                src_ref=source,
                dst_ref=target,
                send_sem=halo_send.at[0],
                recv_sem=halo_recv.at[part],
                device_id=at(dx, dy),
                device_id_type=MESH,
            )
            for source, target in pairs
        ]

        @pl.when(exists(dx, dy))
        def _():
            for copy in copies:
                copy.start()

        if dx >= 0 and dy >= 0:
            for source, _ in pairs:
                count = 1
                for size in source.shape[:-1]:
                    count *= size
                rows_of[part][kind(dx, dy)] += count

    rows_of = [{"x": 0, "y": 0, "both": 0} for _ in range(2 + members)]

    def each_total(counts, action):
        ends_x = jnp.logical_or(plane == 0, plane == planes - 1)
        ends_y = jnp.logical_or(planey == 0, planey == planeys - 1)
        for many_x in (1, 2):
            for many_y in (1, 2):
                total = many_x * counts["x"] + many_y * counts["y"]
                total += many_x * many_y * counts["both"]
                here_x = ends_x if many_x == 1 else jnp.logical_not(ends_x)
                here_y = ends_y if many_y == 1 else jnp.logical_not(ends_y)

                @pl.when(jnp.logical_and(here_x, here_y))
                def _():
                    action(total)

    def counted(total, part):
        block = tally.at[pl.ds(0, total)]
        return pltpu.make_async_remote_copy(
            src_ref=block,
            dst_ref=block,
            send_sem=halo_send.at[0],
            recv_sem=halo_recv.at[part],
            device_id=partner,
            device_id_type=MESH,
        )

    def row_range(dx):
        if dx < 0:
            return pl.ds(OWN, HALO), pl.ds(OWN + rows, HALO)
        if dx > 0:
            return pl.ds(OWN + rows - HALO, HALO), pl.ds(TOP, HALO)
        return pl.ds(OWN, rows), pl.ds(OWN, rows)

    hands = []
    for axis, count in (("plane", planes), ("planey", planeys)):
        reach = 1
        while reach * 2 <= count // 2:
            hands.append((reach, axis))
            reach *= 2
    hands.sort()

    def greet(number):
        reach, axis = hands[number]
        for step in (-reach, reach):
            target = at(step, 0) if axis == "plane" else at(0, step)
            pl.semaphore_signal(
                hand_sem.at[number], inc=1, device_id=target, device_id_type=MESH
            )

    def greeted(number):
        pl.semaphore_wait(hand_sem.at[number], 2)

    def greet_round(reach):
        for number, (distance, _) in enumerate(hands):
            if distance == reach:
                greet(number)

    def greeted_round(reach):
        for number, (distance, _) in enumerate(hands):
            if distance == reach:
                greeted(number)

    lane = lax.broadcasted_iota(jnp.int32, (rows, cols), 1)
    group = lane // PITCH

    def lane_packed(planes_of):
        packed = jnp.zeros((rows, cols), jnp.float32)
        for layer in range(layers):
            turned = pltpu.roll(planes_of(layer), (PITCH * layer + HALO) % cols, 1)
            packed = jnp.where(group == layer, turned, packed)
        return packed

    body = pl.ds(1, layers)

    def send_u(part, member):
        for dx in (-1, 1):
            here, there = row_range(dx)
            send(
                part,
                dx,
                0,
                (uw.at[member, :, body, here, :], uw.at[member, :, body, there, :]),
            )

    def pack_u(member):
        for comp in range(comps):
            xo[u_field(member) + comp, OWN : OWN + rows, :] = lane_packed(
                lambda layer: uw[member, comp, 1 + layer, OWN : OWN + rows, :]
            )

    def send_packed(part, low, count, map_low, map_count):
        fields_here = pl.ds(low, count)
        maps_here = pl.ds(map_low, map_count)
        for dx, dy in sorted(around, key=lambda d: -abs(d[0])):
            here, there = row_range(dx)
            target = xo if dy == 0 else (xr if dy < 0 else xl)
            pairs = [(xo.at[fields_here, here, :], target.at[fields_here, there, :])]
            if dy == 0:
                pairs.append((mw.at[maps_here, here, :], mw.at[maps_here, there, :]))
            send(part, dx, dy, *pairs)

    with scope("p0_load"):
        load_u[0].wait()
    with scope("p1_barrier"):
        pl.semaphore_wait(barrier, len(around) + 1)
    block = tally.at[pl.ds(0, maps_rows)]
    pltpu.make_async_copy(block, block, local_sem.at[members + 1]).wait()
    load_picks.wait()
    mask_own = mask_in[...].astype(jnp.float32)
    bed_own = bed_in[...].astype(jnp.float32) * bed_unit
    mw[0, OWN : OWN + rows, :] = mask_own
    xo[MASK, OWN : OWN + rows, :] = lane_packed(lambda layer: mask_own)
    pack_u(0)
    send_packed(0, 0, 1 + comps, 0, 1)
    send_u(1 + members, 0)
    greet_round(1)
    mw[1, OWN : OWN + rows, :] = bed_own
    xo[bed_field, OWN : OWN + rows, :] = lane_packed(lambda layer: bed_own)
    for member in range(members):
        chosen = table[picks[member]]
        mw[2 + member, OWN : OWN + rows, :] = chosen
        xo[friction_field(member), OWN : OWN + rows, :] = jnp.where(
            lane < PITCH, pltpu.roll(chosen, HALO, 1), 0.0
        )
    send_packed(1, bed_field, 2, 1, 2)
    for member in range(1, members):
        load_u[member].wait()
        send_u(1 + member, member)
        pack_u(member)
        send_packed(1 + member, friction_field(member), 1 + comps, 2 + member, 1)

    with scope("p3_greeted1"):
        greeted_round(1)
    greet_round(2)

    def arrived(part):
        with scope("p4_halo%d" % part):
            each_total(rows_of[part], lambda total: counted(total, part).wait_recv())

    bf16 = jnp.bfloat16
    apart = lax.broadcasted_iota(jnp.int32, (cols, cols), 0) - lax.broadcasted_iota(
        jnp.int32, (cols, cols), 1
    )

    def at_steps(step):
        return jnp.where(apart == step, 1.0, 0.0)

    near_z = at_steps(PITCH) + at_steps(-PITCH)
    corners = (
        at_steps(PITCH + 1) + at_steps(PITCH - 1) + at_steps(1 - PITCH) + at_steps(-PITCH - 1)
    )
    near_y = at_steps(1) + at_steps(-1)
    lane_sums = [
        at_steps(0)
        + along_y[comp] * near_y
        + along_z * near_z
        + along_y[comp] * along_z * corners
        for comp in range(comps)
    ]
    lane_steps = [at_steps(1) - at_steps(-1), at_steps(PITCH) - at_steps(-PITCH)]
    for number, matrix in enumerate(lane_sums + lane_steps):
        matrix = matrix.astype(bf16)
        lane_matrix[number, :cols, :] = matrix
        lane_matrix[number, cols:, :] = matrix

    arrived(0)

    lane = lax.broadcasted_iota(jnp.int32, (wide, cols), 1)
    first_lane = lane == 0
    last_lane = lane == cols - 1
    spot = lax.rem(lane, PITCH)
    outer_left = spot < HALO
    left_edge = spot == HALO - 1
    position = (
        plane * rows - HALO + lax.broadcasted_iota(jnp.int32, (wide, cols), 0)
    ).astype(jnp.float32)
    thickness = 1.0 + 2.0 * position / (rows * planes - 1)

    def sides(number, low=TOP, high=end):
        own = xo[number, low:high, :]
        return (
            jnp.where(outer_left, xl[number, low:high, :], own),
            jnp.where(outer_left, own, xr[number, low:high, :]),
        )

    def edges(pair):
        left, right = pair
        return jnp.where(
            left_edge, pltpu.roll(right, cols - 1, 1), pltpu.roll(left, 1, 1)
        )

    def y_pair(value, near):
        return (
            jnp.where(last_lane, near, pltpu.roll(value, cols - 1, 1)),
            jnp.where(first_lane, near, pltpu.roll(value, 1, 1)),
        )

    def turned_edge(value, layer):
        return pltpu.roll(value, cols - HALO - PITCH * layer, 1)

    mask_main = mw[0, TOP:end, :]
    fixed[0] = mask_main
    for side, mask_here in enumerate(sides(MASK)):
        fixed[3 + side] = mask_here

    def forces():
        bed_pair = sides(bed_field)
        bed_plus, bed_minus = y_pair(mw[1, TOP:end, :], turned_edge(edges(bed_pair), 0))
        scale = -(fixed[0] * thickness)
        fixed[1] = scale * (
            (mw[1, TOP + 1 : end + 1, :] - mw[1, TOP - 1 : end - 1, :]) * 0.5
        )
        fixed[2] = scale * ((bed_plus - bed_minus) * 0.5)
        for side, bed_here in enumerate(bed_pair):
            shifted[side, TOP:end, :] = bed_here
            down = shifted[side, TOP + 1 : end + 1, :] - shifted[side, TOP - 1 : end - 1, :]
            flat = pltpu.roll(bed_here, cols - 1, 1) - pltpu.roll(bed_here, 1, 1)
            scale = -(fixed[3 + side] * thickness)
            fixed[5 + side] = scale * (down * 0.5)
            fixed[7 + side] = scale * (flat * 0.5)

    def power(strain4):
        return jnp.exp(jnp.log(strain4 * 0.25 + 0.1) * (-1.0 / 6.0))

    def strain4_of(ui, vi, uj, vj, uz, vz):
        shear = uj + vi
        return ui * ui + vj * vj + ui * vj + 0.25 * (shear * shear + (uz * uz + vz * vz))

    def lane_halves(values):
        stacked = jnp.concatenate(values, axis=0)
        high = stacked.astype(bf16)
        low = (stacked - high.astype(jnp.float32)).astype(bf16)
        return jnp.concatenate([high, low], axis=1)

    def lane_product(halves, number):
        product = jnp.dot(
            halves, lane_matrix[number], preferred_element_type=jnp.float32
        )
        return [product[low : low + wide] for low in range(0, product.shape[0], wide)]

    def strip_k(pair, comp, slot):
        result = []
        for side, value in enumerate(lane_product(lane_halves(pair), comp)):
            shifted[slot + side, TOP:end, :] = value
            result.append(
                value
                + along_x[comp]
                * (
                    shifted[slot + side, TOP + 1 : end + 1, :]
                    + shifted[slot + side, TOP - 1 : end - 1, :]
                )
            )
        return result

    own_top = lax.broadcasted_iota(jnp.int32, (8, cols), 0) >= HALO

    def own_sum(value):
        total = jnp.where(own_top, value[:8], value[wide - 8 :])
        for low in range(8, wide - 8, 8):
            total = total + value[low : low + 8]
        return total

    def strip_start(member):
        for comp in range(comps):
            pair = sides(u_field(member) + comp)
            edge[EDGE_U + comp] = edges(pair)
            for side in range(2):
                strip[comp * 2 + side, TOP:end, :] = pair[side]
        strip_roots = []
        halves = lane_halves([strip[k, TOP:end, :] for k in range(2 * comps)])
        steps_j = lane_product(halves, comps)
        steps_z = lane_product(halves, comps + 1)
        for side in range(2):
            step_i = [
                strip[comp * 2 + side, TOP + 1 : end + 1, :]
                - strip[comp * 2 + side, TOP - 1 : end - 1, :]
                for comp in range(comps)
            ]
            step_j = [steps_j[comp * 2 + side] for comp in range(comps)]
            step_z = [steps_z[comp * 2 + side] for comp in range(comps)]
            strip_roots.append(
                fixed[3 + side]
                * power(
                    strain4_of(
                        step_i[0], step_i[1], step_j[0], step_j[1], step_z[0], step_z[1]
                    )
                )
            )
            strip_kept[side] = strip_roots[side]
        edge[EDGE_R] = edges(strip_roots)
        for comp in range(comps):
            around_roots = strip_k(strip_roots, comp, comp * 2)
            field = [
                strip_roots[side] * (fixed[3 + side] * strip[comp * 2 + side, TOP:end, :])
                for side in range(2)
            ]
            edge[EDGE_0 + comp] = edges(field)
            near = strip_k(field, comp, 4 + comp * 2)
            for side in range(2):
                strip_kept[2 + 4 * comp + side] = around_roots[side]
                strip_kept[4 + 4 * comp + side] = near[side]

    def strip_end(member):
        strip_roots = [strip_kept[side] for side in range(2)]
        four = [4.0 * root for root in strip_roots]
        friction_pair = sides(friction_field(member))
        diag = [
            fixed[3 + side] * friction_pair[side] + (1.0 - fixed[3 + side])
            for side in range(2)
        ]
        for comp in range(comps):
            main = [
                four[side] * strip_kept[2 + 4 * comp + side] + diag[side]
                for side in range(2)
            ]
            residual = [
                fixed[5 + 2 * comp + side]
                - (
                    main[side] * (fixed[3 + side] * strip[comp * 2 + side, TOP:end, :])
                    - four[side] * strip_kept[4 + 4 * comp + side]
                )
                for side in range(2)
            ]
            field = [strip_roots[side] * residual[side] for side in range(2)]
            edge[EDGE_1 + comp] = edges(field)
            near = strip_k(field, comp, comp * 2)
            image = [
                main[side] * residual[side] - four[side] * near[side] for side in range(2)
            ]
            edge[EDGE_2 + comp] = edges([strip_roots[side] * image[side] for side in range(2)])

    def share_start(member):
        for comp in range(comps):
            for layer in range(layers):
                plus, minus = y_pair(
                    uw[member, comp, layer + 1, TOP:end, :],
                    turned_edge(edge[EDGE_U + comp], layer),
                )
                step_y[comp, layer] = plus - minus
        for layer in range(layers):
            step_i = [
                uw[member, comp, layer + 1, TOP + 1 : end + 1, :]
                - uw[member, comp, layer + 1, TOP - 1 : end - 1, :]
                for comp in range(comps)
            ]
            step_z = [
                uw[member, comp, layer + 2, TOP:end, :] - uw[member, comp, layer, TOP:end, :]
                for comp in range(comps)
            ]
            roots[layer] = fixed[0] * power(
                strain4_of(
                    step_i[0],
                    step_i[1],
                    step_y[0, layer],
                    step_y[1, layer],
                    step_z[0],
                    step_z[1],
                )
            )
        for layer in range(layers):
            root = roots[layer]
            plus, minus = y_pair(root, turned_edge(edge[EDGE_R], layer))
            both = plus + minus
            for comp in range(comps):
                tr[comp, layer + 1, TOP:end, :] = root + along_y[comp] * both
                field = root * (fixed[0] * uw[member, comp, layer + 1, TOP:end, :])
                plus, minus = y_pair(field, turned_edge(edge[EDGE_0 + comp], layer))
                tp[comp, layer + 1, TOP:end, :] = field + along_y[comp] * (plus + minus)

    def x_sum(buffer, comp, layer):
        return buffer[comp, layer, TOP:end, :] + along_x[comp] * (
            buffer[comp, layer, TOP + 1 : end + 1, :]
            + buffer[comp, layer, TOP - 1 : end - 1, :]
        )

    def spread_y(buffer, number):
        for layer in range(layers):
            for comp in range(comps):
                field = step_y[comp, layer]
                plus, minus = y_pair(field, turned_edge(edge[number + comp], layer))
                buffer[comp, layer + 1, TOP:end, :] = field + along_y[comp] * (plus + minus)

    def share_end(member):
        slot = members * ens + member
        empty = jnp.zeros((wide, cols), jnp.float32)

        def residual_layer(layer, carry):
            before, now, total = carry
            root = roots[layer]
            four = 4.0 * root
            here = fixed[0]
            bottom = jnp.where(layer == 0, 1.0, 0.0)
            diag = here * mw[2 + member, TOP:end, :] * bottom + (1.0 - here)
            after = []
            for comp in range(comps):
                after_r = x_sum(tr, comp, layer + 2)
                after_p = x_sum(tp, comp, layer + 2)
                after += [after_r, after_p]
                around_roots = now[2 * comp] + along_z * (before[2 * comp] + after_r)
                near = now[2 * comp + 1] + along_z * (before[2 * comp + 1] + after_p)
                main = four * around_roots + diag
                start = here * uw[member, comp, layer + 1, TOP:end, :]
                residual = fixed[1 + comp] - (main * start - four * near)
                field_a[comp, layer] = main
                all_residual[slot, comp, layer] = residual
                total = total + own_sum(residual * residual)
                step_y[comp, layer] = root * residual
            return tuple(now), tuple(after), total

        nothing = jnp.zeros((8, cols), jnp.float32)
        first = tuple(
            x_sum(buffer, comp, 1) for comp in range(comps) for buffer in (tr, tp)
        )
        with scope("q2_residual"):
            _, _, gram_rr = lax.fori_loop(
                0, layers, residual_layer, ((empty,) * 4, first, nothing), unroll=UNROLL
            )
            spread_y(tq, EDGE_1)

        def image_layer(layer, carry):
            before, now, total_ra, total_aa = carry
            root = roots[layer]
            four = 4.0 * root
            after = []
            for comp in range(comps):
                after_p = x_sum(tq, comp, layer + 2)
                after.append(after_p)
                near = now[comp] + along_z * (before[comp] + after_p)
                residual = all_residual[slot, comp, layer]
                image = field_a[comp, layer] * residual - four * near
                all_image[slot, comp, layer] = image
                total_ra = total_ra + own_sum(residual * image)
                total_aa = total_aa + own_sum(image * image)
                step_y[comp, layer] = root * image
            return tuple(now), tuple(after), total_ra, total_aa

        first = tuple(x_sum(tq, comp, 1) for comp in range(comps))
        with scope("q3_image"):
            _, _, gram_ra, gram_aa = lax.fori_loop(
                0,
                layers,
                image_layer,
                ((empty,) * 2, first, nothing, nothing),
                unroll=UNROLL,
            )
            spread_y(tp, EDGE_2)

        def own_x_sum(comp, layer):
            return tp[comp, layer, OWN : OWN + rows, :] + along_x[comp] * (
                tp[comp, layer, OWN + 1 : OWN + rows + 1, :]
                + tp[comp, layer, OWN - 1 : OWN + rows - 1, :]
            )

        def second_layer(layer, carry):
            before, now, total = carry
            four = 4.0 * roots[layer, HALO : HALO + rows, :]
            after = []
            for comp in range(comps):
                after_p = own_x_sum(comp, layer + 2)
                after.append(after_p)
                near = now[comp] + along_z * (before[comp] + after_p)
                image = all_image[slot, comp, layer, HALO : HALO + rows, :]
                second = (
                    field_a[comp, layer, HALO : HALO + rows, :] * image - four * near
                )
                product = image * second
                for low in range(0, rows, 8):
                    total = total + product[low : low + 8]
            return tuple(now), tuple(after), total

        empty_own = jnp.zeros((rows, cols), jnp.float32)
        first = tuple(own_x_sum(comp, 1) for comp in range(comps))
        with scope("q4_second"):
            _, _, gram_ab = lax.fori_loop(
                0, layers, second_layer, ((empty_own,) * 2, first, nothing), unroll=UNROLL
            )
        for number, value in enumerate((gram_rr, gram_ra, gram_aa, gram_ab)):
            gram[4 * member + number] = value

    def to_partner(block):
        pltpu.make_async_remote_copy(
            src_ref=block,
            dst_ref=block,
            send_sem=pair_send.at[0],
            recv_sem=pair_recv.at[0],
            device_id=partner,
            device_id_type=MESH,
        ).start()

    inner = pl.ds(HALO, rows)

    def share_member(member):
        slot = members * ens + member
        for buffer in (all_residual, all_image):
            to_partner(buffer.at[slot, :, :, inner, :])

    for member in range(members):
        if member > 0:
            arrived(1 + member)
        with scope("q0_start"):
            strip_start(member)
            if member == 0:
                arrived(1 + members)
            share_start(member)
        if member == 0:
            with scope("p5_greeted2"):
                greeted_round(2)
            greet_round(4)
            pl.semaphore_signal(
                hand_sem.at[len(hands)], inc=1, device_id=partner, device_id_type=MESH
            )
            arrived(1)
            forces()
        with scope("q1_end"):
            strip_end(member)
            share_end(member)
        if member < members - 1:
            share_member(member)

    lines = 4 * members
    total = jnp.sum(gram[...], axis=1)
    total = jnp.sum(total, axis=1, keepdims=True)
    lane = lax.broadcasted_iota(jnp.int32, (lines, cols), 1)
    line = lax.broadcasted_iota(jnp.int32, (lines, cols), 0)
    message = jnp.sum(
        jnp.where(lane == line + lines * ens, total, 0.0), axis=0, keepdims=True
    )
    with scope("p7_hand"):
        pl.semaphore_wait(hand_sem.at[len(hands)], 1)

    def exchange(ring, me, count, target, send_sem, recv_sem, value, sign=-1):
        ring[me] = value
        for offset in sorted(range(1, count), key=lambda k: sign * min(k, count - k)):
            pltpu.make_async_remote_copy(
                src_ref=ring.at[me],
                dst_ref=ring.at[me],
                send_sem=send_sem.at[0],
                recv_sem=recv_sem.at[0],
                device_id=target(lax.rem(me + offset, count)),
                device_id_type=MESH,
            ).start()
        return pltpu.make_async_remote_copy(
            src_ref=ring.at[pl.ds(0, count - 1)],
            dst_ref=ring.at[pl.ds(0, count - 1)],
            send_sem=send_sem.at[0],
            recv_sem=recv_sem.at[0],
            device_id=target(lax.rem(me + 1, count)),
            device_id_type=MESH,
        )

    cores = 2
    copies_y = exchange(
        ring_y,
        planey * cores + ens,
        planeys * cores,
        lambda peer: {"planey": peer // cores, "ens": lax.rem(peer, cores)},
        y_send,
        y_recv,
        message,
    )

    share_member(members - 1)
    for comp in range(comps):
        for layer in range(layers):
            total = None
            for member in range(members):
                start = mw[0, OWN : OWN + rows, :] * uw[member, comp, layer + 1, OWN : OWN + rows, :]
                total = start if total is None else total + start
            all_start[ens, comp, layer] = total
    to_partner(all_start.at[ens])
    everything = {
        name: sum(counts[name] for counts in rows_of) for name in ("x", "y", "both")
    }
    each_total(everything, lambda total: counted(total, 0).wait_send())
    with scope("p8_ary"):
        copies_y.wait_recv()
    with scope("p6_greeted4"):
        for reach in (4, 8, 16):
            greeted_round(reach)
            if reach > 2:
                greet_round(2 * reach)
    copies_x = exchange(
        ring_x,
        plane,
        planes,
        lambda peer: {"plane": peer},
        x_send,
        x_recv,
        jnp.sum(ring_y[...], axis=0),
        sign=1,
    )
    copies_y.wait_send()
    block = all_residual.at[:, :, :, pl.ds(0, (2 * members + 1) * rows // (2 * members)), :]
    fields = pltpu.make_async_remote_copy(
        src_ref=block,
        dst_ref=block,
        send_sem=pair_send.at[0],
        recv_sem=pair_recv.at[0],
        device_id=partner,
        device_id_type=MESH,
    )
    fields.wait_send()
    fields.wait_recv()
    with scope("p9_arx"):
        copies_x.wait_recv()
    sums = jnp.sum(ring_x[...], axis=0)
    gram_rr = sums
    gram_ra = pltpu.roll(sums, cols - 1, 1)
    gram_aa = pltpu.roll(sums, cols - 2, 1)
    gram_ab = pltpu.roll(sums, cols - 3, 1)
    first_step = gram_rr / gram_ra
    norm_next = gram_rr - 2.0 * first_step * gram_ra + first_step * first_step * gram_aa
    growth = 1.0 + norm_next / gram_rr
    curve = (
        growth * growth * gram_ra
        - 2.0 * growth * first_step * gram_aa
        + first_step * first_step * gram_ab
    )
    second_step = norm_next / curve
    samples = members * cores
    share = 1.0 / samples
    for_residual = share * (first_step + second_step * growth)
    for_image = share * (second_step * first_step)
    lane = lax.broadcasted_iota(jnp.int32, (1, cols), 1)

    def pick(value, number):
        return jnp.sum(jnp.where(lane == 4 * number, value, 0.0), axis=1, keepdims=True)

    weights = [(pick(for_residual, k), pick(for_image, k)) for k in range(samples)]

    def combine(layer, carry):
        for comp in range(comps):
            total = share * (all_start[0, comp, layer] + all_start[1, comp, layer])
            for number in range(samples):
                total = total + (
                    weights[number][0] * all_residual[number, comp, layer, HALO : HALO + rows, :]
                    - weights[number][1] * all_image[number, comp, layer, HALO : HALO + rows, :]
                )
            out[comp, layer] = total
        return carry

    with scope("pa_combine"):
        lax.fori_loop(0, layers, combine, 0, unroll=UNROLL)
    with scope("pb_sent"):
        copies_x.wait_send()


def body(sizes, u_prior, friction_rows, friction_table, bed_fixed, ice_mask):
    planes, planeys = sizes
    members, comps, layers, rows, cols = u_prior.shape
    wide = rows + 2 * HALO
    deep = rows + 24
    samples = 2 * members
    f32 = jnp.float32
    anywhere = pl.BlockSpec(memory_space=pltpu.HBM)
    fields = 2 + members * (1 + comps)
    vmem = pltpu.VMEM
    dma = pltpu.SemaphoreType.DMA
    return pl.pallas_call(
        functools.partial(kernel, sizes),
        out_shape=jax.ShapeDtypeStruct((comps, layers, rows, cols), f32),
        in_specs=[anywhere] * 5,
        out_specs=pl.BlockSpec(memory_space=pltpu.VMEM),
        scratch_shapes=[
            vmem((members, comps, layers + 2, deep, cols), f32),
            vmem((2 + members, deep, cols), f32),
            vmem((fields, deep, cols), f32),
            vmem((fields, deep, cols), f32),
            vmem((fields, deep, cols), f32),
            vmem(friction_table.shape, f32),
            vmem((rows, cols), jnp.int32),
            vmem((rows, cols), jnp.int32),
            pltpu.SMEM((members,), jnp.int32),
            vmem((2 * comps, deep, cols), f32),
            vmem((4 * comps, deep, cols), f32),
            vmem((2 + 4 * comps, wide, cols), f32),
            vmem((4, 2 * cols, cols), jnp.bfloat16),
            vmem((1536, cols), f32),
            vmem((9, wide, cols), f32),
            vmem((9, wide, cols), f32),
            vmem((layers, wide, cols), f32),
            vmem((comps, layers, wide, cols), f32),
            vmem((comps, layers + 2, deep, cols), f32),
            vmem((comps, layers + 2, deep, cols), f32),
            vmem((comps, layers + 2, deep, cols), f32),
            vmem((comps, layers, wide, cols), f32),
            vmem((samples, comps, layers, wide, cols), f32),
            vmem((samples, comps, layers, wide, cols), f32),
            vmem((2, comps, layers, rows, cols), f32),
            vmem((4 * members, 8, cols), f32),
            vmem((2 * planeys, 1, cols), f32),
            vmem((planes, 1, cols), f32),
            dma((members + 2,)),
            dma((1,)),
            dma((2 + members,)),
            pltpu.SemaphoreType.REGULAR((6,)),
            dma((1,)),
            dma((1,)),
            dma((1,)),
            dma((1,)),
            dma((1,)),
            dma((1,)),
        ],
        compiler_params=pltpu.CompilerParams(
            collective_id=0, has_side_effects=True, vmem_limit_bytes=48 * 1024 * 1024
        ),
    )(*[
        pltpu.with_memory_space_constraint(x, pltpu.HBM)
        for x in (u_prior, friction_rows, friction_table, bed_fixed, ice_mask)
    ])


def solution(mesh):
    in_specs = (
        P(("group", "ens"), None, None, "plane", "planey"),
        P(("group", "ens")),
        P("group", "plane", "planey"),
        P("plane", "planey"),
        P("plane", "planey"),
    )
    out_specs = P("group", None, "plane", "planey")
    sizes = (mesh.shape["plane"], mesh.shape["planey"])
    return jax.shard_map(
        functools.partial(body, sizes),
        mesh=mesh,
        in_specs=in_specs,
        out_specs=out_specs,
        check_vma=False,
    )
```

```python
import contextlib
import functools

import jax
import jax.numpy as jnp
from jax import lax
from jax.experimental import pallas as pl
from jax.experimental.pallas import tpu as pltpu
from jax.sharding import PartitionSpec as P

bed_unit = 2.0 ** (-29)
HALO = 4
TOP = 8
OWN = TOP + HALO
PITCH = 8
MESH = pl.DeviceIdType.MESH
along_z = 0.5
along_x = (0.25, 0.125)
along_y = (0.125, 0.25)
MASK = 0
UNROLL = 10


def scope(name):
    return contextlib.nullcontext()


EDGE_U, EDGE_R, EDGE_0, EDGE_1, EDGE_2 = 0, 2, 3, 5, 7


def kernel(
    sizes,
    u_hbm,
    picks_hbm,
    table_hbm,
    bed_hbm,
    mask_hbm,
    out,
    uw,
    mw,
    xo,
    xl,
    xr,
    table,
    bed_in,
    mask_in,
    picks,
    strip,
    shifted,
    strip_kept,
    lane_matrix,
    tally,
    edge,
    fixed,
    roots,
    step_y,
    tr,
    tp,
    tq,
    field_a,
    all_residual,
    all_image,
    all_start,
    gram,
    ring_y,
    ring_x,
    local_sem,
    halo_send,
    halo_recv,
    hand_sem,
    pair_send,
    pair_recv,
    y_send,
    y_recv,
    x_send,
    x_recv,
):
    planes, planeys = sizes
    members, comps, layers, rows, cols = u_hbm.shape
    wide = rows + 2 * HALO
    end = TOP + wide
    plane = lax.axis_index("plane")
    planey = lax.axis_index("planey")
    ens = lax.axis_index("ens")

    def at(dx, dy):
        return {
            "plane": lax.rem(plane + dx + planes, planes),
            "planey": lax.rem(planey + dy + planeys, planeys),
        }

    partner = {"ens": 1 - ens}
    around = [(dx, dy) for dx in (-1, 0, 1) for dy in (-1, 0, 1) if (dx, dy) != (0, 0)]

    def exists(dx, dy):
        flag = None
        for step, index, count in ((dx, plane, planes), (dy, planey, planeys)):
            if step != 0:
                part = index > 0 if step < 0 else index < count - 1
                flag = part if flag is None else jnp.logical_and(flag, part)
        return flag

    bed_field = 1 + comps

    def friction_field(member):
        return bed_field + 1 + member * (1 + comps) - (comps if member > 0 else 0)

    def u_field(member):
        return 1 if member == 0 else friction_field(member) + 1

    def load_member(member):
        return pltpu.make_async_copy(
            u_hbm.at[member],
            uw.at[member, :, pl.ds(1, layers), pl.ds(OWN, rows), :],
            local_sem.at[member],
        )

    load_u = [load_member(member) for member in range(members)]
    load_picks = pltpu.make_async_copy(picks_hbm, picks, local_sem.at[members])
    load_maps = [
        pltpu.make_async_copy(source, target, local_sem.at[members + 1])
        for source, target in ((table_hbm, table), (bed_hbm, bed_in), (mask_hbm, mask_in))
    ]
    maps_rows = (table.shape[0] + 2) * rows
    for load in (load_u[0], load_picks, *load_maps, *load_u[1:]):
        load.start()

    barrier = pltpu.get_barrier_semaphore()
    for dx, dy in around:
        pl.semaphore_signal(barrier, inc=1, device_id=at(dx, dy), device_id_type=MESH)
    pl.semaphore_signal(barrier, inc=1, device_id=partner, device_id_type=MESH)

    for end_layer in (0, layers + 1):
        uw[:, :, end_layer, TOP:end, :] = jnp.zeros((members, comps, wide, cols), jnp.float32)
        for buffer in (tr, tp, tq):
            buffer[:, end_layer] = jnp.zeros(buffer.shape[:1] + buffer.shape[2:], jnp.float32)
    for step, first in ((-1, TOP), (1, OWN + rows)):

        @pl.when(jnp.logical_not(exists(step, 0)))
        def _():
            uw[:, :, 1 : 1 + layers, first : first + HALO, :] = jnp.zeros(
                (members, comps, layers, HALO, cols), jnp.float32
            )
            for buffer in (mw, xo, xl, xr):
                buffer[:, first : first + HALO, :] = jnp.zeros(
                    (buffer.shape[0], HALO, cols), jnp.float32
                )

    for step, buffer in ((-1, xl), (1, xr)):

        @pl.when(jnp.logical_not(exists(0, step)))
        def _():
            buffer[:, TOP:end, :] = jnp.zeros((buffer.shape[0], wide, cols), jnp.float32)

    def kind(dx, dy):
        return "both" if dx != 0 and dy != 0 else ("x" if dx != 0 else "y")

    def send(part, dx, dy, *pairs):
        copies = [
            pltpu.make_async_remote_copy(
                src_ref=source,
                dst_ref=target,
                send_sem=halo_send.at[0],
                recv_sem=halo_recv.at[part],
                device_id=at(dx, dy),
                device_id_type=MESH,
            )
            for source, target in pairs
        ]

        @pl.when(exists(dx, dy))
        def _():
            for copy in copies:
                copy.start()

        if dx >= 0 and dy >= 0:
            for source, _ in pairs:
                count = 1
                for size in source.shape[:-1]:
                    count *= size
                rows_of[part][kind(dx, dy)] += count

    rows_of = [{"x": 0, "y": 0, "both": 0} for _ in range(2 + members)]

    def each_total(counts, action):
        ends_x = jnp.logical_or(plane == 0, plane == planes - 1)
        ends_y = jnp.logical_or(planey == 0, planey == planeys - 1)
        for many_x in (1, 2):
            for many_y in (1, 2):
                total = many_x * counts["x"] + many_y * counts["y"]
                total += many_x * many_y * counts["both"]
                here_x = ends_x if many_x == 1 else jnp.logical_not(ends_x)
                here_y = ends_y if many_y == 1 else jnp.logical_not(ends_y)

                @pl.when(jnp.logical_and(here_x, here_y))
                def _():
                    action(total)

    def counted(total, part):
        block = tally.at[pl.ds(0, total)]
        return pltpu.make_async_remote_copy(
            src_ref=block,
            dst_ref=block,
            send_sem=halo_send.at[0],
            recv_sem=halo_recv.at[part],
            device_id=partner,
            device_id_type=MESH,
        )

    def row_range(dx):
        if dx < 0:
            return pl.ds(OWN, HALO), pl.ds(OWN + rows, HALO)
        if dx > 0:
            return pl.ds(OWN + rows - HALO, HALO), pl.ds(TOP, HALO)
        return pl.ds(OWN, rows), pl.ds(OWN, rows)

    hands = []
    for axis, count in (("plane", planes), ("planey", planeys)):
        reach = 1
        while reach * 2 <= count // 2:
            hands.append((reach, axis))
            reach *= 2
    hands.sort()

    def greet(number):
        reach, axis = hands[number]
        for step in (-reach, reach):
            target = at(step, 0) if axis == "plane" else at(0, step)
            pl.semaphore_signal(
                hand_sem.at[number], inc=1, device_id=target, device_id_type=MESH
            )

    def greeted(number):
        pl.semaphore_wait(hand_sem.at[number], 2)

    def greet_round(reach):
        for number, (distance, _) in enumerate(hands):
            if distance == reach:
                greet(number)

    def greeted_round(reach):
        for number, (distance, _) in enumerate(hands):
            if distance == reach:
                greeted(number)

    lane = lax.broadcasted_iota(jnp.int32, (rows, cols), 1)
    group = lane // PITCH

    def lane_packed(planes_of):
        packed = jnp.zeros((rows, cols), jnp.float32)
        for layer in range(layers):
            turned = pltpu.roll(planes_of(layer), (PITCH * layer + HALO) % cols, 1)
            packed = jnp.where(group == layer, turned, packed)
        return packed

    body = pl.ds(1, layers)

    def send_u(part, member):
        for dx in (-1, 1):
            here, there = row_range(dx)
            send(
                part,
                dx,
                0,
                (uw.at[member, :, body, here, :], uw.at[member, :, body, there, :]),
            )

    def pack_u(member):
        for comp in range(comps):
            xo[u_field(member) + comp, OWN : OWN + rows, :] = lane_packed(
                lambda layer: uw[member, comp, 1 + layer, OWN : OWN + rows, :]
            )

    def send_packed(part, low, count, map_low, map_count):
        fields_here = pl.ds(low, count)
        maps_here = pl.ds(map_low, map_count)
        for dx, dy in sorted(around, key=lambda d: -abs(d[0])):
            here, there = row_range(dx)
            target = xo if dy == 0 else (xr if dy < 0 else xl)
            pairs = [(xo.at[fields_here, here, :], target.at[fields_here, there, :])]
            if dy == 0:
                pairs.append((mw.at[maps_here, here, :], mw.at[maps_here, there, :]))
            send(part, dx, dy, *pairs)

    with scope("p0_load"):
        load_u[0].wait()
    with scope("p1_barrier"):
        pl.semaphore_wait(barrier, len(around) + 1)
    block = tally.at[pl.ds(0, maps_rows)]
    pltpu.make_async_copy(block, block, local_sem.at[members + 1]).wait()
    load_picks.wait()
    mask_own = mask_in[...].astype(jnp.float32)
    bed_own = bed_in[...].astype(jnp.float32) * bed_unit
    mw[0, OWN : OWN + rows, :] = mask_own
    xo[MASK, OWN : OWN + rows, :] = lane_packed(lambda layer: mask_own)
    pack_u(0)
    send_packed(0, 0, 1 + comps, 0, 1)
    send_u(1 + members, 0)
    greet_round(1)
    mw[1, OWN : OWN + rows, :] = bed_own
    xo[bed_field, OWN : OWN + rows, :] = lane_packed(lambda layer: bed_own)
    for member in range(members):
        chosen = table[picks[member]]
        mw[2 + member, OWN : OWN + rows, :] = chosen
        xo[friction_field(member), OWN : OWN + rows, :] = jnp.where(
            lane < PITCH, pltpu.roll(chosen, HALO, 1), 0.0
        )
    send_packed(1, bed_field, 2, 1, 2)
    for member in range(1, members):
        load_u[member].wait()
        send_u(1 + member, member)
        pack_u(member)
        send_packed(1 + member, friction_field(member), 1 + comps, 2 + member, 1)

    with scope("p3_greeted1"):
        greeted_round(1)
    greet_round(2)

    def arrived(part):
        with scope("p4_halo%d" % part):
            each_total(rows_of[part], lambda total: counted(total, part).wait_recv())

    bf16 = jnp.bfloat16
    apart = lax.broadcasted_iota(jnp.int32, (cols, cols), 0) - lax.broadcasted_iota(
        jnp.int32, (cols, cols), 1
    )

    def at_steps(step):
        return jnp.where(apart == step, 1.0, 0.0)

    near_z = at_steps(PITCH) + at_steps(-PITCH)
    corners = (
        at_steps(PITCH + 1) + at_steps(PITCH - 1) + at_steps(1 - PITCH) + at_steps(-PITCH - 1)
    )
    near_y = at_steps(1) + at_steps(-1)
    lane_sums = [
        at_steps(0)
        + along_y[comp] * near_y
        + along_z * near_z
        + along_y[comp] * along_z * corners
        for comp in range(comps)
    ]
    lane_steps = [at_steps(1) - at_steps(-1), at_steps(PITCH) - at_steps(-PITCH)]
    for number, matrix in enumerate(lane_sums + lane_steps):
        matrix = matrix.astype(bf16)
        lane_matrix[number, :cols, :] = matrix
        lane_matrix[number, cols:, :] = matrix

    arrived(0)

    lane = lax.broadcasted_iota(jnp.int32, (wide, cols), 1)
    first_lane = lane == 0
    last_lane = lane == cols - 1
    spot = lax.rem(lane, PITCH)
    outer_left = spot < HALO
    left_edge = spot == HALO - 1
    position = (
        plane * rows - HALO + lax.broadcasted_iota(jnp.int32, (wide, cols), 0)
    ).astype(jnp.float32)
    thickness = 1.0 + 2.0 * position / (rows * planes - 1)

    def sides(number, low=TOP, high=end):
        own = xo[number, low:high, :]
        return (
            jnp.where(outer_left, xl[number, low:high, :], own),
            jnp.where(outer_left, own, xr[number, low:high, :]),
        )

    def edges(pair):
        left, right = pair
        return jnp.where(
            left_edge, pltpu.roll(right, cols - 1, 1), pltpu.roll(left, 1, 1)
        )

    def y_pair(value, near):
        return (
            jnp.where(last_lane, near, pltpu.roll(value, cols - 1, 1)),
            jnp.where(first_lane, near, pltpu.roll(value, 1, 1)),
        )

    def turned_edge(value, layer):
        return pltpu.roll(value, cols - HALO - PITCH * layer, 1)

    mask_main = mw[0, TOP:end, :]
    fixed[0] = mask_main
    for side, mask_here in enumerate(sides(MASK)):
        fixed[3 + side] = mask_here

    def forces():
        bed_pair = sides(bed_field)
        bed_plus, bed_minus = y_pair(mw[1, TOP:end, :], turned_edge(edges(bed_pair), 0))
        scale = -(fixed[0] * thickness)
        fixed[1] = scale * (
            (mw[1, TOP + 1 : end + 1, :] - mw[1, TOP - 1 : end - 1, :]) * 0.5
        )
        fixed[2] = scale * ((bed_plus - bed_minus) * 0.5)
        for side, bed_here in enumerate(bed_pair):
            shifted[side, TOP:end, :] = bed_here
            down = shifted[side, TOP + 1 : end + 1, :] - shifted[side, TOP - 1 : end - 1, :]
            flat = pltpu.roll(bed_here, cols - 1, 1) - pltpu.roll(bed_here, 1, 1)
            scale = -(fixed[3 + side] * thickness)
            fixed[5 + side] = scale * (down * 0.5)
            fixed[7 + side] = scale * (flat * 0.5)

    def power(strain4):
        return jnp.exp(jnp.log(strain4 * 0.25 + 0.1) * (-1.0 / 6.0))

    def strain4_of(ui, vi, uj, vj, uz, vz):
        shear = uj + vi
        return ui * ui + vj * vj + ui * vj + 0.25 * (shear * shear + (uz * uz + vz * vz))

    def lane_halves(values):
        stacked = jnp.concatenate(values, axis=0)
        high = stacked.astype(bf16)
        low = (stacked - high.astype(jnp.float32)).astype(bf16)
        return jnp.concatenate([high, low], axis=1)

    def lane_product(halves, number):
        product = jnp.dot(
            halves, lane_matrix[number], preferred_element_type=jnp.float32
        )
        return [product[low : low + wide] for low in range(0, product.shape[0], wide)]

    def strip_k(pair, comp, slot):
        result = []
        for side, value in enumerate(lane_product(lane_halves(pair), comp)):
            shifted[slot + side, TOP:end, :] = value
            result.append(
                value
                + along_x[comp]
                * (
                    shifted[slot + side, TOP + 1 : end + 1, :]
                    + shifted[slot + side, TOP - 1 : end - 1, :]
                )
            )
        return result

    own_top = lax.broadcasted_iota(jnp.int32, (8, cols), 0) >= HALO

    def own_sum(value):
        total = jnp.where(own_top, value[:8], value[wide - 8 :])
        for low in range(8, wide - 8, 8):
            total = total + value[low : low + 8]
        return total

    def strip_start(member):
        for comp in range(comps):
            pair = sides(u_field(member) + comp)
            edge[EDGE_U + comp] = edges(pair)
            for side in range(2):
                strip[comp * 2 + side, TOP:end, :] = pair[side]
        strip_roots = []
        halves = lane_halves([strip[k, TOP:end, :] for k in range(2 * comps)])
        steps_j = lane_product(halves, comps)
        steps_z = lane_product(halves, comps + 1)
        for side in range(2):
            step_i = [
                strip[comp * 2 + side, TOP + 1 : end + 1, :]
                - strip[comp * 2 + side, TOP - 1 : end - 1, :]
                for comp in range(comps)
            ]
            step_j = [steps_j[comp * 2 + side] for comp in range(comps)]
            step_z = [steps_z[comp * 2 + side] for comp in range(comps)]
            strip_roots.append(
                fixed[3 + side]
                * power(
                    strain4_of(
                        step_i[0], step_i[1], step_j[0], step_j[1], step_z[0], step_z[1]
                    )
                )
            )
            strip_kept[side] = strip_roots[side]
        edge[EDGE_R] = edges(strip_roots)
        for comp in range(comps):
            around_roots = strip_k(strip_roots, comp, comp * 2)
            field = [
                strip_roots[side] * (fixed[3 + side] * strip[comp * 2 + side, TOP:end, :])
                for side in range(2)
            ]
            edge[EDGE_0 + comp] = edges(field)
            near = strip_k(field, comp, 4 + comp * 2)
            for side in range(2):
                strip_kept[2 + 4 * comp + side] = around_roots[side]
                strip_kept[4 + 4 * comp + side] = near[side]

    def strip_end(member):
        strip_roots = [strip_kept[side] for side in range(2)]
        four = [4.0 * root for root in strip_roots]
        friction_pair = sides(friction_field(member))
        diag = [
            fixed[3 + side] * friction_pair[side] + (1.0 - fixed[3 + side])
            for side in range(2)
        ]
        for comp in range(comps):
            main = [
                four[side] * strip_kept[2 + 4 * comp + side] + diag[side]
                for side in range(2)
            ]
            residual = [
                fixed[5 + 2 * comp + side]
                - (
                    main[side] * (fixed[3 + side] * strip[comp * 2 + side, TOP:end, :])
                    - four[side] * strip_kept[4 + 4 * comp + side]
                )
                for side in range(2)
            ]
            field = [strip_roots[side] * residual[side] for side in range(2)]
            edge[EDGE_1 + comp] = edges(field)
            near = strip_k(field, comp, comp * 2)
            image = [
                main[side] * residual[side] - four[side] * near[side] for side in range(2)
            ]
            edge[EDGE_2 + comp] = edges([strip_roots[side] * image[side] for side in range(2)])

    def share_start(member):
        for comp in range(comps):
            for layer in range(layers):
                plus, minus = y_pair(
                    uw[member, comp, layer + 1, TOP:end, :],
                    turned_edge(edge[EDGE_U + comp], layer),
                )
                step_y[comp, layer] = plus - minus
        for layer in range(layers):
            step_i = [
                uw[member, comp, layer + 1, TOP + 1 : end + 1, :]
                - uw[member, comp, layer + 1, TOP - 1 : end - 1, :]
                for comp in range(comps)
            ]
            step_z = [
                uw[member, comp, layer + 2, TOP:end, :] - uw[member, comp, layer, TOP:end, :]
                for comp in range(comps)
            ]
            roots[layer] = fixed[0] * power(
                strain4_of(
                    step_i[0],
                    step_i[1],
                    step_y[0, layer],
                    step_y[1, layer],
                    step_z[0],
                    step_z[1],
                )
            )
        for layer in range(layers):
            root = roots[layer]
            plus, minus = y_pair(root, turned_edge(edge[EDGE_R], layer))
            both = plus + minus
            for comp in range(comps):
                tr[comp, layer + 1, TOP:end, :] = root + along_y[comp] * both
                field = root * (fixed[0] * uw[member, comp, layer + 1, TOP:end, :])
                plus, minus = y_pair(field, turned_edge(edge[EDGE_0 + comp], layer))
                tp[comp, layer + 1, TOP:end, :] = field + along_y[comp] * (plus + minus)

    def x_sum(buffer, comp, layer):
        return buffer[comp, layer, TOP:end, :] + along_x[comp] * (
            buffer[comp, layer, TOP + 1 : end + 1, :]
            + buffer[comp, layer, TOP - 1 : end - 1, :]
        )

    def spread_y(buffer, number):
        for layer in range(layers):
            for comp in range(comps):
                field = step_y[comp, layer]
                plus, minus = y_pair(field, turned_edge(edge[number + comp], layer))
                buffer[comp, layer + 1, TOP:end, :] = field + along_y[comp] * (plus + minus)

    def share_end(member):
        slot = members * ens + member
        empty = jnp.zeros((wide, cols), jnp.float32)

        def residual_layer(layer, carry):
            before, now, total = carry
            root = roots[layer]
            four = 4.0 * root
            here = fixed[0]
            bottom = jnp.where(layer == 0, 1.0, 0.0)
            diag = here * mw[2 + member, TOP:end, :] * bottom + (1.0 - here)
            after = []
            for comp in range(comps):
                after_r = x_sum(tr, comp, layer + 2)
                after_p = x_sum(tp, comp, layer + 2)
                after += [after_r, after_p]
                around_roots = now[2 * comp] + along_z * (before[2 * comp] + after_r)
                near = now[2 * comp + 1] + along_z * (before[2 * comp + 1] + after_p)
                main = four * around_roots + diag
                start = here * uw[member, comp, layer + 1, TOP:end, :]
                residual = fixed[1 + comp] - (main * start - four * near)
                field_a[comp, layer] = main
                all_residual[slot, comp, layer] = residual
                total = total + own_sum(residual * residual)
                step_y[comp, layer] = root * residual
            return tuple(now), tuple(after), total

        nothing = jnp.zeros((8, cols), jnp.float32)
        first = tuple(
            x_sum(buffer, comp, 1) for comp in range(comps) for buffer in (tr, tp)
        )
        with scope("q2_residual"):
            _, _, gram_rr = lax.fori_loop(
                0, layers, residual_layer, ((empty,) * 4, first, nothing), unroll=UNROLL
            )
            spread_y(tq, EDGE_1)

        def image_layer(layer, carry):
            before, now, total_ra, total_aa = carry
            root = roots[layer]
            four = 4.0 * root
            after = []
            for comp in range(comps):
                after_p = x_sum(tq, comp, layer + 2)
                after.append(after_p)
                near = now[comp] + along_z * (before[comp] + after_p)
                residual = all_residual[slot, comp, layer]
                image = field_a[comp, layer] * residual - four * near
                all_image[slot, comp, layer] = image
                total_ra = total_ra + own_sum(residual * image)
                total_aa = total_aa + own_sum(image * image)
                step_y[comp, layer] = root * image
            return tuple(now), tuple(after), total_ra, total_aa

        first = tuple(x_sum(tq, comp, 1) for comp in range(comps))
        with scope("q3_image"):
            _, _, gram_ra, gram_aa = lax.fori_loop(
                0,
                layers,
                image_layer,
                ((empty,) * 2, first, nothing, nothing),
                unroll=UNROLL,
            )
            spread_y(tp, EDGE_2)

        def own_x_sum(comp, layer):
            return tp[comp, layer, OWN : OWN + rows, :] + along_x[comp] * (
                tp[comp, layer, OWN + 1 : OWN + rows + 1, :]
                + tp[comp, layer, OWN - 1 : OWN + rows - 1, :]
            )

        def second_layer(layer, carry):
            before, now, total = carry
            four = 4.0 * roots[layer, HALO : HALO + rows, :]
            after = []
            for comp in range(comps):
                after_p = own_x_sum(comp, layer + 2)
                after.append(after_p)
                near = now[comp] + along_z * (before[comp] + after_p)
                image = all_image[slot, comp, layer, HALO : HALO + rows, :]
                second = (
                    field_a[comp, layer, HALO : HALO + rows, :] * image - four * near
                )
                product = image * second
                for low in range(0, rows, 8):
                    total = total + product[low : low + 8]
            return tuple(now), tuple(after), total

        empty_own = jnp.zeros((rows, cols), jnp.float32)
        first = tuple(own_x_sum(comp, 1) for comp in range(comps))
        with scope("q4_second"):
            _, _, gram_ab = lax.fori_loop(
                0, layers, second_layer, ((empty_own,) * 2, first, nothing), unroll=UNROLL
            )
        for number, value in enumerate((gram_rr, gram_ra, gram_aa, gram_ab)):
            gram[4 * member + number] = value

    def to_partner(block):
        pltpu.make_async_remote_copy(
            src_ref=block,
            dst_ref=block,
            send_sem=pair_send.at[0],
            recv_sem=pair_recv.at[0],
            device_id=partner,
            device_id_type=MESH,
        ).start()

    inner = pl.ds(HALO, rows)

    def share_member(member):
        slot = members * ens + member
        for buffer in (all_residual, all_image):
            to_partner(buffer.at[slot, :, :, inner, :])

    for member in range(members):
        if member > 0:
            arrived(1 + member)
        with scope("q0_start"):
            strip_start(member)
            if member == 0:
                arrived(1 + members)
            share_start(member)
        if member == 0:
            with scope("p5_greeted2"):
                greeted_round(2)
            greet_round(4)
            pl.semaphore_signal(
                hand_sem.at[len(hands)], inc=1, device_id=partner, device_id_type=MESH
            )
            arrived(1)
            forces()
        with scope("q1_end"):
            strip_end(member)
            share_end(member)
        if member < members - 1:
            share_member(member)

    lines = 4 * members
    total = jnp.sum(gram[...], axis=1)
    total = jnp.sum(total, axis=1, keepdims=True)
    lane = lax.broadcasted_iota(jnp.int32, (lines, cols), 1)
    line = lax.broadcasted_iota(jnp.int32, (lines, cols), 0)
    message = jnp.sum(
        jnp.where(lane == line + lines * ens, total, 0.0), axis=0, keepdims=True
    )
    with scope("p7_hand"):
        pl.semaphore_wait(hand_sem.at[len(hands)], 1)

    def exchange(ring, me, count, target, send_sem, recv_sem, value, sign=-1):
        ring[me] = value
        for offset in sorted(range(1, count), key=lambda k: sign * min(k, count - k)):
            pltpu.make_async_remote_copy(
                src_ref=ring.at[me],
                dst_ref=ring.at[me],
                send_sem=send_sem.at[0],
                recv_sem=recv_sem.at[0],
                device_id=target(lax.rem(me + offset, count)),
                device_id_type=MESH,
            ).start()
        return pltpu.make_async_remote_copy(
            src_ref=ring.at[pl.ds(0, count - 1)],
            dst_ref=ring.at[pl.ds(0, count - 1)],
            send_sem=send_sem.at[0],
            recv_sem=recv_sem.at[0],
            device_id=target(lax.rem(me + 1, count)),
            device_id_type=MESH,
        )

    cores = 2
    copies_y = exchange(
        ring_y,
        planey * cores + ens,
        planeys * cores,
        lambda peer: {"planey": peer // cores, "ens": lax.rem(peer, cores)},
        y_send,
        y_recv,
        message,
    )

    for comp in range(comps):
        for layer in range(layers):
            total = None
            for member in range(members):
                start = mw[0, OWN : OWN + rows, :] * uw[member, comp, layer + 1, OWN : OWN + rows, :]
                total = start if total is None else total + start
            all_start[ens, comp, layer] = total
    everything = {
        name: sum(counts[name] for counts in rows_of) for name in ("x", "y", "both")
    }
    each_total(everything, lambda total: counted(total, 0).wait_send())
    with scope("p8_ary"):
        copies_y.wait_recv()
    with scope("p6_greeted4"):
        for reach in (4, 8, 16):
            greeted_round(reach)
            if reach > 2:
                greet_round(2 * reach)
    copies_x = exchange(
        ring_x,
        plane,
        planes,
        lambda peer: {"plane": peer},
        x_send,
        x_recv,
        jnp.sum(ring_y[...], axis=0),
        sign=1,
    )
    share_member(members - 1)
    to_partner(all_start.at[ens])
    copies_y.wait_send()
    block = all_residual.at[:, :, :, pl.ds(0, (2 * members + 1) * rows // (2 * members)), :]
    fields = pltpu.make_async_remote_copy(
        src_ref=block,
        dst_ref=block,
        send_sem=pair_send.at[0],
        recv_sem=pair_recv.at[0],
        device_id=partner,
        device_id_type=MESH,
    )
    fields.wait_send()
    fields.wait_recv()
    with scope("p9_arx"):
        copies_x.wait_recv()
    sums = jnp.sum(ring_x[...], axis=0)
    gram_rr = sums
    gram_ra = pltpu.roll(sums, cols - 1, 1)
    gram_aa = pltpu.roll(sums, cols - 2, 1)
    gram_ab = pltpu.roll(sums, cols - 3, 1)
    first_step = gram_rr / gram_ra
    norm_next = gram_rr - 2.0 * first_step * gram_ra + first_step * first_step * gram_aa
    growth = 1.0 + norm_next / gram_rr
    curve = (
        growth * growth * gram_ra
        - 2.0 * growth * first_step * gram_aa
        + first_step * first_step * gram_ab
    )
    second_step = norm_next / curve
    samples = members * cores
    share = 1.0 / samples
    for_residual = share * (first_step + second_step * growth)
    for_image = share * (second_step * first_step)
    lane = lax.broadcasted_iota(jnp.int32, (1, cols), 1)

    def pick(value, number):
        return jnp.sum(jnp.where(lane == 4 * number, value, 0.0), axis=1, keepdims=True)

    weights = [(pick(for_residual, k), pick(for_image, k)) for k in range(samples)]

    def combine(layer, carry):
        for comp in range(comps):
            total = share * (all_start[0, comp, layer] + all_start[1, comp, layer])
            for number in range(samples):
                total = total + (
                    weights[number][0] * all_residual[number, comp, layer, HALO : HALO + rows, :]
                    - weights[number][1] * all_image[number, comp, layer, HALO : HALO + rows, :]
                )
            out[comp, layer] = total
        return carry

    with scope("pa_combine"):
        lax.fori_loop(0, layers, combine, 0, unroll=UNROLL)
    with scope("pb_sent"):
        copies_x.wait_send()


def body(sizes, u_prior, friction_rows, friction_table, bed_fixed, ice_mask):
    planes, planeys = sizes
    members, comps, layers, rows, cols = u_prior.shape
    wide = rows + 2 * HALO
    deep = rows + 24
    samples = 2 * members
    f32 = jnp.float32
    anywhere = pl.BlockSpec(memory_space=pltpu.HBM)
    fields = 2 + members * (1 + comps)
    vmem = pltpu.VMEM
    dma = pltpu.SemaphoreType.DMA
    return pl.pallas_call(
        functools.partial(kernel, sizes),
        out_shape=jax.ShapeDtypeStruct((comps, layers, rows, cols), f32),
        in_specs=[anywhere] * 5,
        out_specs=pl.BlockSpec(memory_space=pltpu.VMEM),
        scratch_shapes=[
            vmem((members, comps, layers + 2, deep, cols), f32),
            vmem((2 + members, deep, cols), f32),
            vmem((fields, deep, cols), f32),
            vmem((fields, deep, cols), f32),
            vmem((fields, deep, cols), f32),
            vmem(friction_table.shape, f32),
            vmem((rows, cols), jnp.int32),
            vmem((rows, cols), jnp.int32),
            pltpu.SMEM((members,), jnp.int32),
            vmem((2 * comps, deep, cols), f32),
            vmem((4 * comps, deep, cols), f32),
            vmem((2 + 4 * comps, wide, cols), f32),
            vmem((4, 2 * cols, cols), jnp.bfloat16),
            vmem((1536, cols), f32),
            vmem((9, wide, cols), f32),
            vmem((9, wide, cols), f32),
            vmem((layers, wide, cols), f32),
            vmem((comps, layers, wide, cols), f32),
            vmem((comps, layers + 2, deep, cols), f32),
            vmem((comps, layers + 2, deep, cols), f32),
            vmem((comps, layers + 2, deep, cols), f32),
            vmem((comps, layers, wide, cols), f32),
            vmem((samples, comps, layers, wide, cols), f32),
            vmem((samples, comps, layers, wide, cols), f32),
            vmem((2, comps, layers, rows, cols), f32),
            vmem((4 * members, 8, cols), f32),
            vmem((2 * planeys, 1, cols), f32),
            vmem((planes, 1, cols), f32),
            dma((members + 2,)),
            dma((1,)),
            dma((2 + members,)),
            pltpu.SemaphoreType.REGULAR((6,)),
            dma((1,)),
            dma((1,)),
            dma((1,)),
            dma((1,)),
            dma((1,)),
            dma((1,)),
        ],
        compiler_params=pltpu.CompilerParams(
            collective_id=0, has_side_effects=True, vmem_limit_bytes=48 * 1024 * 1024
        ),
    )(*[
        pltpu.with_memory_space_constraint(x, pltpu.HBM)
        for x in (u_prior, friction_rows, friction_table, bed_fixed, ice_mask)
    ])


def solution(mesh):
    in_specs = (
        P(("group", "ens"), None, None, "plane", "planey"),
        P(("group", "ens")),
        P("group", "plane", "planey"),
        P("plane", "planey"),
        P("plane", "planey"),
    )
    out_specs = P("group", None, "plane", "planey")
    sizes = (mesh.shape["plane"], mesh.shape["planey"])
    return jax.shard_map(
        functools.partial(body, sizes),
        mesh=mesh,
        in_specs=in_specs,
        out_specs=out_specs,
        check_vma=False,
    )
```

```python
import contextlib
import functools

import jax
import jax.numpy as jnp
from jax import lax
from jax.experimental import pallas as pl
from jax.experimental.pallas import tpu as pltpu
from jax.sharding import PartitionSpec as P

bed_unit = 2.0 ** (-29)
HALO = 4
TOP = 8
OWN = TOP + HALO
PITCH = 8
MESH = pl.DeviceIdType.MESH
along_z = 0.5
along_x = (0.25, 0.125)
along_y = (0.125, 0.25)
MASK = 0
UNROLL = 10


def scope(name):
    return contextlib.nullcontext()


EDGE_U, EDGE_R, EDGE_0, EDGE_1, EDGE_2 = 0, 2, 3, 5, 7


def kernel(
    sizes,
    u_hbm,
    picks_hbm,
    table_hbm,
    bed_hbm,
    mask_hbm,
    out,
    uw,
    mw,
    xo,
    xl,
    xr,
    table,
    bed_in,
    mask_in,
    picks,
    strip,
    shifted,
    strip_kept,
    lane_matrix,
    tally,
    edge,
    fixed,
    roots,
    step_y,
    tr,
    tp,
    tq,
    field_a,
    all_residual,
    all_image,
    all_start,
    gram,
    ring_y,
    ring_x,
    local_sem,
    halo_send,
    halo_recv,
    hand_sem,
    pair_send,
    pair_recv,
    y_send,
    y_recv,
    x_send,
    x_recv,
):
    planes, planeys = sizes
    members, comps, layers, rows, cols = u_hbm.shape
    wide = rows + 2 * HALO
    end = TOP + wide
    plane = lax.axis_index("plane")
    planey = lax.axis_index("planey")
    ens = lax.axis_index("ens")

    def at(dx, dy):
        return {
            "plane": lax.rem(plane + dx + planes, planes),
            "planey": lax.rem(planey + dy + planeys, planeys),
        }

    partner = {"ens": 1 - ens}
    around = [(dx, dy) for dx in (-1, 0, 1) for dy in (-1, 0, 1) if (dx, dy) != (0, 0)]

    def exists(dx, dy):
        flag = None
        for step, index, count in ((dx, plane, planes), (dy, planey, planeys)):
            if step != 0:
                part = index > 0 if step < 0 else index < count - 1
                flag = part if flag is None else jnp.logical_and(flag, part)
        return flag

    bed_field = 1 + comps

    def friction_field(member):
        return bed_field + 1 + member * (1 + comps) - (comps if member > 0 else 0)

    def u_field(member):
        return 1 if member == 0 else friction_field(member) + 1

    def load_member(member):
        return pltpu.make_async_copy(
            u_hbm.at[member],
            uw.at[member, :, pl.ds(1, layers), pl.ds(OWN, rows), :],
            local_sem.at[member],
        )

    load_u = [load_member(member) for member in range(members)]
    load_picks = pltpu.make_async_copy(picks_hbm, picks, local_sem.at[members])
    load_maps = [
        pltpu.make_async_copy(source, target, local_sem.at[members + 1])
        for source, target in ((table_hbm, table), (bed_hbm, bed_in), (mask_hbm, mask_in))
    ]
    maps_rows = (table.shape[0] + 2) * rows
    for load in (load_u[0], load_picks, *load_maps, *load_u[1:]):
        load.start()

    barrier = pltpu.get_barrier_semaphore()
    for dx, dy in around:
        pl.semaphore_signal(barrier, inc=1, device_id=at(dx, dy), device_id_type=MESH)
    pl.semaphore_signal(barrier, inc=1, device_id=partner, device_id_type=MESH)

    for end_layer in (0, layers + 1):
        uw[:, :, end_layer, TOP:end, :] = jnp.zeros((members, comps, wide, cols), jnp.float32)
        for buffer in (tr, tp, tq):
            buffer[:, end_layer] = jnp.zeros(buffer.shape[:1] + buffer.shape[2:], jnp.float32)
    for step, first in ((-1, TOP), (1, OWN + rows)):

        @pl.when(jnp.logical_not(exists(step, 0)))
        def _():
            uw[:, :, 1 : 1 + layers, first : first + HALO, :] = jnp.zeros(
                (members, comps, layers, HALO, cols), jnp.float32
            )
            for buffer in (mw, xo, xl, xr):
                buffer[:, first : first + HALO, :] = jnp.zeros(
                    (buffer.shape[0], HALO, cols), jnp.float32
                )

    for step, buffer in ((-1, xl), (1, xr)):

        @pl.when(jnp.logical_not(exists(0, step)))
        def _():
            buffer[:, TOP:end, :] = jnp.zeros((buffer.shape[0], wide, cols), jnp.float32)

    def kind(dx, dy):
        return "both" if dx != 0 and dy != 0 else ("x" if dx != 0 else "y")

    def send(part, dx, dy, *pairs):
        copies = [
            pltpu.make_async_remote_copy(
                src_ref=source,
                dst_ref=target,
                send_sem=halo_send.at[0],
                recv_sem=halo_recv.at[part],
                device_id=at(dx, dy),
                device_id_type=MESH,
            )
            for source, target in pairs
        ]

        @pl.when(exists(dx, dy))
        def _():
            for copy in copies:
                copy.start()

        if dx >= 0 and dy >= 0:
            for source, _ in pairs:
                count = 1
                for size in source.shape[:-1]:
                    count *= size
                rows_of[part][kind(dx, dy)] += count

    rows_of = [{"x": 0, "y": 0, "both": 0} for _ in range(2 + members)]

    def each_total(counts, action):
        ends_x = jnp.logical_or(plane == 0, plane == planes - 1)
        ends_y = jnp.logical_or(planey == 0, planey == planeys - 1)
        for many_x in (1, 2):
            for many_y in (1, 2):
                total = many_x * counts["x"] + many_y * counts["y"]
                total += many_x * many_y * counts["both"]
                here_x = ends_x if many_x == 1 else jnp.logical_not(ends_x)
                here_y = ends_y if many_y == 1 else jnp.logical_not(ends_y)

                @pl.when(jnp.logical_and(here_x, here_y))
                def _():
                    action(total)

    def counted(total, part):
        block = tally.at[pl.ds(0, total)]
        return pltpu.make_async_remote_copy(
            src_ref=block,
            dst_ref=block,
            send_sem=halo_send.at[0],
            recv_sem=halo_recv.at[part],
            device_id=partner,
            device_id_type=MESH,
        )

    def row_range(dx):
        if dx < 0:
            return pl.ds(OWN, HALO), pl.ds(OWN + rows, HALO)
        if dx > 0:
            return pl.ds(OWN + rows - HALO, HALO), pl.ds(TOP, HALO)
        return pl.ds(OWN, rows), pl.ds(OWN, rows)

    hands = []
    for axis, count in (("plane", planes), ("planey", planeys)):
        reach = 1
        while reach * 2 <= count // 2:
            hands.append((reach, axis))
            reach *= 2
    hands.sort()

    def greet(number):
        reach, axis = hands[number]
        for step in (-reach, reach):
            target = at(step, 0) if axis == "plane" else at(0, step)
            pl.semaphore_signal(
                hand_sem.at[number], inc=1, device_id=target, device_id_type=MESH
            )

    def greeted(number):
        pl.semaphore_wait(hand_sem.at[number], 2)

    def greet_round(reach):
        for number, (distance, _) in enumerate(hands):
            if distance == reach:
                greet(number)

    def greeted_round(reach):
        for number, (distance, _) in enumerate(hands):
            if distance == reach:
                greeted(number)

    lane = lax.broadcasted_iota(jnp.int32, (rows, cols), 1)
    group = lane // PITCH

    def lane_packed(planes_of):
        packed = jnp.zeros((rows, cols), jnp.float32)
        for layer in range(layers):
            turned = pltpu.roll(planes_of(layer), (PITCH * layer + HALO) % cols, 1)
            packed = jnp.where(group == layer, turned, packed)
        return packed

    body = pl.ds(1, layers)

    def send_u(part, member):
        for dx in (-1, 1):
            here, there = row_range(dx)
            send(
                part,
                dx,
                0,
                (uw.at[member, :, body, here, :], uw.at[member, :, body, there, :]),
            )

    def pack_u(member):
        for comp in range(comps):
            xo[u_field(member) + comp, OWN : OWN + rows, :] = lane_packed(
                lambda layer: uw[member, comp, 1 + layer, OWN : OWN + rows, :]
            )

    def send_packed(part, low, count, map_low, map_count):
        fields_here = pl.ds(low, count)
        maps_here = pl.ds(map_low, map_count)
        for dx, dy in sorted(around, key=lambda d: -abs(d[0])):
            here, there = row_range(dx)
            target = xo if dy == 0 else (xr if dy < 0 else xl)
            pairs = [(xo.at[fields_here, here, :], target.at[fields_here, there, :])]
            if dy == 0:
                pairs.append((mw.at[maps_here, here, :], mw.at[maps_here, there, :]))
            send(part, dx, dy, *pairs)

    with scope("p0_load"):
        load_u[0].wait()
    with scope("p1_barrier"):
        pl.semaphore_wait(barrier, len(around) + 1)
    greet_round(1)
    block = tally.at[pl.ds(0, maps_rows)]
    pltpu.make_async_copy(block, block, local_sem.at[members + 1]).wait()
    load_picks.wait()
    mask_own = mask_in[...].astype(jnp.float32)
    bed_own = bed_in[...].astype(jnp.float32) * bed_unit
    mw[0, OWN : OWN + rows, :] = mask_own
    xo[MASK, OWN : OWN + rows, :] = lane_packed(lambda layer: mask_own)
    pack_u(0)
    send_packed(0, 0, 1 + comps, 0, 1)
    send_u(1 + members, 0)
    mw[1, OWN : OWN + rows, :] = bed_own
    xo[bed_field, OWN : OWN + rows, :] = lane_packed(lambda layer: bed_own)
    for member in range(members):
        chosen = table[picks[member]]
        mw[2 + member, OWN : OWN + rows, :] = chosen
        xo[friction_field(member), OWN : OWN + rows, :] = jnp.where(
            lane < PITCH, pltpu.roll(chosen, HALO, 1), 0.0
        )
    send_packed(1, bed_field, 2, 1, 2)
    for member in range(1, members):
        load_u[member].wait()
        send_u(1 + member, member)
        pack_u(member)
        send_packed(1 + member, friction_field(member), 1 + comps, 2 + member, 1)

    with scope("p3_greeted1"):
        greeted_round(1)
    greet_round(2)

    def arrived(part):
        with scope("p4_halo%d" % part):
            each_total(rows_of[part], lambda total: counted(total, part).wait_recv())

    bf16 = jnp.bfloat16
    apart = lax.broadcasted_iota(jnp.int32, (cols, cols), 0) - lax.broadcasted_iota(
        jnp.int32, (cols, cols), 1
    )

    def at_steps(step):
        return jnp.where(apart == step, 1.0, 0.0)

    near_z = at_steps(PITCH) + at_steps(-PITCH)
    corners = (
        at_steps(PITCH + 1) + at_steps(PITCH - 1) + at_steps(1 - PITCH) + at_steps(-PITCH - 1)
    )
    near_y = at_steps(1) + at_steps(-1)
    lane_sums = [
        at_steps(0)
        + along_y[comp] * near_y
        + along_z * near_z
        + along_y[comp] * along_z * corners
        for comp in range(comps)
    ]
    lane_steps = [at_steps(1) - at_steps(-1), at_steps(PITCH) - at_steps(-PITCH)]
    for number, matrix in enumerate(lane_sums + lane_steps):
        matrix = matrix.astype(bf16)
        lane_matrix[number, :cols, :] = matrix
        lane_matrix[number, cols:, :] = matrix

    arrived(0)

    lane = lax.broadcasted_iota(jnp.int32, (wide, cols), 1)
    first_lane = lane == 0
    last_lane = lane == cols - 1
    spot = lax.rem(lane, PITCH)
    outer_left = spot < HALO
    left_edge = spot == HALO - 1
    position = (
        plane * rows - HALO + lax.broadcasted_iota(jnp.int32, (wide, cols), 0)
    ).astype(jnp.float32)
    thickness = 1.0 + 2.0 * position / (rows * planes - 1)

    def sides(number, low=TOP, high=end):
        own = xo[number, low:high, :]
        return (
            jnp.where(outer_left, xl[number, low:high, :], own),
            jnp.where(outer_left, own, xr[number, low:high, :]),
        )

    def edges(pair):
        left, right = pair
        return jnp.where(
            left_edge, pltpu.roll(right, cols - 1, 1), pltpu.roll(left, 1, 1)
        )

    def y_pair(value, near):
        return (
            jnp.where(last_lane, near, pltpu.roll(value, cols - 1, 1)),
            jnp.where(first_lane, near, pltpu.roll(value, 1, 1)),
        )

    def turned_edge(value, layer):
        return pltpu.roll(value, cols - HALO - PITCH * layer, 1)

    mask_main = mw[0, TOP:end, :]
    fixed[0] = mask_main
    for side, mask_here in enumerate(sides(MASK)):
        fixed[3 + side] = mask_here

    def forces():
        bed_pair = sides(bed_field)
        bed_plus, bed_minus = y_pair(mw[1, TOP:end, :], turned_edge(edges(bed_pair), 0))
        scale = -(fixed[0] * thickness)
        fixed[1] = scale * (
            (mw[1, TOP + 1 : end + 1, :] - mw[1, TOP - 1 : end - 1, :]) * 0.5
        )
        fixed[2] = scale * ((bed_plus - bed_minus) * 0.5)
        for side, bed_here in enumerate(bed_pair):
            shifted[side, TOP:end, :] = bed_here
            down = shifted[side, TOP + 1 : end + 1, :] - shifted[side, TOP - 1 : end - 1, :]
            flat = pltpu.roll(bed_here, cols - 1, 1) - pltpu.roll(bed_here, 1, 1)
            scale = -(fixed[3 + side] * thickness)
            fixed[5 + side] = scale * (down * 0.5)
            fixed[7 + side] = scale * (flat * 0.5)

    def power(strain4):
        return jnp.exp(jnp.log(strain4 * 0.25 + 0.1) * (-1.0 / 6.0))

    def strain4_of(ui, vi, uj, vj, uz, vz):
        shear = uj + vi
        return ui * ui + vj * vj + ui * vj + 0.25 * (shear * shear + (uz * uz + vz * vz))

    def lane_halves(values):
        stacked = jnp.concatenate(values, axis=0)
        high = stacked.astype(bf16)
        low = (stacked - high.astype(jnp.float32)).astype(bf16)
        return jnp.concatenate([high, low], axis=1)

    def lane_product(halves, number):
        product = jnp.dot(
            halves, lane_matrix[number], preferred_element_type=jnp.float32
        )
        return [product[low : low + wide] for low in range(0, product.shape[0], wide)]

    def strip_k(pair, comp, slot):
        result = []
        for side, value in enumerate(lane_product(lane_halves(pair), comp)):
            shifted[slot + side, TOP:end, :] = value
            result.append(
                value
                + along_x[comp]
                * (
                    shifted[slot + side, TOP + 1 : end + 1, :]
                    + shifted[slot + side, TOP - 1 : end - 1, :]
                )
            )
        return result

    own_top = lax.broadcasted_iota(jnp.int32, (8, cols), 0) >= HALO

    def own_sum(value):
        total = jnp.where(own_top, value[:8], value[wide - 8 :])
        for low in range(8, wide - 8, 8):
            total = total + value[low : low + 8]
        return total

    def strip_start(member):
        for comp in range(comps):
            pair = sides(u_field(member) + comp)
            edge[EDGE_U + comp] = edges(pair)
            for side in range(2):
                strip[comp * 2 + side, TOP:end, :] = pair[side]
        strip_roots = []
        halves = lane_halves([strip[k, TOP:end, :] for k in range(2 * comps)])
        steps_j = lane_product(halves, comps)
        steps_z = lane_product(halves, comps + 1)
        for side in range(2):
            step_i = [
                strip[comp * 2 + side, TOP + 1 : end + 1, :]
                - strip[comp * 2 + side, TOP - 1 : end - 1, :]
                for comp in range(comps)
            ]
            step_j = [steps_j[comp * 2 + side] for comp in range(comps)]
            step_z = [steps_z[comp * 2 + side] for comp in range(comps)]
            strip_roots.append(
                fixed[3 + side]
                * power(
                    strain4_of(
                        step_i[0], step_i[1], step_j[0], step_j[1], step_z[0], step_z[1]
                    )
                )
            )
            strip_kept[side] = strip_roots[side]
        edge[EDGE_R] = edges(strip_roots)
        for comp in range(comps):
            around_roots = strip_k(strip_roots, comp, comp * 2)
            field = [
                strip_roots[side] * (fixed[3 + side] * strip[comp * 2 + side, TOP:end, :])
                for side in range(2)
            ]
            edge[EDGE_0 + comp] = edges(field)
            near = strip_k(field, comp, 4 + comp * 2)
            for side in range(2):
                strip_kept[2 + 4 * comp + side] = around_roots[side]
                strip_kept[4 + 4 * comp + side] = near[side]

    def strip_end(member):
        strip_roots = [strip_kept[side] for side in range(2)]
        four = [4.0 * root for root in strip_roots]
        friction_pair = sides(friction_field(member))
        diag = [
            fixed[3 + side] * friction_pair[side] + (1.0 - fixed[3 + side])
            for side in range(2)
        ]
        for comp in range(comps):
            main = [
                four[side] * strip_kept[2 + 4 * comp + side] + diag[side]
                for side in range(2)
            ]
            residual = [
                fixed[5 + 2 * comp + side]
                - (
                    main[side] * (fixed[3 + side] * strip[comp * 2 + side, TOP:end, :])
                    - four[side] * strip_kept[4 + 4 * comp + side]
                )
                for side in range(2)
            ]
            field = [strip_roots[side] * residual[side] for side in range(2)]
            edge[EDGE_1 + comp] = edges(field)
            near = strip_k(field, comp, comp * 2)
            image = [
                main[side] * residual[side] - four[side] * near[side] for side in range(2)
            ]
            edge[EDGE_2 + comp] = edges([strip_roots[side] * image[side] for side in range(2)])

    def share_start(member):
        for comp in range(comps):
            for layer in range(layers):
                plus, minus = y_pair(
                    uw[member, comp, layer + 1, TOP:end, :],
                    turned_edge(edge[EDGE_U + comp], layer),
                )
                step_y[comp, layer] = plus - minus
        for layer in range(layers):
            step_i = [
                uw[member, comp, layer + 1, TOP + 1 : end + 1, :]
                - uw[member, comp, layer + 1, TOP - 1 : end - 1, :]
                for comp in range(comps)
            ]
            step_z = [
                uw[member, comp, layer + 2, TOP:end, :] - uw[member, comp, layer, TOP:end, :]
                for comp in range(comps)
            ]
            roots[layer] = fixed[0] * power(
                strain4_of(
                    step_i[0],
                    step_i[1],
                    step_y[0, layer],
                    step_y[1, layer],
                    step_z[0],
                    step_z[1],
                )
            )
        for layer in range(layers):
            root = roots[layer]
            plus, minus = y_pair(root, turned_edge(edge[EDGE_R], layer))
            both = plus + minus
            for comp in range(comps):
                tr[comp, layer + 1, TOP:end, :] = root + along_y[comp] * both
                field = root * (fixed[0] * uw[member, comp, layer + 1, TOP:end, :])
                plus, minus = y_pair(field, turned_edge(edge[EDGE_0 + comp], layer))
                tp[comp, layer + 1, TOP:end, :] = field + along_y[comp] * (plus + minus)

    def x_sum(buffer, comp, layer):
        return buffer[comp, layer, TOP:end, :] + along_x[comp] * (
            buffer[comp, layer, TOP + 1 : end + 1, :]
            + buffer[comp, layer, TOP - 1 : end - 1, :]
        )

    def spread_y(buffer, number):
        for layer in range(layers):
            for comp in range(comps):
                field = step_y[comp, layer]
                plus, minus = y_pair(field, turned_edge(edge[number + comp], layer))
                buffer[comp, layer + 1, TOP:end, :] = field + along_y[comp] * (plus + minus)

    def share_end(member):
        slot = members * ens + member
        empty = jnp.zeros((wide, cols), jnp.float32)

        def residual_layer(layer, carry):
            before, now, total = carry
            root = roots[layer]
            four = 4.0 * root
            here = fixed[0]
            bottom = jnp.where(layer == 0, 1.0, 0.0)
            diag = here * mw[2 + member, TOP:end, :] * bottom + (1.0 - here)
            after = []
            for comp in range(comps):
                after_r = x_sum(tr, comp, layer + 2)
                after_p = x_sum(tp, comp, layer + 2)
                after += [after_r, after_p]
                around_roots = now[2 * comp] + along_z * (before[2 * comp] + after_r)
                near = now[2 * comp + 1] + along_z * (before[2 * comp + 1] + after_p)
                main = four * around_roots + diag
                start = here * uw[member, comp, layer + 1, TOP:end, :]
                residual = fixed[1 + comp] - (main * start - four * near)
                field_a[comp, layer] = main
                all_residual[slot, comp, layer] = residual
                total = total + own_sum(residual * residual)
                step_y[comp, layer] = root * residual
            return tuple(now), tuple(after), total

        nothing = jnp.zeros((8, cols), jnp.float32)
        first = tuple(
            x_sum(buffer, comp, 1) for comp in range(comps) for buffer in (tr, tp)
        )
        with scope("q2_residual"):
            _, _, gram_rr = lax.fori_loop(
                0, layers, residual_layer, ((empty,) * 4, first, nothing), unroll=UNROLL
            )
            spread_y(tq, EDGE_1)

        def image_layer(layer, carry):
            before, now, total_ra, total_aa = carry
            root = roots[layer]
            four = 4.0 * root
            after = []
            for comp in range(comps):
                after_p = x_sum(tq, comp, layer + 2)
                after.append(after_p)
                near = now[comp] + along_z * (before[comp] + after_p)
                residual = all_residual[slot, comp, layer]
                image = field_a[comp, layer] * residual - four * near
                all_image[slot, comp, layer] = image
                total_ra = total_ra + own_sum(residual * image)
                total_aa = total_aa + own_sum(image * image)
                step_y[comp, layer] = root * image
            return tuple(now), tuple(after), total_ra, total_aa

        first = tuple(x_sum(tq, comp, 1) for comp in range(comps))
        with scope("q3_image"):
            _, _, gram_ra, gram_aa = lax.fori_loop(
                0,
                layers,
                image_layer,
                ((empty,) * 2, first, nothing, nothing),
                unroll=UNROLL,
            )
            spread_y(tp, EDGE_2)

        def own_x_sum(comp, layer):
            return tp[comp, layer, OWN : OWN + rows, :] + along_x[comp] * (
                tp[comp, layer, OWN + 1 : OWN + rows + 1, :]
                + tp[comp, layer, OWN - 1 : OWN + rows - 1, :]
            )

        def second_layer(layer, carry):
            before, now, total = carry
            four = 4.0 * roots[layer, HALO : HALO + rows, :]
            after = []
            for comp in range(comps):
                after_p = own_x_sum(comp, layer + 2)
                after.append(after_p)
                near = now[comp] + along_z * (before[comp] + after_p)
                image = all_image[slot, comp, layer, HALO : HALO + rows, :]
                second = (
                    field_a[comp, layer, HALO : HALO + rows, :] * image - four * near
                )
                product = image * second
                for low in range(0, rows, 8):
                    total = total + product[low : low + 8]
            return tuple(now), tuple(after), total

        empty_own = jnp.zeros((rows, cols), jnp.float32)
        first = tuple(own_x_sum(comp, 1) for comp in range(comps))
        with scope("q4_second"):
            _, _, gram_ab = lax.fori_loop(
                0, layers, second_layer, ((empty_own,) * 2, first, nothing), unroll=UNROLL
            )
        for number, value in enumerate((gram_rr, gram_ra, gram_aa, gram_ab)):
            gram[4 * member + number] = value

    def to_partner(block):
        pltpu.make_async_remote_copy(
            src_ref=block,
            dst_ref=block,
            send_sem=pair_send.at[0],
            recv_sem=pair_recv.at[0],
            device_id=partner,
            device_id_type=MESH,
        ).start()

    inner = pl.ds(HALO, rows)

    def share_member(member):
        slot = members * ens + member
        for buffer in (all_residual, all_image):
            to_partner(buffer.at[slot, :, :, inner, :])

    for member in range(members):
        if member > 0:
            arrived(1 + member)
        with scope("q0_start"):
            strip_start(member)
            if member == 0:
                arrived(1 + members)
            share_start(member)
        if member == 0:
            with scope("p5_greeted2"):
                greeted_round(2)
            greet_round(4)
            pl.semaphore_signal(
                hand_sem.at[len(hands)], inc=1, device_id=partner, device_id_type=MESH
            )
            arrived(1)
            forces()
        with scope("q1_end"):
            strip_end(member)
            share_end(member)
        if member < members - 1:
            share_member(member)

    lines = 4 * members
    total = jnp.sum(gram[...], axis=1)
    total = jnp.sum(total, axis=1, keepdims=True)
    lane = lax.broadcasted_iota(jnp.int32, (lines, cols), 1)
    line = lax.broadcasted_iota(jnp.int32, (lines, cols), 0)
    message = jnp.sum(
        jnp.where(lane == line + lines * ens, total, 0.0), axis=0, keepdims=True
    )
    with scope("p7_hand"):
        pl.semaphore_wait(hand_sem.at[len(hands)], 1)

    def exchange(ring, me, count, target, send_sem, recv_sem, value, sign=-1):
        ring[me] = value
        for offset in sorted(range(1, count), key=lambda k: sign * min(k, count - k)):
            pltpu.make_async_remote_copy(
                src_ref=ring.at[me],
                dst_ref=ring.at[me],
                send_sem=send_sem.at[0],
                recv_sem=recv_sem.at[0],
                device_id=target(lax.rem(me + offset, count)),
                device_id_type=MESH,
            ).start()
        return pltpu.make_async_remote_copy(
            src_ref=ring.at[pl.ds(0, count - 1)],
            dst_ref=ring.at[pl.ds(0, count - 1)],
            send_sem=send_sem.at[0],
            recv_sem=recv_sem.at[0],
            device_id=target(lax.rem(me + 1, count)),
            device_id_type=MESH,
        )

    cores = 2
    copies_y = exchange(
        ring_y,
        planey * cores + ens,
        planeys * cores,
        lambda peer: {"planey": peer // cores, "ens": lax.rem(peer, cores)},
        y_send,
        y_recv,
        message,
    )

    share_member(members - 1)
    for comp in range(comps):
        for layer in range(layers):
            total = None
            for member in range(members):
                start = mw[0, OWN : OWN + rows, :] * uw[member, comp, layer + 1, OWN : OWN + rows, :]
                total = start if total is None else total + start
            all_start[ens, comp, layer] = total
    to_partner(all_start.at[ens])
    everything = {
        name: sum(counts[name] for counts in rows_of) for name in ("x", "y", "both")
    }
    each_total(everything, lambda total: counted(total, 0).wait_send())
    with scope("p8_ary"):
        copies_y.wait_recv()
    with scope("p6_greeted4"):
        for reach in (4, 8, 16):
            greeted_round(reach)
            if reach > 2:
                greet_round(2 * reach)
    copies_x = exchange(
        ring_x,
        plane,
        planes,
        lambda peer: {"plane": peer},
        x_send,
        x_recv,
        jnp.sum(ring_y[...], axis=0),
        sign=1,
    )
    copies_y.wait_send()
    block = all_residual.at[:, :, :, pl.ds(0, (2 * members + 1) * rows // (2 * members)), :]
    fields = pltpu.make_async_remote_copy(
        src_ref=block,
        dst_ref=block,
        send_sem=pair_send.at[0],
        recv_sem=pair_recv.at[0],
        device_id=partner,
        device_id_type=MESH,
    )
    fields.wait_send()
    fields.wait_recv()
    with scope("p9_arx"):
        copies_x.wait_recv()
    sums = jnp.sum(ring_x[...], axis=0)
    gram_rr = sums
    gram_ra = pltpu.roll(sums, cols - 1, 1)
    gram_aa = pltpu.roll(sums, cols - 2, 1)
    gram_ab = pltpu.roll(sums, cols - 3, 1)
    first_step = gram_rr / gram_ra
    norm_next = gram_rr - 2.0 * first_step * gram_ra + first_step * first_step * gram_aa
    growth = 1.0 + norm_next / gram_rr
    curve = (
        growth * growth * gram_ra
        - 2.0 * growth * first_step * gram_aa
        + first_step * first_step * gram_ab
    )
    second_step = norm_next / curve
    samples = members * cores
    share = 1.0 / samples
    for_residual = share * (first_step + second_step * growth)
    for_image = share * (second_step * first_step)
    lane = lax.broadcasted_iota(jnp.int32, (1, cols), 1)

    def pick(value, number):
        return jnp.sum(jnp.where(lane == 4 * number, value, 0.0), axis=1, keepdims=True)

    weights = [(pick(for_residual, k), pick(for_image, k)) for k in range(samples)]

    def combine(layer, carry):
        for comp in range(comps):
            total = share * (all_start[0, comp, layer] + all_start[1, comp, layer])
            for number in range(samples):
                total = total + (
                    weights[number][0] * all_residual[number, comp, layer, HALO : HALO + rows, :]
                    - weights[number][1] * all_image[number, comp, layer, HALO : HALO + rows, :]
                )
            out[comp, layer] = total
        return carry

    with scope("pa_combine"):
        lax.fori_loop(0, layers, combine, 0, unroll=UNROLL)
    with scope("pb_sent"):
        copies_x.wait_send()


def body(sizes, u_prior, friction_rows, friction_table, bed_fixed, ice_mask):
    planes, planeys = sizes
    members, comps, layers, rows, cols = u_prior.shape
    wide = rows + 2 * HALO
    deep = rows + 24
    samples = 2 * members
    f32 = jnp.float32
    anywhere = pl.BlockSpec(memory_space=pltpu.HBM)
    fields = 2 + members * (1 + comps)
    vmem = pltpu.VMEM
    dma = pltpu.SemaphoreType.DMA
    return pl.pallas_call(
        functools.partial(kernel, sizes),
        out_shape=jax.ShapeDtypeStruct((comps, layers, rows, cols), f32),
        in_specs=[anywhere] * 5,
        out_specs=pl.BlockSpec(memory_space=pltpu.VMEM),
        scratch_shapes=[
            vmem((members, comps, layers + 2, deep, cols), f32),
            vmem((2 + members, deep, cols), f32),
            vmem((fields, deep, cols), f32),
            vmem((fields, deep, cols), f32),
            vmem((fields, deep, cols), f32),
            vmem(friction_table.shape, f32),
            vmem((rows, cols), jnp.int32),
            vmem((rows, cols), jnp.int32),
            pltpu.SMEM((members,), jnp.int32),
            vmem((2 * comps, deep, cols), f32),
            vmem((4 * comps, deep, cols), f32),
            vmem((2 + 4 * comps, wide, cols), f32),
            vmem((4, 2 * cols, cols), jnp.bfloat16),
            vmem((1536, cols), f32),
            vmem((9, wide, cols), f32),
            vmem((9, wide, cols), f32),
            vmem((layers, wide, cols), f32),
            vmem((comps, layers, wide, cols), f32),
            vmem((comps, layers + 2, deep, cols), f32),
            vmem((comps, layers + 2, deep, cols), f32),
            vmem((comps, layers + 2, deep, cols), f32),
            vmem((comps, layers, wide, cols), f32),
            vmem((samples, comps, layers, wide, cols), f32),
            vmem((samples, comps, layers, wide, cols), f32),
            vmem((2, comps, layers, rows, cols), f32),
            vmem((4 * members, 8, cols), f32),
            vmem((2 * planeys, 1, cols), f32),
            vmem((planes, 1, cols), f32),
            dma((members + 2,)),
            dma((1,)),
            dma((2 + members,)),
            pltpu.SemaphoreType.REGULAR((6,)),
            dma((1,)),
            dma((1,)),
            dma((1,)),
            dma((1,)),
            dma((1,)),
            dma((1,)),
        ],
        compiler_params=pltpu.CompilerParams(
            collective_id=0, has_side_effects=True, vmem_limit_bytes=48 * 1024 * 1024
        ),
    )(*[
        pltpu.with_memory_space_constraint(x, pltpu.HBM)
        for x in (u_prior, friction_rows, friction_table, bed_fixed, ice_mask)
    ])


def solution(mesh):
    in_specs = (
        P(("group", "ens"), None, None, "plane", "planey"),
        P(("group", "ens")),
        P("group", "plane", "planey"),
        P("plane", "planey"),
        P("plane", "planey"),
    )
    out_specs = P("group", None, "plane", "planey")
    sizes = (mesh.shape["plane"], mesh.shape["planey"])
    return jax.shard_map(
        functools.partial(body, sizes),
        mesh=mesh,
        in_specs=in_specs,
        out_specs=out_specs,
        check_vma=False,
    )
```
